32 devices in a mesh: row: 8 (over z, core), loop: 4 (over y, x).
Axes of the slice: x: 2, y: 2, z: 4, core: 2. Of those that a mesh axis runs over, the one named last changes fastest.
Arguments:
- student_image: bfloat16 [5120, 1024], P(('row', 'loop')), may hold values from -12 to 12
- student_text: bfloat16 [5120, 1024], P(('row', 'loop')), may hold values from -12 to 12
- teacher_image: bfloat16 [5120, 1024], P('row', 'loop'), may hold values from -12 to 12
- teacher_text: bfloat16 [5120, 1024], P('row', 'loop'), may hold values from -12 to 12
- student_scale: float32 [1], replicated, may hold values from 30 to 100
- teacher_scale: float32 [1], replicated, may hold values from 30 to 100
Outputs:
- loss: float32 [1], replicated
- grad_image: bfloat16 [5120, 1024], P(('row', 'loop'))
- grad_text: bfloat16 [5120, 1024], P(('row', 'loop'))
The draws below stay inside these ranges and needn't reach their ends.
All inputs are finite; a program needn't handle non-finite values.
Results may differ from the reference program's by a relative error of at most 0.014.
The reference program's roundings to bfloat16 on the way (of `simg` and `grad_logits`) count: a program that leaves them out, or rounds other values in their place, can miss the bound.
Values may be sent and summed in bfloat16 or wider, within the bound.
A program may use at most 128 MiB of HBM per device.

```python
import math
import jax
import jax.numpy as jnp
from jax import lax

CODE = 1024
ROWS_DEV = 160
BATCH = 5120
ROW_BLOCK = 640
N_ROW = 8
N_LOOP = 4


def raw_codes(key, stream):
    base_key = jax.random.fold_in(key, stream)
    first = jax.random.normal(jax.random.fold_in(base_key, 1), (BATCH, CODE), jnp.float32)
    second = jax.random.normal(jax.random.fold_in(base_key, 2), (BATCH, CODE), jnp.float32)
    return (first, second)


def blend_weights():
    groups = BATCH // ROW_BLOCK
    group = (jnp.arange(BATCH, dtype=jnp.int32) // ROW_BLOCK).astype(jnp.float32)
    frac = group / float(max(groups - 1, 1))
    theta = 0.1 + (0.5 * math.pi - 0.1) * frac
    return (jnp.cos(theta)[:, None], jnp.sin(theta)[:, None])


def pair_codes(key, stream):
    teach_img, teach_txt = raw_codes(key, 202)
    if stream == 202:
        images, text_rows = (teach_img, teach_txt)
    else:
        own_img, own_txt = raw_codes(key, 101)
        near, far = blend_weights()
        images = near * teach_img + far * own_img
        text_rows = near * teach_txt + far * own_txt
    return (jnp.clip(images, -6.0, 6.0), jnp.clip(text_rows, -6.0, 6.0))


def logit_scales(key):
    scale_key = jax.random.fold_in(key, 300)
    student = jnp.exp(jax.random.uniform(jax.random.fold_in(scale_key, 1), (1,), jnp.float32, math.log(30.0), math.log(100.0)))
    factor = jnp.exp(jax.random.uniform(jax.random.fold_in(scale_key, 2), (1,), jnp.float32, -0.1, 0.1))
    teacher = jnp.clip(student * factor, 30.0, 100.0)
    return (student, teacher)


def draw_student_image(key, part):
    return pair_codes(key, 101)[0].astype(jnp.bfloat16)


def draw_student_text(key, part):
    return pair_codes(key, 101)[1].astype(jnp.bfloat16)


def draw_teacher_image(key, part):
    return pair_codes(key, 202)[0].astype(jnp.bfloat16)


def draw_teacher_text(key, part):
    return pair_codes(key, 202)[1].astype(jnp.bfloat16)


def draw_student_scale(key, part):
    return logit_scales(key)[0]


def draw_teacher_scale(key, part):
    return logit_scales(key)[1]


def setup_inputs(seed: int = 0) -> dict:
    key_of = jax.random.split(jax.random.key(seed), 7)
    student_image = draw_student_image(jax.random.fold_in(key_of[6], 71), 0)
    student_text = draw_student_text(jax.random.fold_in(key_of[6], 71), 0)
    teacher_image = draw_teacher_image(jax.random.fold_in(key_of[6], 71), 0)
    teacher_text = draw_teacher_text(jax.random.fold_in(key_of[6], 71), 0)
    student_scale = draw_student_scale(jax.random.fold_in(key_of[6], 71), 0)
    teacher_scale = draw_teacher_scale(jax.random.fold_in(key_of[6], 71), 0)
    return dict(student_image=student_image, student_text=student_text, teacher_image=teacher_image, teacher_text=teacher_text, student_scale=student_scale, teacher_scale=teacher_scale)


EPS = 1e-06

def unit_rows(codes):
    values = codes.astype(jnp.float32)
    norms = jnp.sqrt(lax.optimization_barrier(jnp.sum(values * values, axis=1, keepdims=True)) + EPS)
    return (values / norms, norms)

def back_norm(grad_unit, units, norms):
    inner = lax.optimization_barrier(jnp.sum(grad_unit * units, axis=1, keepdims=True))
    return ((grad_unit - units * inner) / norms).astype(jnp.bfloat16)

def rounded_term(term):
    narrow = lax.optimization_barrier(term.astype(jnp.bfloat16))
    return narrow.astype(jnp.float32)

def reference(student_image, student_text, teacher_image, teacher_text, student_scale, teacher_scale):
    simg_unit, simg_norm = unit_rows(student_image)
    stxt_unit, stxt_norm = unit_rows(student_text)
    simg = simg_unit.astype(jnp.bfloat16)
    stxt = stxt_unit.astype(jnp.bfloat16)
    timg = unit_rows(teacher_image)[0].astype(jnp.bfloat16)
    ttxt = unit_rows(teacher_text)[0].astype(jnp.bfloat16)
    sscale = student_scale[0]
    tscale = teacher_scale[0]
    block = ROWS_DEV * N_LOOP
    count = BATCH // block
    stxt_split = stxt.reshape(N_ROW, N_LOOP, ROWS_DEV, CODE)

    def one_block(carry, index):
        total, text_acc = carry
        start = (index * block).astype(jnp.int32)
        simg_b = lax.dynamic_slice_in_dim(simg, start, block, 0)
        timg_b = lax.dynamic_slice_in_dim(timg, start, block, 0)
        slog = sscale * jnp.dot(simg_b, stxt.T, preferred_element_type=jnp.float32)
        tlog = tscale * jnp.dot(timg_b, ttxt.T, preferred_element_type=jnp.float32)
        lses = jax.nn.logsumexp(slog, axis=1)
        lset = jax.nn.logsumexp(tlog, axis=1)
        probt = jnp.exp(tlog - lset[:, None])
        probs = jnp.exp(slog - lses[:, None])
        diverge = lax.optimization_barrier(jnp.sum(probt * (tlog - slog), axis=1)) - lset + lses
        grad_logits = (sscale * (probs - probt)).astype(jnp.bfloat16)
        grad_split = grad_logits.reshape(block, N_ROW, N_LOOP, ROWS_DEV)
        dimg = jnp.zeros((block, CODE), jnp.float32)
        for column_class in range(N_LOOP):
            class_cols = grad_split[:, :, column_class, :].reshape(block, N_ROW * ROWS_DEV)
            class_text = stxt_split[:, column_class, :, :].reshape(N_ROW * ROWS_DEV, CODE)
            dimg = dimg + rounded_term(jnp.dot(class_cols, class_text, preferred_element_type=jnp.float32))
        text_term = jnp.dot(grad_logits.T, simg_b, preferred_element_type=jnp.float32)
        text_acc = text_acc + rounded_term(text_term)
        return ((total + jnp.sum(diverge), text_acc), dimg)
    start_carry = (jnp.zeros((), jnp.float32), jnp.zeros((BATCH, CODE), jnp.float32))
    (total, dtxt), dimg_blocks = lax.scan(one_block, start_carry, jnp.arange(count, dtype=jnp.int32))
    dimg = dimg_blocks.reshape(BATCH, CODE)
    loss = (total / BATCH).reshape(1)
    return (loss, back_norm(dimg, simg_unit, simg_norm), back_norm(dtxt, stxt_unit, stxt_norm))
```

```python
import functools
import jax
import jax.numpy as jnp
from jax import lax
from jax.experimental import pallas as pl
from jax.experimental.pallas import tpu as pltpu
from jax.sharding import PartitionSpec as P

EPS = 1e-06
F32 = jnp.float32
BF16 = jnp.bfloat16
MESH = pl.DeviceIdType.MESH
PART = 64
UNIT = 32
STEP = 32


class Ids:
    def __init__(self):
        self.table = {}
        self.count = 0

    def take(self, name, size=1):
        self.table[name] = self.count
        self.count += size

    def __getitem__(self, name):
        return self.table[name]


def chunk_sizes(D):
    sizes = [PART] * (D // PART)
    if D % PART:
        sizes.append(D % PART)
    return sizes


def make_ids(H, n_kh, n_kl, n_lx, n_ly):
    recv, sent = Ids(), Ids()
    recv.take("t_img")
    recv.take("t_txt")
    for a in range(2):
        recv.take(("iz", a), n_kl * H)
        recv.take(("iy", a), H)
        recv.take(("tz", a), n_kh * H)
        recv.take(("tx", a), n_lx * H)
        recv.take(("tc", a), H)
    recv.take("stat")
    recv.take("dc", n_lx * n_kh)
    recv.take("dx", n_lx * n_kh * H)
    recv.take("dz")
    recv.take("gy", n_kl * H)
    recv.take("gz")
    for name in ("lk", "lx", "lc"):
        recv.take(name)
    for name in ("t_img", "t_txt", "stat", "dc", "dx", "dz", "gy", "gz", "loss"):
        sent.take(name)
    for a in range(2):
        for kind in ("img", "first", "txt"):
            sent.take((kind, a))
    return recv, sent


def kernel(
    dims, rid, sid,
    si, st, ti, tt, ssc, tsc,
    loss_out, gi_out, gt_out,
    img_s, img_t, own_s, own_t, txt_s, txt_t, raw_i, raw_t,
    slog, tlog, grad, stat, acc, r1, r2, r3, ry, rz, part, inv_i, inv_t,
    ss, rs,
):
    n_row, n_loop, n_kh, n_kl, n_lx, n_ly, D, code = dims
    sizes = chunk_sizes(D)
    H = len(sizes)
    off = [sum(sizes[:h]) for h in range(H)]
    n_img = n_kl * n_ly
    n_txt = n_kh * n_lx * 2
    rows = n_img * D
    cols = n_txt * D
    r = lax.axis_index("row")
    l = lax.axis_index("loop")
    k, c = r // 2, r % 2
    kh, kl = k // n_kl, k % n_kl
    src_kl, src_j = k // n_kh, k % n_kh
    ly, lx = l // n_lx, l % n_lx
    sscale = ssc[0]
    tscale = tsc[0]

    def dev(k_=None, c_=None, ly_=None, lx_=None):
        kk = k if k_ is None else k_
        cc = c if c_ is None else c_
        yy = ly if ly_ is None else ly_
        xx = lx if lx_ is None else lx_
        return (kk * 2 + cc, yy * n_lx + xx)

    def islot(kl_, ly_):
        return ly_ * n_kl + kl_

    def tslot(j, lx_, c_):
        return (j * n_lx + lx_) * 2 + c_

    def span(start, size, step):
        return pl.ds(pl.multiple_of(start, step), size)

    def irng(h, slot):
        return span(n_img * off[h] + slot * sizes[h], sizes[h], UNIT)

    def trng(h, slot):
        return span(n_txt * off[h] + slot * sizes[h], sizes[h], UNIT)

    def srng(slot, h):
        return span(slot * D + off[h], sizes[h], UNIT)

    def at(slot):
        return span(slot * D, D, UNIT)

    half = [pl.ds(off[h], sizes[h]) for h in range(H)]

    def copy(src, dst, q_send, q_recv, device):
        return pltpu.make_async_remote_copy(
            src_ref=src, dst_ref=dst, send_sem=ss.at[q_send], recv_sem=rs.at[q_recv],
            device_id=device, device_id_type=MESH,
        )

    sent_rows = {}

    def send(src, dst, name, q, device, n=0):
        copy(src, dst, sid[name], q, device).start()
        sent_rows[name] = sent_rows.get(name, 0) + n

    def got(dst, q):
        copy(dst, dst, 0, q, dev(c_=1 - c)).wait_recv()

    def got_rows(n, q):
        got(txt_s.at[pl.ds(0, n), :], q)

    def left(ref, q):
        copy(ref, ref, q, 0, dev(c_=1 - c)).wait_send()

    def left_rows(*names):
        for name in names:
            left(txt_s.at[pl.ds(0, sent_rows.pop(name)), :], sid[name])

    barrier = pltpu.get_barrier_semaphore()
    n_peer = 0
    for d in range(1, n_loop):
        pl.semaphore_signal(barrier, inc=1, device_id=(r, (l + d) % n_loop), device_id_type=MESH)
        n_peer += 1
    for d in range(1, n_kh * n_kl):
        pl.semaphore_signal(barrier, inc=1, device_id=dev(k_=(k + d) % (n_kh * n_kl)), device_id_type=MESH)
        n_peer += 1
    pl.semaphore_signal(barrier, inc=1, device_id=dev(c_=1 - c), device_id_type=MESH)
    n_peer += 1
    for d in range(1, n_kl):
        for e in range(1, n_ly):
            diagonal = dev(k_=kh * n_kl + (kl + d) % n_kl, ly_=(ly + e) % n_ly)
            pl.semaphore_signal(barrier, inc=1, device_id=diagonal, device_id_type=MESH)
            n_peer += 1

    slot0 = islot(kl, ly)

    def unit(load, dst, first, n, keep=None):
        for o in range(0, n, UNIT):
            x = load(o)
            n2 = jnp.sum(x * x, axis=1, keepdims=True) + EPS
            inv = 1.0 / jnp.sqrt(n2)
            if keep is not None:
                keep(o, inv)
            dst[span(first + o, UNIT, UNIT), :] = (x * inv).astype(BF16)

    def student_unit(src, dst, first, h, inv_ref):
        def load(o):
            return src[pl.ds(off[h] + o, UNIT), :].astype(F32)

        def keep(o, inv):
            inv_ref[pl.ds(off[h] + o, UNIT), :] = jnp.broadcast_to(inv, (UNIT, 128))
        unit(load, dst, first, sizes[h], keep)

    def own_text(h):
        student_unit(st, own_s, off[h], h, inv_t)

    def own_image(h):
        student_unit(si, img_s, n_img * off[h] + slot0 * sizes[h], h, inv_i)

    own_text(0)
    own_image(0)
    pl.semaphore_wait(barrier, n_peer)

    def a2a(src, raw, name):
        for d in range(1, n_loop):
            peer = (l + d) % n_loop
            send(src.at[at(peer), :], raw.at[l], name, rid[name], (r, peer))

    def image_first(a, buf, h):
        rng = irng(h, slot0)
        for d in range(1, n_kl):
            q = rid[("iz", a)] + d * H + h
            send(buf.at[rng, :], buf.at[rng, :], ("img", a), q, dev(k_=kh * n_kl + (kl + d) % n_kl), sizes[h])
        for e in range(1, n_ly):
            send(buf.at[rng, :], buf.at[rng, :], ("img", a), rid[("iy", a)] + h, dev(ly_=(ly + e) % n_ly), sizes[h])

    def image_relay(a, buf, h):
        for d in range(1, n_kl):
            rng = irng(h, islot((kl + n_kl - d) % n_kl, ly))
            got(buf.at[rng, :], rid[("iz", a)] + d * H + h)
            for e in range(1, n_ly):
                send(buf.at[rng, :], buf.at[rng, :], ("img", a), rid[("iy", a)] + h, dev(ly_=(ly + e) % n_ly), sizes[h])

    def image_finish(a, h):
        got_rows((n_ly - 1) * n_kl * sizes[h], rid[("iy", a)] + h)

    def text_first(a, own, buf, h):
        rng = trng(h, tslot(src_j, lx, c))
        for g in range(n_kh):
            dest = g * n_kl + src_kl
            op = copy(own.at[half[h], :], buf.at[rng, :], sid[("first", a)],
                      rid[("tz", a)] + src_j * H + h, dev(k_=dest))

            @pl.when(dest != k)
            def _():
                op.start()

            @pl.when(dest == k)
            def _():
                buf[rng, :] = own[half[h], :]

    def first_left(a):
        @pl.when(src_kl == kl)
        def _():
            left(txt_s.at[pl.ds(0, (n_kh - 1) * D), :], sid[("first", a)])

        @pl.when(src_kl != kl)
        def _():
            left(txt_s.at[pl.ds(0, n_kh * D), :], sid[("first", a)])

    def text_relay(a, buf, h):
        for j in range(n_kh):
            rng = trng(h, tslot(j, lx, c))

            @pl.when(kl * n_kh + j != k)
            def _():
                got(buf.at[rng, :], rid[("tz", a)] + j * H + h)

            for e in range(1, n_lx):
                send(buf.at[rng, :], buf.at[rng, :], ("txt", a), rid[("tx", a)] + e * H + h,
                     dev(lx_=(lx + e) % n_lx), sizes[h])
            send(buf.at[rng, :], buf.at[rng, :], ("txt", a), rid[("tc", a)] + h, dev(c_=1 - c), sizes[h])

    def text_cross(a, buf, h):
        for e in range(1, n_lx):
            got_rows(n_kh * sizes[h], rid[("tx", a)] + e * H + h)
            for j in range(n_kh):
                rng = trng(h, tslot(j, (lx + n_lx - e) % n_lx, c))
                send(buf.at[rng, :], buf.at[rng, :], ("txt", a), rid[("tc", a)] + h, dev(c_=1 - c), sizes[h])

    def text_finish(a, h):
        got_rows(n_lx * n_kh * sizes[h], rid[("tc", a)] + h)

    def teacher_wait(src, raw, name):
        raw[l] = src[at(l), :]
        got(raw.at[pl.ds(0, n_loop - 1)], rid[name])

    def teacher_unit(raw, dst, first, h):
        def load(o):
            xs = [raw[f, pl.ds(off[h] + o, UNIT), :].astype(F32) for f in range(n_loop)]
            return jnp.concatenate(xs, axis=1)
        unit(load, dst, first, sizes[h])

    a2a(tt, raw_t, "t_txt")
    a2a(ti, raw_i, "t_img")
    for h in range(H):
        if h:
            own_text(h)
        text_first(0, own_s, txt_s, h)
        if h:
            own_image(h)
        image_first(0, img_s, h)
    text_relay(0, txt_s, 0)
    image_relay(0, img_s, 0)
    teacher_wait(tt, raw_t, "t_txt")
    for h in range(H):
        teacher_unit(raw_t, own_t, off[h], h)
        text_first(1, own_t, txt_t, h)
        if h == 0:
            teacher_wait(ti, raw_i, "t_img")
        teacher_unit(raw_i, img_t, n_img * off[h] + slot0 * sizes[h], h)
        image_first(1, img_t, h)
    for h in range(1, H):
        text_relay(0, txt_s, h)
        image_relay(0, img_s, h)
    for h in range(H):
        text_cross(0, txt_s, h)
        if h == 0:
            text_relay(1, txt_t, 0)
            image_relay(1, img_t, 0)
    for h in range(H):
        image_finish(0, h)
        text_finish(0, h)

    TILE = 256

    def logits(txt, img, scale, out, row0, n, lane0, width):
        lanes = pl.ds(lane0, width)

        def body(i, m):
            o = pl.multiple_of(row0 + i * TILE, TILE)
            v = scale * lax.dot_general(
                txt[pl.ds(o, TILE), :], img[lanes, :], (((1,), (1,)), ((), ())),
                preferred_element_type=F32,
            )
            out[pl.ds(o, TILE), lanes] = v
            return jnp.maximum(m, jnp.max(v.reshape(TILE // 8, 8, width), axis=0))
        m = lax.fori_loop(0, n // TILE, body, jnp.full((8, width), -jnp.inf, F32))
        return jnp.max(m, axis=0, keepdims=True)

    smax = logits(txt_s, img_s, sscale, slog, 0, cols, 0, rows)

    def exps(row0, n, lane0, width, tmax):
        lanes = pl.ds(lane0, width)
        top_s = smax[:, lane0:lane0 + width]

        def fold(v):
            return jnp.sum(v.reshape(STEP // 8, 8, width), axis=0)

        def body(i, carry):
            a, b, x = carry
            o = pl.multiple_of(row0 + i * STEP, STEP)
            s = slog[pl.ds(o, STEP), lanes]
            t = tlog[pl.ds(o, STEP), lanes]
            es = jnp.exp(s - top_s)
            et = jnp.exp(t - tmax)
            slog[pl.ds(o, STEP), lanes] = es
            tlog[pl.ds(o, STEP), lanes] = et
            return (a + fold(es), b + fold(et), x + fold(et * (t - s)))
        zero = jnp.zeros((8, width), F32)
        sums = lax.fori_loop(0, n // STEP, body, (zero, zero, zero), unroll=2)
        return [jnp.sum(v, axis=0, keepdims=True) for v in sums]

    lane0 = [n_img * o for o in off]
    width = [n_img * s for s in sizes]
    row0 = [n_txt * o for o in off]
    height = [n_txt * s for s in sizes]
    tops = {}
    sums = {}

    def group(h, hi):
        first = 0 if h == hi else row0[h]
        n = row0[h] + height[h] - first
        m = logits(txt_t, img_t, tscale, tlog, first, n, lane0[hi], width[hi])
        tops[h, hi] = m
        sums[h, hi] = exps(first, n, lane0[hi], width[hi], m)

    def arrive(h):
        text_cross(1, txt_t, h)
        image_finish(1, h)
        text_finish(1, h)
        for hi in range(h):
            group(h, hi)
        group(h, h)

    for h in range(1, H):
        text_relay(1, txt_t, h)
        image_relay(1, img_t, h)
        if h < H - 1:
            arrive(h - 1)
    for h in range(max(H - 2, 0), H):
        arrive(h)

    best = [functools.reduce(jnp.maximum, [tops[h, hi] for h in range(hi, H)]) for hi in range(H)]

    def wide(parts):
        return jnp.concatenate(parts, axis=1)

    def total(i, hi):
        return sum(sums[h, hi][i] * jnp.exp(tops[h, hi] - best[hi]) for h in range(hi, H))
    asum = wide([sum(sums[h, hi][0] for h in range(hi, H)) for hi in range(H)])
    tmax = wide(best)
    bsum = wide([total(1, hi) for hi in range(H)])
    xsum = wide([total(2, hi) for hi in range(H)])
    pack = [smax, tmax, asum, bsum, xsum]
    stat[slot0] = jnp.concatenate(pack + [jnp.zeros((3, rows), F32)], axis=0)
    for d in range(n_kl):
        for e in range(n_ly):
            if d or e:
                send(stat.at[slot0], stat.at[slot0], "stat", rid["stat"],
                     dev(k_=kh * n_kl + (kl + d) % n_kl, ly_=(ly + e) % n_ly))
    for a in range(2):
        first_left(a)
        left_rows(("img", a), ("txt", a))
    got(stat.at[pl.ds(0, n_img - 1)], rid["stat"])

    all_stat = [stat[s] for s in range(n_img)]
    gs = functools.reduce(jnp.maximum, [v[0:1] for v in all_stat])
    gt = functools.reduce(jnp.maximum, [v[1:2] for v in all_stat])
    es = [jnp.exp(v[0:1] - gs) for v in all_stat]
    et = [jnp.exp(v[1:2] - gt) for v in all_stat]
    ssum = sum(v[2:3] * e for v, e in zip(all_stat, es))
    tsum = sum(v[3:4] * e for v, e in zip(all_stat, et))
    s_mul = sscale * jnp.exp(smax - gs) / ssum
    t_scale = sscale / tsum

    def t_factor(h):
        m = wide([tops[max(h, hi), hi] for hi in range(H)])
        return t_scale * jnp.exp(m - gt)
    t_mul = [t_factor(h) for h in range(H)]

    dtxt = txt_t

    def grad_of(rng, h):
        v = (slog[rng, :] * s_mul - tlog[rng, :] * t_mul[h]).astype(BF16)
        grad[rng, :] = v
        return v

    def text_piece(j, lx_, c_, fresh=False):
        slot = tslot(j, lx_, c_)
        if fresh:
            g = [grad_of(trng(h, slot), h) for h in range(H)]
        else:
            g = [grad[trng(h, slot), :] for h in range(H)]
        v = jnp.dot(jnp.concatenate(g, axis=0), img_s[...], preferred_element_type=F32)
        dtxt[at(slot), :] = v.astype(BF16)

    def to_core(j, x_, q):
        send(dtxt.at[at(tslot(j, x_, 1 - c)), :], r1.at[x_ * n_kh + j], "dc", q, dev(c_=1 - c), D)

    order = [(n_kh - 1 - kh + i) % n_kh for i in range(n_kh)]

    def to_x(e, i):
        x_ = (lx + e) % n_lx
        j = order[i]
        s = x_ * n_kh + j
        got(r1.at[s], rid["dc"] + e * n_kh + i)
        for h in range(H):
            rng = srng(tslot(j, x_, c), h)
            dtxt[rng, :] = (dtxt[rng, :].astype(F32) + r1[s, half[h], :].astype(F32)).astype(BF16)
            q = rid["dx"] + (e * n_kh + i) * H + h
            send(dtxt.at[rng, :], r2.at[(e - 1) * n_kh + j, half[h], :], "dx", q, dev(lx_=x_), sizes[h])

    dimg = img_t
    full = [h for h in range(H) if (n_kl * sizes[h]) % 128 == 0]
    rest = [h for h in range(H) if h not in full]
    KT = 256

    def image_piece(y_, with_rest):
        windows = [pl.ds(pl.multiple_of(lane0[h] + y_ * n_kl * sizes[h], 128), n_kl * sizes[h]) for h in full]
        lens = [n_kl * sizes[h] for h in full]
        if with_rest:
            windows += [pl.ds(lane0[h], width[h]) for h in rest]
            lens += [width[h] for h in rest]
        M = sum(lens)

        def body(i, _):
            o = pl.multiple_of(i * KT, KT)
            g = jnp.concatenate([grad[pl.ds(o, KT), w] for w in windows], axis=1)
            v = lax.dot_general(g, txt_s[pl.ds(o, KT), :], (((0,), (0,)), ((), ())), preferred_element_type=F32)

            @pl.when(i == 0)
            def _():
                acc[pl.ds(0, M), :] = v

            @pl.when(i != 0)
            def _():
                acc[pl.ds(0, M), :] += v
            return 0
        lax.fori_loop(0, cols // KT, body, 0)
        o = 0
        for h in full:
            for p in range(n_kl):
                dimg[srng(islot(p, y_), h), :] = acc[pl.ds(o, sizes[h]), :].astype(BF16)
                o += sizes[h]
        if with_rest:
            for h in rest:
                for s in range(n_img):
                    dimg[srng(s, h), :] = acc[pl.ds(o, sizes[h]), :].astype(BF16)
                    o += sizes[h]

    def to_y(e):
        y_ = (ly + e) % n_ly
        image_piece(y_, e == 1)
        for d in [*range(1, n_kl), 0]:
            for h in range(H):
                q = rid["gy"] + d * H + h
                send(dimg.at[srng(islot((kl + d) % n_kl, y_), h), :], ry.at[(e - 1) * n_kl + d, half[h], :],
                     "gy", q, dev(ly_=y_), sizes[h])

    x1 = (lx + 1) % n_lx
    text_piece(order[0], x1, 1 - c, True)
    to_core(order[0], x1, rid["dc"] + n_kh)
    text_piece(order[0], x1, c, True)

    for h in range(H):
        def to_grad(i, _):
            grad_of(span(row0[h] + i * STEP, STEP, STEP), h)
            return 0
        lax.fori_loop(0, height[h] // STEP, to_grad, 0, unroll=2)
    to_x(1, 0)
    for e in range(1, n_ly):
        to_y(e)

    cross = sum(v[4:5] * e for v, e in zip(all_stat, et))
    diverge = cross / tsum - (gt + jnp.log(tsum)) + (gs + jnp.log(ssum))
    part[kh] = jnp.broadcast_to(jnp.sum(diverge, axis=1, keepdims=True), (8, 128))
    for d in range(1, n_kh):
        send(part.at[kh], part.at[kh], "loss", rid["lk"], dev(k_=((kh + d) % n_kh) * n_kl + kl))

    for e in range(1, n_lx):
        x_ = (lx + e) % n_lx
        for i in range(1 if e == 1 else 0, n_kh):
            text_piece(order[i], x_, 1 - c)
            to_core(order[i], x_, rid["dc"] + e * n_kh + i)
            text_piece(order[i], x_, c)
            to_x(e, i)

    got(part.at[pl.ds(0, n_kh - 1)], rid["lk"])
    base = n_kh
    part[base + lx] = sum(part[i] for i in range(n_kh))
    for d in range(1, n_lx):
        send(part.at[base + lx], part.at[base + lx], "loss", rid["lx"], dev(lx_=(lx + d) % n_lx))

    for i in range(n_kh):
        text_piece(order[i], lx, 1 - c)
        to_core(order[i], lx, rid["dc"] + i)
    for i in range(n_kh):
        text_piece(order[i], lx, c)
    image_piece(ly, n_ly == 1)

    got(part.at[pl.ds(0, n_lx - 1)], rid["lx"])
    base = n_kh + n_lx
    part[base + c] = sum(part[n_kh + i] for i in range(n_lx))
    send(part.at[base + c], part.at[base + c], "loss", rid["lc"], dev(c_=1 - c))

    def owner_copy(i, h):
        j = order[i]
        dest = kl * n_kh + j
        op = copy(dtxt.at[srng(tslot(j, lx, c), h), :], r3.at[kh, half[h], :], sid["dz"], rid["dz"], dev(k_=dest))
        return dest, op

    def text_sum(i, h):
        j = order[i]
        s = lx * n_kh + j
        if h == 0:
            got(r1.at[s], rid["dc"] + i)
        rng = srng(tslot(j, lx, c), h)
        v = dtxt[rng, :].astype(F32) + r1[s, half[h], :].astype(F32)
        for e in range(1, n_lx):
            got(r2.at[(e - 1) * n_kh + j, half[h], :], rid["dx"] + (e * n_kh + i) * H + h)
            v = v + r2[(e - 1) * n_kh + j, half[h], :].astype(F32)
        dtxt[rng, :] = v.astype(BF16)
        dest, op = owner_copy(i, h)

        @pl.when(dest != k)
        def _():
            op.start()

        @pl.when(dest == k)
        def _():
            r3[kh, half[h], :] = dtxt[rng, :]

    def got_y(d, h):
        got_rows((n_ly - 1) * sizes[h], rid["gy"] + d * H + h)

    def image_sum(d, h):
        got_y(d, h)
        rng = srng(islot((kl + d) % n_kl, ly), h)
        v = dimg[rng, :].astype(F32)
        for e in range(1, n_ly):
            v = v + ry[(e - 1) * n_kl + d, half[h], :].astype(F32)
        dimg[rng, :] = v.astype(BF16)
        send(dimg.at[rng, :], rz.at[d - 1, half[h], :], "gz", rid["gz"], dev(k_=kh * n_kl + (kl + d) % n_kl), sizes[h])

    for i in range(n_kh):
        for h in range(H):
            text_sum(i, h)
            if 1 <= i + 1 < n_kl:
                image_sum(i + 1, h)
    for d in range(n_kh + 1, n_kl):
        for h in range(H):
            image_sum(d, h)

    got(part.at[base + 1 - c], rid["lc"])
    loss_out[...] = (part[base] + part[base + 1]) / float(D * n_row * n_loop)

    def finish(terms, src, inv_ref, out):
        for o in range(0, D, UNIT):
            rng = pl.ds(o, UNIT)
            g = terms(o)
            x = src[rng, :].astype(F32)
            inv = inv_ref[rng, 0:1]
            along = jnp.sum(g * x, axis=1, keepdims=True) * inv * inv
            out[rng, :] = ((g - x * along) * inv).astype(BF16)

    for h in range(H):
        got_y(0, h)
    got_rows((n_kl - 1) * D, rid["gz"])

    def image_terms(o):
        v = dimg[span(slot0 * D + o, UNIT, UNIT), :].astype(F32)
        for e in range(1, n_ly):
            v = v + ry[(e - 1) * n_kl, pl.ds(o, UNIT), :].astype(F32)
        for d in range(1, n_kl):
            v = v + rz[d - 1, pl.ds(o, UNIT), :].astype(F32)
        return v
    finish(image_terms, si, inv_i, gi_out)

    def on_owner(wait):
        @pl.when(src_kl == kl)
        def _():
            wait(n_kh - 1)

        @pl.when(src_kl != kl)
        def _():
            wait(n_kh)
    on_owner(lambda n: got(txt_s.at[pl.ds(0, n * D), :], rid["dz"]))
    finish(lambda o: sum(r3[g, pl.ds(o, UNIT), :].astype(F32) for g in range(n_kh)), st, inv_t, gt_out)

    for name, raw in (("t_txt", raw_t), ("t_img", raw_i)):
        left(raw.at[pl.ds(0, n_loop - 1)], sid[name])
    left(stat.at[pl.ds(0, n_img - 1)], sid["stat"])
    left_rows("dc", "dx", "gy", "gz")
    left(part.at[pl.ds(0, n_kh - 1 + n_lx - 1 + 1)], sid["loss"])

    on_owner(lambda n: left(txt_s.at[pl.ds(0, n * D), :], sid["dz"]))


def emit(total, gi, gt, loss_out, gi_out, gt_out):
    loss_out[0] = total[0, 0]
    gi_out[...] = gi[...]
    gt_out[...] = gt[...]


def on_device(n_row, n_loop, si, st, ti, tt, ssc, tsc):
    D, code = si.shape
    n_kl, n_lx = 2, 2
    n_kh, n_ly = n_row // (2 * n_kl), n_loop // n_lx
    n_img, n_txt = n_kl * n_ly, n_kh * n_lx * 2
    rows, cols = n_img * D, n_txt * D
    sizes = chunk_sizes(D)
    rid, sid = make_ids(len(sizes), n_kh, n_kl, n_lx, n_ly)
    window = sum(n_kl * s if (n_kl * s) % 128 == 0 else n_img * s for s in sizes)
    dims = (n_row, n_loop, n_kh, n_kl, n_lx, n_ly, D, code)
    vm = pl.BlockSpec(memory_space=pltpu.VMEM)
    sm = pl.BlockSpec(memory_space=pltpu.SMEM)
    V = pltpu.VMEM
    loss, gi, gt = pl.pallas_call(
        functools.partial(kernel, dims, rid, sid),
        out_shape=(
            jax.ShapeDtypeStruct((8, 128), F32),
            jax.ShapeDtypeStruct((D, code), BF16),
            jax.ShapeDtypeStruct((D, code), BF16),
        ),
        in_specs=[vm] * 4 + [sm] * 2,
        out_specs=(vm, vm, vm),
        scratch_shapes=[
            V((rows, code), BF16), V((rows, code), BF16),
            V((D, code), BF16), V((D, code), BF16),
            V((cols, code), BF16), V((cols, code), BF16),
            V((n_loop, D, code // n_loop), BF16), V((n_loop, D, code // n_loop), BF16),
            V((cols, rows), F32), V((cols, rows), F32), V((cols, rows), BF16),
            V((n_img, 8, rows), F32),
            V((window, code), F32),
            V((n_lx * n_kh, D, code), BF16),
            V(((n_lx - 1) * n_kh, D, code), BF16),
            V((n_kh, D, code), BF16),
            V(((n_ly - 1) * n_kl, D, code), BF16),
            V((n_kl - 1, D, code), BF16),
            V((n_kh + n_lx + 2, 8, 128), F32),
            V((D, 128), F32), V((D, 128), F32),
            pltpu.SemaphoreType.DMA((sid.count,)),
            pltpu.SemaphoreType.DMA((rid.count,)),
        ],
        compiler_params=pltpu.CompilerParams(
            collective_id=0, has_side_effects=True, vmem_limit_bytes=67043328,
        ),
    )(si, st, ti, tt, ssc, tsc)
    return pl.pallas_call(
        emit,
        out_shape=(
            jax.ShapeDtypeStruct((1,), F32),
            jax.ShapeDtypeStruct((D, code), BF16),
            jax.ShapeDtypeStruct((D, code), BF16),
        ),
        in_specs=[vm] * 3,
        out_specs=(sm, vm, vm),
    )(loss, gi, gt)


def solution(mesh):
    return jax.shard_map(
        functools.partial(on_device, mesh.shape["row"], mesh.shape["loop"]),
        mesh=mesh,
        in_specs=(
            P(("row", "loop"), None),
            P(("row", "loop"), None),
            P("row", "loop"),
            P("row", "loop"),
            P(),
            P(),
        ),
        out_specs=(P(), P(("row", "loop"), None), P(("row", "loop"), None)),
        check_vma=False,
    )
```

```python
import functools
import jax
import jax.numpy as jnp
from jax import lax
from jax.experimental import pallas as pl
from jax.experimental.pallas import tpu as pltpu
from jax.sharding import PartitionSpec as P

EPS = 1e-06
F32 = jnp.float32
BF16 = jnp.bfloat16
MESH = pl.DeviceIdType.MESH
PART = 64
UNIT = 32
STEP = 32


class Ids:
    def __init__(self):
        self.table = {}
        self.count = 0

    def take(self, name, size=1):
        self.table[name] = self.count
        self.count += size

    def __getitem__(self, name):
        return self.table[name]


def chunk_sizes(D):
    sizes = [PART] * (D // PART)
    if D % PART:
        sizes.append(D % PART)
    return sizes


def make_ids(H, n_kh, n_kl, n_lx, n_ly):
    recv, sent = Ids(), Ids()
    recv.take("t_img")
    recv.take("t_txt")
    for a in range(2):
        recv.take(("iz", a), n_kl * H)
        recv.take(("iy", a), H)
        recv.take(("tz", a), n_kh * H)
        recv.take(("tx", a), n_lx * H)
        recv.take(("tc", a), H)
    recv.take("stat")
    recv.take("dc", n_lx * n_kh * H)
    recv.take("dx", n_lx * n_kh * H)
    recv.take("dz")
    recv.take("gy", n_kl * H)
    recv.take("gz")
    recv.take("loss")
    for name in ("t_img", "t_txt", "stat", "dc", "dx", "dz", "gy", "gz", "loss"):
        sent.take(name)
    for a in range(2):
        for kind in ("img", "first", "txt"):
            sent.take((kind, a))
    return recv, sent


def kernel(
    dims, rid, sid,
    si, st, ti, tt, ssc, tsc,
    loss_out, gi_out, gt_out,
    img_s, img_t, own_s, own_t, txt_s, txt_t, raw_i, raw_t,
    slog, tlog, grad, stat, acc, r1, r2, r3, ry, rz, part, inv_i, inv_t,
    ss, rs,
):
    n_row, n_loop, n_kh, n_kl, n_lx, n_ly, D, code = dims
    sizes = chunk_sizes(D)
    H = len(sizes)
    off = [sum(sizes[:h]) for h in range(H)]
    n_img = n_kl * n_ly
    n_txt = n_kh * n_lx * 2
    rows = n_img * D
    cols = n_txt * D
    r = lax.axis_index("row")
    l = lax.axis_index("loop")
    k, c = r // 2, r % 2
    kh, kl = k // n_kl, k % n_kl
    src_kl, src_j = k // n_kh, k % n_kh
    ly, lx = l // n_lx, l % n_lx
    sscale = ssc[0]
    tscale = tsc[0]

    def dev(k_=None, c_=None, ly_=None, lx_=None):
        kk = k if k_ is None else k_
        cc = c if c_ is None else c_
        yy = ly if ly_ is None else ly_
        xx = lx if lx_ is None else lx_
        return (kk * 2 + cc, yy * n_lx + xx)

    def islot(kl_, ly_):
        return ly_ * n_kl + kl_

    def tslot(j, lx_, c_):
        return (j * n_lx + lx_) * 2 + c_

    def span(start, size, step):
        return pl.ds(pl.multiple_of(start, step), size)

    def irng(h, slot):
        return span(n_img * off[h] + slot * sizes[h], sizes[h], UNIT)

    def trng(h, slot):
        return span(n_txt * off[h] + slot * sizes[h], sizes[h], UNIT)

    def srng(slot, h):
        return span(slot * D + off[h], sizes[h], UNIT)

    def at(slot):
        return span(slot * D, D, UNIT)

    half = [pl.ds(off[h], sizes[h]) for h in range(H)]

    def copy(src, dst, q_send, q_recv, device):
        return pltpu.make_async_remote_copy(
            src_ref=src, dst_ref=dst, send_sem=ss.at[q_send], recv_sem=rs.at[q_recv],
            device_id=device, device_id_type=MESH,
        )

    sent_rows = {}

    def send(src, dst, name, q, device, n=0):
        copy(src, dst, sid[name], q, device).start()
        sent_rows[name] = sent_rows.get(name, 0) + n

    def got(dst, q):
        copy(dst, dst, 0, q, dev(c_=1 - c)).wait_recv()

    def got_rows(n, q):
        got(txt_s.at[pl.ds(0, n), :], q)

    def left(ref, q):
        copy(ref, ref, q, 0, dev(c_=1 - c)).wait_send()

    def left_rows(*names):
        for name in names:
            left(txt_s.at[pl.ds(0, sent_rows.pop(name)), :], sid[name])

    loss_peers = [
        (kd, xd, cd) for kd in range(n_kh) for xd in range(n_lx) for cd in range(2) if kd or xd or cd
    ]

    def loss_peer(kd, xd, cd):
        return dev(k_=((kh + kd) % n_kh) * n_kl + kl, c_=(c + cd) % 2, lx_=(lx + xd) % n_lx)

    barrier = pltpu.get_barrier_semaphore()
    n_peer = 0
    for kd, xd, cd in loss_peers:
        if (kd != 0) + (xd != 0) + (cd != 0) > 1:
            pl.semaphore_signal(barrier, inc=1, device_id=loss_peer(kd, xd, cd), device_id_type=MESH)
            n_peer += 1
    for d in range(1, n_loop):
        pl.semaphore_signal(barrier, inc=1, device_id=(r, (l + d) % n_loop), device_id_type=MESH)
        n_peer += 1
    for d in range(1, n_kh * n_kl):
        pl.semaphore_signal(barrier, inc=1, device_id=dev(k_=(k + d) % (n_kh * n_kl)), device_id_type=MESH)
        n_peer += 1
    pl.semaphore_signal(barrier, inc=1, device_id=dev(c_=1 - c), device_id_type=MESH)
    n_peer += 1
    for d in range(1, n_kl):
        for e in range(1, n_ly):
            diagonal = dev(k_=kh * n_kl + (kl + d) % n_kl, ly_=(ly + e) % n_ly)
            pl.semaphore_signal(barrier, inc=1, device_id=diagonal, device_id_type=MESH)
            n_peer += 1

    slot0 = islot(kl, ly)

    def unit(load, dst, first, n, keep=None):
        for o in range(0, n, UNIT):
            x = load(o)
            n2 = jnp.sum(x * x, axis=1, keepdims=True) + EPS
            inv = 1.0 / jnp.sqrt(n2)
            if keep is not None:
                keep(o, inv)
            dst[span(first + o, UNIT, UNIT), :] = (x * inv).astype(BF16)

    def student_unit(src, dst, first, h, inv_ref):
        def load(o):
            return src[pl.ds(off[h] + o, UNIT), :].astype(F32)

        def keep(o, inv):
            inv_ref[pl.ds(off[h] + o, UNIT), :] = jnp.broadcast_to(inv, (UNIT, 128))
        unit(load, dst, first, sizes[h], keep)

    def own_text(h):
        student_unit(st, own_s, off[h], h, inv_t)

    def own_image(h):
        student_unit(si, img_s, n_img * off[h] + slot0 * sizes[h], h, inv_i)

    own_text(0)
    own_image(0)
    pl.semaphore_wait(barrier, n_peer)

    def a2a(src, raw, name):
        for d in range(1, n_loop):
            peer = (l + d) % n_loop
            send(src.at[at(peer), :], raw.at[l], name, rid[name], (r, peer))

    def image_first(a, buf, h):
        rng = irng(h, slot0)
        for d in range(1, n_kl):
            q = rid[("iz", a)] + d * H + h
            send(buf.at[rng, :], buf.at[rng, :], ("img", a), q, dev(k_=kh * n_kl + (kl + d) % n_kl), sizes[h])

    def image_y(a, buf, h):
        rng = irng(h, slot0)
        for e in range(1, n_ly):
            send(buf.at[rng, :], buf.at[rng, :], ("img", a), rid[("iy", a)] + h, dev(ly_=(ly + e) % n_ly), sizes[h])

    def image_relay(a, buf, h):
        for d in range(1, n_kl):
            rng = irng(h, islot((kl + n_kl - d) % n_kl, ly))
            got(buf.at[rng, :], rid[("iz", a)] + d * H + h)
            for e in range(1, n_ly):
                send(buf.at[rng, :], buf.at[rng, :], ("img", a), rid[("iy", a)] + h, dev(ly_=(ly + e) % n_ly), sizes[h])

    def image_finish(a, h):
        got_rows((n_ly - 1) * n_kl * sizes[h], rid[("iy", a)] + h)

    def text_first(a, own, buf, h):
        rng = trng(h, tslot(src_j, lx, c))
        for g in range(n_kh):
            dest = g * n_kl + src_kl
            op = copy(own.at[half[h], :], buf.at[rng, :], sid[("first", a)],
                      rid[("tz", a)] + src_j * H + h, dev(k_=dest))

            @pl.when(dest != k)
            def _():
                op.start()

            @pl.when(dest == k)
            def _():
                buf[rng, :] = own[half[h], :]

    def first_left(a):
        @pl.when(src_kl == kl)
        def _():
            left(txt_s.at[pl.ds(0, (n_kh - 1) * D), :], sid[("first", a)])

        @pl.when(src_kl != kl)
        def _():
            left(txt_s.at[pl.ds(0, n_kh * D), :], sid[("first", a)])

    def text_relay(a, buf, h):
        for j in range(n_kh):
            rng = trng(h, tslot(j, lx, c))

            @pl.when(kl * n_kh + j != k)
            def _():
                got(buf.at[rng, :], rid[("tz", a)] + j * H + h)

            for e in range(1, n_lx):
                send(buf.at[rng, :], buf.at[rng, :], ("txt", a), rid[("tx", a)] + e * H + h,
                     dev(lx_=(lx + e) % n_lx), sizes[h])
            send(buf.at[rng, :], buf.at[rng, :], ("txt", a), rid[("tc", a)] + h, dev(c_=1 - c), sizes[h])

    def text_cross(a, buf, h):
        for e in range(1, n_lx):
            got_rows(n_kh * sizes[h], rid[("tx", a)] + e * H + h)
            for j in range(n_kh):
                rng = trng(h, tslot(j, (lx + n_lx - e) % n_lx, c))
                send(buf.at[rng, :], buf.at[rng, :], ("txt", a), rid[("tc", a)] + h, dev(c_=1 - c), sizes[h])

    def text_finish(a, h):
        got_rows(n_lx * n_kh * sizes[h], rid[("tc", a)] + h)

    def teacher_wait(src, raw, name):
        raw[l] = src[at(l), :]
        got(raw.at[pl.ds(0, n_loop - 1)], rid[name])

    def teacher_unit(raw, dst, first, h):
        def load(o):
            xs = [raw[f, pl.ds(off[h] + o, UNIT), :].astype(F32) for f in range(n_loop)]
            return jnp.concatenate(xs, axis=1)
        unit(load, dst, first, sizes[h])

    a2a(tt, raw_t, "t_txt")
    a2a(ti, raw_i, "t_img")
    for h in range(H):
        if h:
            own_text(h)
        text_first(0, own_s, txt_s, h)
        if h:
            own_image(h)
        image_first(0, img_s, h)
        image_y(0, img_s, h)
    text_relay(0, txt_s, 0)
    image_relay(0, img_s, 0)
    teacher_wait(tt, raw_t, "t_txt")
    for h in range(H):
        teacher_unit(raw_t, own_t, off[h], h)
        text_first(1, own_t, txt_t, h)
        if h == 0:
            teacher_wait(ti, raw_i, "t_img")
        teacher_unit(raw_i, img_t, n_img * off[h] + slot0 * sizes[h], h)
        image_first(1, img_t, h)
    for h in range(1, H):
        text_relay(0, txt_s, h)
        image_relay(0, img_s, h)
    for h in range(H):
        image_y(1, img_t, h)
    for h in range(H):
        text_cross(0, txt_s, h)
        if h == H - 2:
            text_relay(1, txt_t, 0)
            image_relay(1, img_t, 0)
    for h in range(H):
        image_finish(0, h)
        text_finish(0, h)

    TILE = 256

    def logits(txt, img, scale, out, row0, n, lane0, width):
        lanes = pl.ds(lane0, width)

        def body(i, m):
            o = pl.multiple_of(row0 + i * TILE, TILE)
            v = scale * lax.dot_general(
                txt[pl.ds(o, TILE), :], img[lanes, :], (((1,), (1,)), ((), ())),
                preferred_element_type=F32,
            )
            out[pl.ds(o, TILE), lanes] = v
            return jnp.maximum(m, jnp.max(v.reshape(TILE // 8, 8, width), axis=0))
        m = lax.fori_loop(0, n // TILE, body, jnp.full((8, width), -jnp.inf, F32))
        return jnp.max(m, axis=0, keepdims=True)

    smax = logits(txt_s, img_s, sscale, slog, 0, cols, 0, rows)

    def exps(row0, n, lane0, width, tmax):
        lanes = pl.ds(lane0, width)
        top_s = smax[:, lane0:lane0 + width]

        def fold(v):
            return jnp.sum(v.reshape(STEP // 8, 8, width), axis=0)

        def body(i, carry):
            a, b, x = carry
            o = pl.multiple_of(row0 + i * STEP, STEP)
            s = slog[pl.ds(o, STEP), lanes]
            t = tlog[pl.ds(o, STEP), lanes]
            es = jnp.exp(s - top_s)
            et = jnp.exp(t - tmax)
            slog[pl.ds(o, STEP), lanes] = es
            tlog[pl.ds(o, STEP), lanes] = et
            return (a + fold(es), b + fold(et), x + fold(et * (t - s)))
        zero = jnp.zeros((8, width), F32)
        sums = lax.fori_loop(0, n // STEP, body, (zero, zero, zero), unroll=2)
        return [jnp.sum(v, axis=0, keepdims=True) for v in sums]

    lane0 = [n_img * o for o in off]
    width = [n_img * s for s in sizes]
    row0 = [n_txt * o for o in off]
    height = [n_txt * s for s in sizes]
    tops = {}
    sums = {}

    def group(h, hi):
        first = 0 if h == hi else row0[h]
        n = row0[h] + height[h] - first
        m = logits(txt_t, img_t, tscale, tlog, first, n, lane0[hi], width[hi])
        tops[h, hi] = m
        sums[h, hi] = exps(first, n, lane0[hi], width[hi], m)

    def arrive(h):
        text_cross(1, txt_t, h)
        image_finish(1, h)
        text_finish(1, h)
        for hi in range(h):
            group(h, hi)
        group(h, h)

    for h in range(1, H):
        text_relay(1, txt_t, h)
        image_relay(1, img_t, h)
    for h in range(H):
        arrive(h)

    best = [functools.reduce(jnp.maximum, [tops[h, hi] for h in range(hi, H)]) for hi in range(H)]

    def wide(parts):
        return jnp.concatenate(parts, axis=1)

    def total(i, hi):
        return sum(sums[h, hi][i] * jnp.exp(tops[h, hi] - best[hi]) for h in range(hi, H))
    asum = wide([sum(sums[h, hi][0] for h in range(hi, H)) for hi in range(H)])
    tmax = wide(best)
    bsum = wide([total(1, hi) for hi in range(H)])
    xsum = wide([total(2, hi) for hi in range(H)])
    pack = [smax, tmax, asum, bsum, xsum]
    stat[slot0] = jnp.concatenate(pack + [jnp.zeros((3, rows), F32)], axis=0)
    for d in range(n_kl):
        for e in range(n_ly):
            if d or e:
                send(stat.at[slot0], stat.at[slot0], "stat", rid["stat"],
                     dev(k_=kh * n_kl + (kl + d) % n_kl, ly_=(ly + e) % n_ly))
    for a in range(2):
        first_left(a)
        left_rows(("img", a), ("txt", a))
    got(stat.at[pl.ds(0, n_img - 1)], rid["stat"])

    all_stat = [stat[s] for s in range(n_img)]
    gs = functools.reduce(jnp.maximum, [v[0:1] for v in all_stat])
    gt = functools.reduce(jnp.maximum, [v[1:2] for v in all_stat])
    es = [jnp.exp(v[0:1] - gs) for v in all_stat]
    et = [jnp.exp(v[1:2] - gt) for v in all_stat]
    ssum = sum(v[2:3] * e for v, e in zip(all_stat, es))
    tsum = sum(v[3:4] * e for v, e in zip(all_stat, et))
    cross = sum(v[4:5] * e for v, e in zip(all_stat, et))
    diverge = cross / tsum - (gt + jnp.log(tsum)) + (gs + jnp.log(ssum))
    mine = tslot(kh, lx, c)
    part[mine] = jnp.broadcast_to(jnp.sum(diverge, axis=1, keepdims=True), (8, 128))
    for peer in loss_peers:
        send(part.at[mine], part.at[mine], "loss", rid["loss"], loss_peer(*peer))

    s_mul = sscale * jnp.exp(smax - gs) / ssum
    t_scale = sscale / tsum

    def t_factor(h):
        m = wide([tops[max(h, hi), hi] for hi in range(H)])
        return t_scale * jnp.exp(m - gt)
    t_mul = [t_factor(h) for h in range(H)]

    dtxt = txt_t

    def grad_of(rng, h):
        v = (slog[rng, :] * s_mul - tlog[rng, :] * t_mul[h]).astype(BF16)
        grad[rng, :] = v
        return v

    def text_piece(j, lx_, c_, fresh=False):
        slot = tslot(j, lx_, c_)
        if fresh:
            g = [grad_of(trng(h, slot), h) for h in range(H)]
        else:
            g = [grad[trng(h, slot), :] for h in range(H)]
        v = jnp.dot(jnp.concatenate(g, axis=0), img_s[...], preferred_element_type=F32)
        dtxt[at(slot), :] = v.astype(BF16)

    order = [(n_kh - 1 - kh + i) % n_kh for i in range(n_kh)]

    def to_core(e, i, fresh=False):
        x_ = (lx + e) % n_lx
        j = order[i]
        text_piece(j, x_, 1 - c, fresh)
        for h in range(H):
            send(dtxt.at[srng(tslot(j, x_, 1 - c), h), :], r1.at[x_ * n_kh + j, half[h], :], "dc",
                 rid["dc"] + (e * n_kh + i) * H + h, dev(c_=1 - c), sizes[h])

    def from_core(e, i, h):
        s = ((lx + e) % n_lx) * n_kh + order[i]
        got(r1.at[s, half[h], :], rid["dc"] + (e * n_kh + i) * H + h)
        return r1[s, half[h], :].astype(F32)

    def to_x(e, i):
        x_ = (lx + e) % n_lx
        j = order[i]
        for h in range(H):
            rng = srng(tslot(j, x_, c), h)
            dtxt[rng, :] = (dtxt[rng, :].astype(F32) + from_core(e, i, h)).astype(BF16)
            q = rid["dx"] + (e * n_kh + i) * H + h
            send(dtxt.at[rng, :], r2.at[(e - 1) * n_kh + j, half[h], :], "dx", q, dev(lx_=x_), sizes[h])

    dimg = img_t
    full = [h for h in range(H) if (n_kl * sizes[h]) % 128 == 0]
    rest = [h for h in range(H) if h not in full]
    KT = 256

    def image_piece(y_, with_rest):
        windows = [pl.ds(pl.multiple_of(lane0[h] + y_ * n_kl * sizes[h], 128), n_kl * sizes[h]) for h in full]
        lens = [n_kl * sizes[h] for h in full]
        if with_rest:
            windows += [pl.ds(lane0[h], width[h]) for h in rest]
            lens += [width[h] for h in rest]
        M = sum(lens)

        def body(i, _):
            o = pl.multiple_of(i * KT, KT)
            g = jnp.concatenate([grad[pl.ds(o, KT), w] for w in windows], axis=1)
            v = lax.dot_general(g, txt_s[pl.ds(o, KT), :], (((0,), (0,)), ((), ())), preferred_element_type=F32)

            @pl.when(i == 0)
            def _():
                acc[pl.ds(0, M), :] = v

            @pl.when(i != 0)
            def _():
                acc[pl.ds(0, M), :] += v
            return 0
        lax.fori_loop(0, cols // KT, body, 0)
        o = 0
        for h in full:
            for p in range(n_kl):
                dimg[srng(islot(p, y_), h), :] = acc[pl.ds(o, sizes[h]), :].astype(BF16)
                o += sizes[h]
        if with_rest:
            for h in rest:
                for s in range(n_img):
                    dimg[srng(s, h), :] = acc[pl.ds(o, sizes[h]), :].astype(BF16)
                    o += sizes[h]

    def to_y(e):
        y_ = (ly + e) % n_ly
        image_piece(y_, e == 1)
        for d in [*range(1, n_kl), 0]:
            for h in range(H):
                q = rid["gy"] + d * H + h
                send(dimg.at[srng(islot((kl + d) % n_kl, y_), h), :], ry.at[(e - 1) * n_kl + d, half[h], :],
                     "gy", q, dev(ly_=y_), sizes[h])

    x1 = (lx + 1) % n_lx
    to_core(1, 0, True)
    text_piece(order[0], x1, c, True)
    for h in range(H):
        def to_grad(i, _):
            grad_of(span(row0[h] + i * STEP, STEP, STEP), h)
            return 0
        lax.fori_loop(0, height[h] // STEP, to_grad, 0, unroll=2)
    to_x(1, 0)
    for e in range(1, n_ly):
        to_y(e)
    to_core(0, 0)
    text_piece(order[0], lx, c)
    for e in range(1, n_lx):
        for i in range(1 if e == 1 else 0, n_kh):
            to_core(e, i)
            text_piece(order[i], (lx + e) % n_lx, c)
            if e > 1 or i > 1:
                to_x(e, i)
    image_piece(ly, n_ly == 1)
    if n_kh > 1:
        to_x(1, 1)

    def owner_copy(i, h):
        j = order[i]
        dest = kl * n_kh + j
        op = copy(dtxt.at[srng(tslot(j, lx, c), h), :], r3.at[kh, half[h], :], sid["dz"], rid["dz"], dev(k_=dest))
        return dest, op

    def text_sum(i, h):
        j = order[i]
        rng = srng(tslot(j, lx, c), h)
        v = dtxt[rng, :].astype(F32) + from_core(0, i, h)
        for e in range(1, n_lx):
            got(r2.at[(e - 1) * n_kh + j, half[h], :], rid["dx"] + (e * n_kh + i) * H + h)
            v = v + r2[(e - 1) * n_kh + j, half[h], :].astype(F32)
        dtxt[rng, :] = v.astype(BF16)
        dest, op = owner_copy(i, h)

        @pl.when(dest != k)
        def _():
            op.start()

        @pl.when(dest == k)
        def _():
            r3[kh, half[h], :] = dtxt[rng, :]

    def got_y(d, h):
        got_rows((n_ly - 1) * sizes[h], rid["gy"] + d * H + h)

    def image_sum(d, h):
        got_y(d, h)
        rng = srng(islot((kl + d) % n_kl, ly), h)
        v = dimg[rng, :].astype(F32)
        for e in range(1, n_ly):
            v = v + ry[(e - 1) * n_kl + d, half[h], :].astype(F32)
        dimg[rng, :] = v.astype(BF16)
        send(dimg.at[rng, :], rz.at[d - 1, half[h], :], "gz", rid["gz"], dev(k_=kh * n_kl + (kl + d) % n_kl), sizes[h])

    for i in range(n_kh):
        for h in range(H):
            text_sum(i, h)
            if h == 0 and i + 1 < n_kh:
                to_core(0, i + 1)
                text_piece(order[i + 1], lx, c)
            if 1 <= i + 1 < n_kl:
                image_sum(i + 1, h)
    for d in range(n_kh + 1, n_kl):
        for h in range(H):
            image_sum(d, h)
    got(part.at[pl.ds(0, len(loss_peers))], rid["loss"])
    loss_out[...] = sum(part[i] for i in range(n_txt)) / float(D * n_row * n_loop)

    def finish(terms, src, inv_ref, out):
        for o in range(0, D, UNIT):
            rng = pl.ds(o, UNIT)
            g = terms(o)
            x = src[rng, :].astype(F32)
            inv = inv_ref[rng, 0:1]
            along = jnp.sum(g * x, axis=1, keepdims=True) * inv * inv
            out[rng, :] = ((g - x * along) * inv).astype(BF16)

    for h in range(H):
        got_y(0, h)
    got_rows((n_kl - 1) * D, rid["gz"])

    def image_terms(o):
        v = dimg[span(slot0 * D + o, UNIT, UNIT), :].astype(F32)
        for e in range(1, n_ly):
            v = v + ry[(e - 1) * n_kl, pl.ds(o, UNIT), :].astype(F32)
        for d in range(1, n_kl):
            v = v + rz[d - 1, pl.ds(o, UNIT), :].astype(F32)
        return v
    finish(image_terms, si, inv_i, gi_out)

    def on_owner(wait):
        @pl.when(src_kl == kl)
        def _():
            wait(n_kh - 1)

        @pl.when(src_kl != kl)
        def _():
            wait(n_kh)
    on_owner(lambda n: got(txt_s.at[pl.ds(0, n * D), :], rid["dz"]))
    finish(lambda o: sum(r3[g, pl.ds(o, UNIT), :].astype(F32) for g in range(n_kh)), st, inv_t, gt_out)

    for name, raw in (("t_txt", raw_t), ("t_img", raw_i)):
        left(raw.at[pl.ds(0, n_loop - 1)], sid[name])
    left(stat.at[pl.ds(0, n_img - 1)], sid["stat"])
    left_rows("dc", "dx", "gy", "gz")
    left(part.at[pl.ds(0, len(loss_peers))], sid["loss"])

    on_owner(lambda n: left(txt_s.at[pl.ds(0, n * D), :], sid["dz"]))


def emit(total, gi, gt, loss_out, gi_out, gt_out):
    loss_out[0] = total[0, 0]
    gi_out[...] = gi[...]
    gt_out[...] = gt[...]


def on_device(n_row, n_loop, si, st, ti, tt, ssc, tsc):
    D, code = si.shape
    n_kl, n_lx = 2, 2
    n_kh, n_ly = n_row // (2 * n_kl), n_loop // n_lx
    n_img, n_txt = n_kl * n_ly, n_kh * n_lx * 2
    rows, cols = n_img * D, n_txt * D
    sizes = chunk_sizes(D)
    rid, sid = make_ids(len(sizes), n_kh, n_kl, n_lx, n_ly)
    window = sum(n_kl * s if (n_kl * s) % 128 == 0 else n_img * s for s in sizes)
    dims = (n_row, n_loop, n_kh, n_kl, n_lx, n_ly, D, code)
    vm = pl.BlockSpec(memory_space=pltpu.VMEM)
    sm = pl.BlockSpec(memory_space=pltpu.SMEM)
    V = pltpu.VMEM
    loss, gi, gt = pl.pallas_call(
        functools.partial(kernel, dims, rid, sid),
        out_shape=(
            jax.ShapeDtypeStruct((8, 128), F32),
            jax.ShapeDtypeStruct((D, code), BF16),
            jax.ShapeDtypeStruct((D, code), BF16),
        ),
        in_specs=[vm] * 4 + [sm] * 2,
        out_specs=(vm, vm, vm),
        scratch_shapes=[
            V((rows, code), BF16), V((rows, code), BF16),
            V((D, code), BF16), V((D, code), BF16),
            V((cols, code), BF16), V((cols, code), BF16),
            V((n_loop, D, code // n_loop), BF16), V((n_loop, D, code // n_loop), BF16),
            V((cols, rows), F32), V((cols, rows), F32), V((cols, rows), BF16),
            V((n_img, 8, rows), F32),
            V((window, code), F32),
            V((n_lx * n_kh, D, code), BF16),
            V(((n_lx - 1) * n_kh, D, code), BF16),
            V((n_kh, D, code), BF16),
            V(((n_ly - 1) * n_kl, D, code), BF16),
            V((n_kl - 1, D, code), BF16),
            V((n_txt, 8, 128), F32),
            V((D, 128), F32), V((D, 128), F32),
            pltpu.SemaphoreType.DMA((sid.count,)),
            pltpu.SemaphoreType.DMA((rid.count,)),
        ],
        compiler_params=pltpu.CompilerParams(
            collective_id=0, has_side_effects=True, vmem_limit_bytes=67043328,
        ),
    )(si, st, ti, tt, ssc, tsc)
    return pl.pallas_call(
        emit,
        out_shape=(
            jax.ShapeDtypeStruct((1,), F32),
            jax.ShapeDtypeStruct((D, code), BF16),
            jax.ShapeDtypeStruct((D, code), BF16),
        ),
        in_specs=[vm] * 3,
        out_specs=(sm, vm, vm),
    )(loss, gi, gt)


def solution(mesh):
    return jax.shard_map(
        functools.partial(on_device, mesh.shape["row"], mesh.shape["loop"]),
        mesh=mesh,
        in_specs=(
            P(("row", "loop"), None),
            P(("row", "loop"), None),
            P("row", "loop"),
            P("row", "loop"),
            P(),
            P(),
        ),
        out_specs=(P(), P(("row", "loop"), None), P(("row", "loop"), None)),
        check_vma=False,
    )
```

```python
import functools
import jax
import jax.numpy as jnp
from jax import lax
from jax.experimental import pallas as pl
from jax.experimental.pallas import tpu as pltpu
from jax.sharding import PartitionSpec as P

EPS = 1e-06
F32 = jnp.float32
BF16 = jnp.bfloat16
MESH = pl.DeviceIdType.MESH
PART = 64
UNIT = 32
STEP = 32
DOT = 1280


class Ids:
    def __init__(self):
        self.table = {}
        self.count = 0

    def take(self, name, size=1):
        self.table[name] = self.count
        self.count += size

    def __getitem__(self, name):
        return self.table[name]


def chunk_sizes(D):
    sizes = [PART] * (D // PART)
    if D % PART:
        sizes.append(D % PART)
    return sizes


def make_ids(H, n_kh, n_kl, n_lx, n_ly):
    recv, sent = Ids(), Ids()
    recv.take("t_img")
    recv.take("t_txt")
    for a in range(2):
        recv.take(("iz", a), n_kl * H)
        recv.take(("iy", a), H)
        recv.take(("tz", a), n_kh * H)
        recv.take(("tx", a), n_lx * H)
        recv.take(("tc", a), H)
    recv.take("stat")
    recv.take("dc", n_lx * n_kh * H)
    recv.take("dx", n_lx * n_kh * H)
    recv.take("dz")
    recv.take("gy", n_kl * H)
    recv.take("gz")
    recv.take("loss")
    for name in ("t_img", "t_txt", "stat", "dc", "dx", "dz", "gy", "gz", "loss"):
        sent.take(name)
    for a in range(2):
        for kind in ("img", "first", "txt"):
            sent.take((kind, a))
    return recv, sent


def kernel(
    dims, rid, sid,
    si, st, ti, tt, ssc, tsc,
    loss_out, gi_out, gt_out,
    img_s, img_t, own_s, own_t, txt_s, txt_t, raw_i, raw_t,
    slog, tlog, grad, stat, r1, r2, r3, ry, rz, part, inv_i, inv_t,
    ss, rs,
):
    n_row, n_loop, n_kh, n_kl, n_lx, n_ly, D, code = dims
    sizes = chunk_sizes(D)
    H = len(sizes)
    off = [sum(sizes[:h]) for h in range(H)]
    n_img = n_kl * n_ly
    n_txt = n_kh * n_lx * 2
    rows = n_img * D
    cols = n_txt * D
    r = lax.axis_index("row")
    l = lax.axis_index("loop")
    k, c = r // 2, r % 2
    kh, kl = k // n_kl, k % n_kl
    src_kl, src_j = k // n_kh, k % n_kh
    ly, lx = l // n_lx, l % n_lx
    sscale = ssc[0]
    tscale = tsc[0]

    def dev(k_=None, c_=None, ly_=None, lx_=None):
        kk = k if k_ is None else k_
        cc = c if c_ is None else c_
        yy = ly if ly_ is None else ly_
        xx = lx if lx_ is None else lx_
        return (kk * 2 + cc, yy * n_lx + xx)

    def islot(kl_, ly_):
        return ly_ * n_kl + kl_

    def tslot(j, lx_, c_):
        return (j * n_lx + lx_) * 2 + c_

    def span(start, size, step):
        return pl.ds(pl.multiple_of(start, step), size)

    def irng(h, slot):
        return span(n_img * off[h] + slot * sizes[h], sizes[h], UNIT)

    def trng(h, slot):
        return span(n_txt * off[h] + slot * sizes[h], sizes[h], UNIT)

    def srng(slot, h):
        return span(slot * D + off[h], sizes[h], UNIT)

    def at(slot):
        return span(slot * D, D, UNIT)

    half = [pl.ds(off[h], sizes[h]) for h in range(H)]
    back = sorted(range(H), key=lambda h: sizes[h])

    def copy(src, dst, q_send, q_recv, device):
        return pltpu.make_async_remote_copy(
            src_ref=src, dst_ref=dst, send_sem=ss.at[q_send], recv_sem=rs.at[q_recv],
            device_id=device, device_id_type=MESH,
        )

    sent_rows = {}

    def send(src, dst, name, q, device, n=0):
        copy(src, dst, sid[name], q, device).start()
        sent_rows[name] = sent_rows.get(name, 0) + n

    def got(dst, q):
        copy(dst, dst, 0, q, dev(c_=1 - c)).wait_recv()

    def got_rows(n, q):
        got(txt_s.at[pl.ds(0, n), :], q)

    def left(ref, q):
        copy(ref, ref, q, 0, dev(c_=1 - c)).wait_send()

    def left_rows(*names):
        for name in names:
            left(txt_s.at[pl.ds(0, sent_rows.pop(name)), :], sid[name])

    loss_peers = [
        (kd, xd, cd) for kd in range(n_kh) for xd in range(n_lx) for cd in range(2) if kd or xd or cd
    ]

    def loss_peer(kd, xd, cd):
        return dev(k_=((kh + kd) % n_kh) * n_kl + kl, c_=(c + cd) % 2, lx_=(lx + xd) % n_lx)

    barrier = pltpu.get_barrier_semaphore()
    n_peer = 0
    for kd, xd, cd in loss_peers:
        if (kd != 0) + (xd != 0) + (cd != 0) > 1:
            pl.semaphore_signal(barrier, inc=1, device_id=loss_peer(kd, xd, cd), device_id_type=MESH)
            n_peer += 1
    for d in range(1, n_loop):
        pl.semaphore_signal(barrier, inc=1, device_id=(r, (l + d) % n_loop), device_id_type=MESH)
        n_peer += 1
    for d in range(1, n_kh * n_kl):
        pl.semaphore_signal(barrier, inc=1, device_id=dev(k_=(k + d) % (n_kh * n_kl)), device_id_type=MESH)
        n_peer += 1
    pl.semaphore_signal(barrier, inc=1, device_id=dev(c_=1 - c), device_id_type=MESH)
    n_peer += 1
    for d in range(1, n_kl):
        for e in range(1, n_ly):
            diagonal = dev(k_=kh * n_kl + (kl + d) % n_kl, ly_=(ly + e) % n_ly)
            pl.semaphore_signal(barrier, inc=1, device_id=diagonal, device_id_type=MESH)
            n_peer += 1

    slot0 = islot(kl, ly)

    def unit(load, dst, first, n, keep=None):
        for o in range(0, n, UNIT):
            x = load(o)
            n2 = jnp.sum(x * x, axis=1, keepdims=True) + EPS
            inv = 1.0 / jnp.sqrt(n2)
            if keep is not None:
                keep(o, inv)
            dst[span(first + o, UNIT, UNIT), :] = (x * inv).astype(BF16)

    def student_unit(src, dst, first, h, inv_ref):
        def load(o):
            return src[pl.ds(off[h] + o, UNIT), :].astype(F32)

        def keep(o, inv):
            inv_ref[pl.ds(off[h] + o, UNIT), :] = jnp.broadcast_to(inv, (UNIT, 128))
        unit(load, dst, first, sizes[h], keep)

    def own_text(h):
        student_unit(st, own_s, off[h], h, inv_t)

    def own_image(h):
        student_unit(si, img_s, n_img * off[h] + slot0 * sizes[h], h, inv_i)

    own_text(0)
    own_image(0)
    pl.semaphore_wait(barrier, n_peer)

    def a2a(src, raw, name):
        for d in range(1, n_loop):
            peer = (l + d) % n_loop
            send(src.at[at(peer), :], raw.at[l], name, rid[name], (r, peer))

    def image_first(a, buf, h):
        rng = irng(h, slot0)
        for d in range(1, n_kl):
            q = rid[("iz", a)] + d * H + h
            send(buf.at[rng, :], buf.at[rng, :], ("img", a), q, dev(k_=kh * n_kl + (kl + d) % n_kl), sizes[h])

    def image_y(a, buf, h):
        rng = irng(h, slot0)
        for e in range(1, n_ly):
            send(buf.at[rng, :], buf.at[rng, :], ("img", a), rid[("iy", a)] + h, dev(ly_=(ly + e) % n_ly), sizes[h])

    def image_relay(a, buf, h):
        for d in range(1, n_kl):
            rng = irng(h, islot((kl + n_kl - d) % n_kl, ly))
            got(buf.at[rng, :], rid[("iz", a)] + d * H + h)
            for e in range(1, n_ly):
                send(buf.at[rng, :], buf.at[rng, :], ("img", a), rid[("iy", a)] + h, dev(ly_=(ly + e) % n_ly), sizes[h])

    def image_finish(a, h):
        got_rows((n_ly - 1) * n_kl * sizes[h], rid[("iy", a)] + h)

    def text_first(a, own, buf, h):
        rng = trng(h, tslot(src_j, lx, c))
        for g in range(n_kh):
            dest = g * n_kl + src_kl
            op = copy(own.at[half[h], :], buf.at[rng, :], sid[("first", a)],
                      rid[("tz", a)] + src_j * H + h, dev(k_=dest))

            @pl.when(dest != k)
            def _():
                op.start()

            @pl.when(dest == k)
            def _():
                buf[rng, :] = own[half[h], :]

    def first_left(a):
        @pl.when(src_kl == kl)
        def _():
            left(txt_s.at[pl.ds(0, (n_kh - 1) * D), :], sid[("first", a)])

        @pl.when(src_kl != kl)
        def _():
            left(txt_s.at[pl.ds(0, n_kh * D), :], sid[("first", a)])

    def text_relay(a, buf, h):
        for j in range(n_kh):
            rng = trng(h, tslot(j, lx, c))

            @pl.when(kl * n_kh + j != k)
            def _():
                got(buf.at[rng, :], rid[("tz", a)] + j * H + h)

            for e in range(1, n_lx):
                send(buf.at[rng, :], buf.at[rng, :], ("txt", a), rid[("tx", a)] + e * H + h,
                     dev(lx_=(lx + e) % n_lx), sizes[h])
            send(buf.at[rng, :], buf.at[rng, :], ("txt", a), rid[("tc", a)] + h, dev(c_=1 - c), sizes[h])

    def text_cross(a, buf, h):
        for e in range(1, n_lx):
            got_rows(n_kh * sizes[h], rid[("tx", a)] + e * H + h)
            for j in range(n_kh):
                rng = trng(h, tslot(j, (lx + n_lx - e) % n_lx, c))
                send(buf.at[rng, :], buf.at[rng, :], ("txt", a), rid[("tc", a)] + h, dev(c_=1 - c), sizes[h])

    def text_finish(a, h):
        got_rows(n_lx * n_kh * sizes[h], rid[("tc", a)] + h)

    def teacher_wait(src, raw, name):
        raw[l] = src[at(l), :]
        got(raw.at[pl.ds(0, n_loop - 1)], rid[name])

    def teacher_unit(raw, dst, first, h):
        def load(o):
            xs = [raw[f, pl.ds(off[h] + o, UNIT), :].astype(F32) for f in range(n_loop)]
            return jnp.concatenate(xs, axis=1)
        unit(load, dst, first, sizes[h])

    a2a(tt, raw_t, "t_txt")
    a2a(ti, raw_i, "t_img")
    for h in range(H):
        if h:
            own_text(h)
        text_first(0, own_s, txt_s, h)
        if h:
            own_image(h)
        image_first(0, img_s, h)
        image_y(0, img_s, h)
    text_relay(0, txt_s, 0)
    image_relay(0, img_s, 0)
    teacher_wait(tt, raw_t, "t_txt")
    for h in range(H):
        teacher_unit(raw_t, own_t, off[h], h)
        text_first(1, own_t, txt_t, h)
        if h == 0:
            teacher_wait(ti, raw_i, "t_img")
        teacher_unit(raw_i, img_t, n_img * off[h] + slot0 * sizes[h], h)
        image_first(1, img_t, h)
    for h in range(1, H):
        text_relay(0, txt_s, h)
        image_relay(0, img_s, h)
    for h in range(H):
        image_y(1, img_t, h)
    for h in range(H):
        text_cross(0, txt_s, h)
        if h == H - 2:
            text_relay(1, txt_t, 0)
            image_relay(1, img_t, 0)
    for h in range(H):
        image_finish(0, h)
        text_finish(0, h)

    def tile_of(n):
        return max(t for t in range(UNIT, min(n, DOT) + 1, UNIT) if n % t == 0)

    def logits(txt, img, scale, out, row0, n, lane0, width):
        lanes = pl.ds(lane0, width)

        tile = tile_of(n)
        m = jnp.full((8, width), -jnp.inf, F32)
        for o in range(row0, row0 + n, tile):
            v = scale * lax.dot_general(
                txt[pl.ds(o, tile), :], img[lanes, :], (((1,), (1,)), ((), ())),
                preferred_element_type=F32,
            )
            out[pl.ds(o, tile), lanes] = v
            m = jnp.maximum(m, jnp.max(v.reshape(tile // 8, 8, width), axis=0))
        return jnp.max(m, axis=0, keepdims=True)

    smax = logits(txt_s, img_s, sscale, slog, 0, cols, 0, rows)

    def exps(row0, n, lane0, width, tmax):
        lanes = pl.ds(lane0, width)
        top_s = smax[:, lane0:lane0 + width]

        def fold(v):
            return jnp.sum(v.reshape(STEP // 8, 8, width), axis=0)

        def body(i, carry):
            a, b, x = carry
            o = pl.multiple_of(row0 + i * STEP, STEP)
            s = slog[pl.ds(o, STEP), lanes]
            t = tlog[pl.ds(o, STEP), lanes]
            es = jnp.exp(s - top_s)
            et = jnp.exp(t - tmax)
            slog[pl.ds(o, STEP), lanes] = es
            tlog[pl.ds(o, STEP), lanes] = et
            return (a + fold(es), b + fold(et), x + fold(et * (t - s)))
        zero = jnp.zeros((8, width), F32)
        sums = lax.fori_loop(0, n // STEP, body, (zero, zero, zero), unroll=2)
        return [jnp.sum(v, axis=0, keepdims=True) for v in sums]

    lane0 = [n_img * o for o in off]
    width = [n_img * s for s in sizes]
    row0 = [n_txt * o for o in off]
    height = [n_txt * s for s in sizes]
    tops = {}
    sums = {}

    def group(h, hi):
        first = 0 if h == hi else row0[h]
        n = row0[h] + height[h] - first
        m = logits(txt_t, img_t, tscale, tlog, first, n, lane0[hi], width[hi])
        tops[h, hi] = m
        sums[h, hi] = exps(first, n, lane0[hi], width[hi], m)

    def arrive(h):
        image_finish(1, h)
        text_finish(1, h)
        for hi in range(h):
            group(h, hi)
        if 0 < h < H - 1:
            text_cross(1, txt_t, h + 1)
        group(h, h)

    for h in range(1, H):
        text_relay(1, txt_t, h)
        image_relay(1, img_t, h)
    for h in range(H):
        if h < 2:
            text_cross(1, txt_t, h)
        arrive(h)

    best = [functools.reduce(jnp.maximum, [tops[h, hi] for h in range(hi, H)]) for hi in range(H)]

    def wide(parts):
        return jnp.concatenate(parts, axis=1)

    def total(i, hi):
        return sum(sums[h, hi][i] * jnp.exp(tops[h, hi] - best[hi]) for h in range(hi, H))
    asum = wide([sum(sums[h, hi][0] for h in range(hi, H)) for hi in range(H)])
    tmax = wide(best)
    bsum = wide([total(1, hi) for hi in range(H)])
    xsum = wide([total(2, hi) for hi in range(H)])
    pack = [smax, tmax, asum, bsum, xsum]
    stat[slot0] = jnp.concatenate(pack + [jnp.zeros((3, rows), F32)], axis=0)
    for d in range(n_kl):
        for e in range(n_ly):
            if d or e:
                send(stat.at[slot0], stat.at[slot0], "stat", rid["stat"],
                     dev(k_=kh * n_kl + (kl + d) % n_kl, ly_=(ly + e) % n_ly))
    for a in range(2):
        first_left(a)
        left_rows(("img", a), ("txt", a))
    got(stat.at[pl.ds(0, n_img - 1)], rid["stat"])

    all_stat = [stat[s] for s in range(n_img)]
    gs = functools.reduce(jnp.maximum, [v[0:1] for v in all_stat])
    gt = functools.reduce(jnp.maximum, [v[1:2] for v in all_stat])
    es = [jnp.exp(v[0:1] - gs) for v in all_stat]
    et = [jnp.exp(v[1:2] - gt) for v in all_stat]
    ssum = sum(v[2:3] * e for v, e in zip(all_stat, es))
    tsum = sum(v[3:4] * e for v, e in zip(all_stat, et))
    cross = sum(v[4:5] * e for v, e in zip(all_stat, et))
    diverge = cross / tsum - (gt + jnp.log(tsum)) + (gs + jnp.log(ssum))
    mine = tslot(kh, lx, c)
    part[mine] = jnp.broadcast_to(jnp.sum(diverge, axis=1, keepdims=True), (8, 128))
    for peer in loss_peers:
        send(part.at[mine], part.at[mine], "loss", rid["loss"], loss_peer(*peer))

    s_mul = sscale * jnp.exp(smax - gs) / ssum
    t_scale = sscale / tsum

    def t_factor(h):
        m = wide([tops[max(h, hi), hi] for hi in range(H)])
        return t_scale * jnp.exp(m - gt)
    t_mul = [t_factor(h) for h in range(H)]

    dtxt = txt_t

    def grad_of(rng, h):
        v = (slog[rng, :] * s_mul - tlog[rng, :] * t_mul[h]).astype(BF16)
        grad[rng, :] = v
        return v

    def text_piece(j, lx_, c_, fresh=False):
        slot = tslot(j, lx_, c_)
        if fresh:
            g = [grad_of(trng(h, slot), h) for h in range(H)]
        else:
            g = [grad[trng(h, slot), :] for h in range(H)]
        v = jnp.dot(jnp.concatenate(g, axis=0), img_s[...], preferred_element_type=F32)
        dtxt[at(slot), :] = v.astype(BF16)

    order = [(n_kh - 1 - kh + i) % n_kh for i in range(n_kh)]

    def to_core(e, i, fresh=False):
        x_ = (lx + e) % n_lx
        j = order[i]
        text_piece(j, x_, 1 - c, fresh)
        for h in back:
            send(dtxt.at[srng(tslot(j, x_, 1 - c), h), :], r1.at[x_ * n_kh + j, half[h], :], "dc",
                 rid["dc"] + (e * n_kh + i) * H + h, dev(c_=1 - c), sizes[h])

    def from_core(e, i, h):
        s = ((lx + e) % n_lx) * n_kh + order[i]
        got(r1.at[s, half[h], :], rid["dc"] + (e * n_kh + i) * H + h)
        return r1[s, half[h], :].astype(F32)

    def to_x(e, i):
        x_ = (lx + e) % n_lx
        j = order[i]
        for h in back:
            rng = srng(tslot(j, x_, c), h)
            dtxt[rng, :] = (dtxt[rng, :].astype(F32) + from_core(e, i, h)).astype(BF16)
            q = rid["dx"] + (e * n_kh + i) * H + h
            send(dtxt.at[rng, :], r2.at[(e - 1) * n_kh + j, half[h], :], "dx", q, dev(lx_=x_), sizes[h])

    dimg = img_t
    full = [h for h in range(H) if (n_kl * sizes[h]) % 128 == 0]
    rest = [h for h in range(H) if h not in full]

    def image_piece(y_, with_rest):
        windows = [pl.ds(pl.multiple_of(lane0[h] + y_ * n_kl * sizes[h], 128), n_kl * sizes[h]) for h in full]
        if with_rest:
            windows += [pl.ds(lane0[h], width[h]) for h in rest]
        tile = tile_of(cols)
        v = 0.0
        for o in range(0, cols, tile):
            g = jnp.concatenate([grad[pl.ds(o, tile), w] for w in windows], axis=1)
            v = v + lax.dot_general(g, txt_s[pl.ds(o, tile), :], (((0,), (0,)), ((), ())), preferred_element_type=F32)
        v = v.astype(BF16)
        o = 0
        for h in full:
            for p in range(n_kl):
                dimg[srng(islot(p, y_), h), :] = v[o:o + sizes[h]]
                o += sizes[h]
        if with_rest:
            for h in rest:
                for s in range(n_img):
                    dimg[srng(s, h), :] = v[o:o + sizes[h]]
                    o += sizes[h]

    def to_y(e):
        y_ = (ly + e) % n_ly
        image_piece(y_, e == 1)
        for d in [*range(1, n_kl), 0]:
            for h in back:
                q = rid["gy"] + d * H + h
                send(dimg.at[srng(islot((kl + d) % n_kl, y_), h), :], ry.at[(e - 1) * n_kl + d, half[h], :],
                     "gy", q, dev(ly_=y_), sizes[h])

    x1 = (lx + 1) % n_lx
    to_core(1, 0, True)
    text_piece(order[0], x1, c, True)
    for h in range(H):
        def to_grad(i, _):
            grad_of(span(row0[h] + i * STEP, STEP, STEP), h)
            return 0
        lax.fori_loop(0, height[h] // STEP, to_grad, 0, unroll=2)
    to_x(1, 0)
    to_core(0, 0)
    text_piece(order[0], lx, c)
    for e in range(1, n_ly):
        to_y(e)

    def owner_copy(i, h):
        j = order[i]
        dest = kl * n_kh + j
        op = copy(dtxt.at[srng(tslot(j, lx, c), h), :], r3.at[kh, half[h], :], sid["dz"], rid["dz"], dev(k_=dest))
        return dest, op

    def text_sum(i, h):
        j = order[i]
        rng = srng(tslot(j, lx, c), h)
        v = dtxt[rng, :].astype(F32) + from_core(0, i, h)
        for e in range(1, n_lx):
            got(r2.at[(e - 1) * n_kh + j, half[h], :], rid["dx"] + (e * n_kh + i) * H + h)
            v = v + r2[(e - 1) * n_kh + j, half[h], :].astype(F32)
        dtxt[rng, :] = v.astype(BF16)
        dest, op = owner_copy(i, h)

        @pl.when(dest != k)
        def _():
            op.start()

        @pl.when(dest == k)
        def _():
            r3[kh, half[h], :] = dtxt[rng, :]

    def got_y(d, h):
        got_rows((n_ly - 1) * sizes[h], rid["gy"] + d * H + h)

    def image_sum(d, h):
        got_y(d, h)
        rng = srng(islot((kl + d) % n_kl, ly), h)
        v = dimg[rng, :].astype(F32)
        for e in range(1, n_ly):
            v = v + ry[(e - 1) * n_kl + d, half[h], :].astype(F32)
        dimg[rng, :] = v.astype(BF16)
        send(dimg.at[rng, :], rz.at[d - 1, half[h], :], "gz", rid["gz"], dev(k_=kh * n_kl + (kl + d) % n_kl), sizes[h])

    text_sum(0, back[0])
    for e in range(1, n_lx):
        for i in range(1 if e == 1 else 0, n_kh):
            to_core(e, i)
            text_piece(order[i], (lx + e) % n_lx, c)
            if e > 1 or i > 1:
                to_x(e, i)
    image_piece(ly, n_ly == 1)
    if n_kh > 1:
        to_x(1, 1)
    texts = [(i, h) for i in range(n_kh) for h in back][1:]
    images = [(d, h) for d in range(1, n_kl) for h in back]
    while texts or images:
        if texts:
            i, h = texts.pop(0)
            if h == back[-1] and i + 1 < n_kh:
                to_core(0, i + 1)
                text_piece(order[i + 1], lx, c)
            text_sum(i, h)
        if images:
            image_sum(*images.pop(0))
    got(part.at[pl.ds(0, len(loss_peers))], rid["loss"])
    loss_out[...] = sum(part[i] for i in range(n_txt)) / float(D * n_row * n_loop)

    def finish(terms, src, inv_ref, out):
        for o in range(0, D, UNIT):
            rng = pl.ds(o, UNIT)
            g = terms(o)
            x = src[rng, :].astype(F32)
            inv = inv_ref[rng, 0:1]
            along = jnp.sum(g * x, axis=1, keepdims=True) * inv * inv
            out[rng, :] = ((g - x * along) * inv).astype(BF16)

    for h in range(H):
        got_y(0, h)
    got_rows((n_kl - 1) * D, rid["gz"])

    def image_terms(o):
        v = dimg[span(slot0 * D + o, UNIT, UNIT), :].astype(F32)
        for e in range(1, n_ly):
            v = v + ry[(e - 1) * n_kl, pl.ds(o, UNIT), :].astype(F32)
        for d in range(1, n_kl):
            v = v + rz[d - 1, pl.ds(o, UNIT), :].astype(F32)
        return v
    finish(image_terms, si, inv_i, gi_out)

    def on_owner(wait):
        @pl.when(src_kl == kl)
        def _():
            wait(n_kh - 1)

        @pl.when(src_kl != kl)
        def _():
            wait(n_kh)
    on_owner(lambda n: got(txt_s.at[pl.ds(0, n * D), :], rid["dz"]))
    finish(lambda o: sum(r3[g, pl.ds(o, UNIT), :].astype(F32) for g in range(n_kh)), st, inv_t, gt_out)

    for name, raw in (("t_txt", raw_t), ("t_img", raw_i)):
        left(raw.at[pl.ds(0, n_loop - 1)], sid[name])
    left(stat.at[pl.ds(0, n_img - 1)], sid["stat"])
    left_rows("dc", "dx", "gy", "gz")
    left(part.at[pl.ds(0, len(loss_peers))], sid["loss"])

    on_owner(lambda n: left(txt_s.at[pl.ds(0, n * D), :], sid["dz"]))


def emit(total, gi, gt, loss_out, gi_out, gt_out):
    loss_out[0] = total[0, 0]
    gi_out[...] = gi[...]
    gt_out[...] = gt[...]


def on_device(n_row, n_loop, si, st, ti, tt, ssc, tsc):
    D, code = si.shape
    n_kl, n_lx = 2, 2
    n_kh, n_ly = n_row // (2 * n_kl), n_loop // n_lx
    n_img, n_txt = n_kl * n_ly, n_kh * n_lx * 2
    rows, cols = n_img * D, n_txt * D
    sizes = chunk_sizes(D)
    rid, sid = make_ids(len(sizes), n_kh, n_kl, n_lx, n_ly)
    dims = (n_row, n_loop, n_kh, n_kl, n_lx, n_ly, D, code)
    vm = pl.BlockSpec(memory_space=pltpu.VMEM)
    sm = pl.BlockSpec(memory_space=pltpu.SMEM)
    V = pltpu.VMEM
    loss, gi, gt = pl.pallas_call(
        functools.partial(kernel, dims, rid, sid),
        out_shape=(
            jax.ShapeDtypeStruct((8, 128), F32),
            jax.ShapeDtypeStruct((D, code), BF16),
            jax.ShapeDtypeStruct((D, code), BF16),
        ),
        in_specs=[vm] * 4 + [sm] * 2,
        out_specs=(vm, vm, vm),
        scratch_shapes=[
            V((rows, code), BF16), V((rows, code), BF16),
            V((D, code), BF16), V((D, code), BF16),
            V((cols, code), BF16), V((cols, code), BF16),
            V((n_loop, D, code // n_loop), BF16), V((n_loop, D, code // n_loop), BF16),
            V((cols, rows), F32), V((cols, rows), F32), V((cols, rows), BF16),
            V((n_img, 8, rows), F32),
            V((n_lx * n_kh, D, code), BF16),
            V(((n_lx - 1) * n_kh, D, code), BF16),
            V((n_kh, D, code), BF16),
            V(((n_ly - 1) * n_kl, D, code), BF16),
            V((n_kl - 1, D, code), BF16),
            V((n_txt, 8, 128), F32),
            V((D, 128), F32), V((D, 128), F32),
            pltpu.SemaphoreType.DMA((sid.count,)),
            pltpu.SemaphoreType.DMA((rid.count,)),
        ],
        compiler_params=pltpu.CompilerParams(
            collective_id=0, has_side_effects=True, vmem_limit_bytes=67043328,
        ),
    )(si, st, ti, tt, ssc, tsc)
    return pl.pallas_call(
        emit,
        out_shape=(
            jax.ShapeDtypeStruct((1,), F32),
            jax.ShapeDtypeStruct((D, code), BF16),
            jax.ShapeDtypeStruct((D, code), BF16),
        ),
        in_specs=[vm] * 3,
        out_specs=(sm, vm, vm),
    )(loss, gi, gt)


def solution(mesh):
    return jax.shard_map(
        functools.partial(on_device, mesh.shape["row"], mesh.shape["loop"]),
        mesh=mesh,
        in_specs=(
            P(("row", "loop"), None),
            P(("row", "loop"), None),
            P("row", "loop"),
            P("row", "loop"),
            P(),
            P(),
        ),
        out_specs=(P(), P(("row", "loop"), None), P(("row", "loop"), None)),
        check_vma=False,
    )
```

```python
import functools
import jax
import jax.numpy as jnp
from jax import lax
from jax.experimental import pallas as pl
from jax.experimental.pallas import tpu as pltpu
from jax.sharding import PartitionSpec as P

EPS = 1e-06
F32 = jnp.float32
BF16 = jnp.bfloat16
MESH = pl.DeviceIdType.MESH
UNIT = 32
IMAGE_PART = 64
STEP = 32
DOT = 1280
TILE = 256


class Ids:
    def __init__(self):
        self.table = {}
        self.count = 0

    def take(self, name, size=1):
        self.table[name] = self.count
        self.count += size

    def __getitem__(self, name):
        return self.table[name]


def split(D, part):
    return [min(part, D - o) for o in range(0, D, part)]


def offsets(sizes):
    return [sum(sizes[:h]) for h in range(len(sizes))]


def back_sizes(D):
    units = D // UNIT
    if units < 4:
        return [UNIT] * units
    return [UNIT, D - 3 * UNIT, UNIT, UNIT]


def make_ids(D, n_kh, n_kl, n_lx, n_ly):
    HI, HT, HB = len(split(D, IMAGE_PART)), D // UNIT, len(back_sizes(D))
    recv, sent = Ids(), Ids()
    recv.take("t_img")
    recv.take("t_txt")
    for a in range(2):
        recv.take(("iz", a), n_kl * HI)
        recv.take(("iy", a), HI)
        recv.take(("tz", a), n_kh * HT)
        recv.take(("tx", a), n_lx * HT)
        recv.take(("tc", a), HT)
    recv.take("stat")
    recv.take("dc", n_lx * n_kh * HB)
    recv.take("dx", n_lx * n_kh * HB)
    recv.take("dz")
    recv.take("gy", n_kl * HB)
    recv.take("gz")
    recv.take("loss")
    recv.take("keep")
    for name in ("t_img", "t_txt", "stat", "dc", "dx", "dz", "gy", "gz", "loss"):
        sent.take(name)
    for a in range(2):
        for kind in ("img", "first", "txt"):
            sent.take((kind, a))
    return recv, sent


def kernel(
    dims, rid, sid,
    si, st, ti, tt, ssc, tsc,
    loss_out, gi_out, gt_out,
    img_s, img_t, own_s, own_t, txt_s, txt_t, raw_i, raw_t,
    slog, tlog, grad, stat, r1, r2, r3, ry, rz, part, inv_i, inv_t,
    ss, rs,
):
    n_row, n_loop, n_kh, n_kl, n_lx, n_ly, D, code = dims
    isz, tsz, bsz = split(D, IMAGE_PART), split(D, UNIT), back_sizes(D)
    ioff, toff, boff = offsets(isz), offsets(tsz), offsets(bsz)
    HI, HT, HB = len(isz), len(tsz), len(bsz)
    n_img = n_kl * n_ly
    n_txt = n_kh * n_lx * 2
    rows = n_img * D
    cols = n_txt * D
    r = lax.axis_index("row")
    l = lax.axis_index("loop")
    k, c = r // 2, r % 2
    kh, kl = k // n_kl, k % n_kl
    src_kl, src_j = k // n_kh, k % n_kh
    ly, lx = l // n_lx, l % n_lx
    sscale = ssc[0]
    tscale = tsc[0]

    def dev(k_=None, c_=None, ly_=None, lx_=None):
        kk = k if k_ is None else k_
        cc = c if c_ is None else c_
        yy = ly if ly_ is None else ly_
        xx = lx if lx_ is None else lx_
        return (kk * 2 + cc, yy * n_lx + xx)

    def islot(kl_, ly_):
        return ly_ * n_kl + kl_

    def tslot(j, lx_, c_):
        return (j * n_lx + lx_) * 2 + c_

    def span(start, size, step):
        return pl.ds(pl.multiple_of(start, step), size)

    def irng(h, slot):
        return span(n_img * ioff[h] + slot * isz[h], isz[h], UNIT)

    def trng(h, slot):
        return span(n_txt * toff[h] + slot * tsz[h], tsz[h], UNIT)

    def brng(slot, h):
        return span(slot * D + boff[h], bsz[h], UNIT)

    def at(slot):
        return span(slot * D, D, UNIT)

    part_of = [pl.ds(boff[h], bsz[h]) for h in range(HB)]

    def image_ref(a, kl_, ly_, h):
        if a == 0:
            return img_s.at[irng(h, islot(kl_, ly_)), :]
        return raw_i.at[kl_, ly_, :, pl.ds(n_ly * ioff[h], n_ly * isz[h]), :]

    def text_ref(a, j, lx_, h):
        if a == 0:
            return txt_s.at[trng(h, tslot(j, lx_, c)), :]
        return raw_t.at[j, lx_, :, pl.ds(n_lx * toff[h], n_lx * tsz[h]), :]

    def own_ref(a, h):
        if a == 0:
            return own_s.at[pl.ds(toff[h], tsz[h]), :]
        return own_t.at[:, pl.ds(n_lx * toff[h], n_lx * tsz[h]), :]

    def copy(src, dst, q_send, q_recv, device):
        return pltpu.make_async_remote_copy(
            src_ref=src, dst_ref=dst, send_sem=ss.at[q_send], recv_sem=rs.at[q_recv],
            device_id=device, device_id_type=MESH,
        )

    sent_rows = {}

    def send(src, dst, name, q, device, n=0):
        copy(src, dst, sid[name], q, device).start()
        sent_rows[name] = sent_rows.get(name, 0) + n

    def got(dst, q):
        copy(dst, dst, 0, q, dev(c_=1 - c)).wait_recv()

    def got_rows(n, q):
        got(txt_s.at[pl.ds(0, n), :], q)

    def left(ref, q):
        copy(ref, ref, q, 0, dev(c_=1 - c)).wait_send()

    def left_rows(*names):
        for name in names:
            left(txt_s.at[pl.ds(0, sent_rows.pop(name)), :], sid[name])

    loss_peers = [
        (kd, xd, cd) for kd in range(n_kh) for xd in range(n_lx) for cd in range(2) if kd or xd or cd
    ]

    def loss_peer(kd, xd, cd):
        return dev(k_=((kh + kd) % n_kh) * n_kl + kl, c_=(c + cd) % 2, lx_=(lx + xd) % n_lx)

    barrier = pltpu.get_barrier_semaphore()
    n_peer = 0
    for kd, xd, cd in loss_peers:
        if (kd != 0) + (xd != 0) + (cd != 0) > 1:
            pl.semaphore_signal(barrier, inc=1, device_id=loss_peer(kd, xd, cd), device_id_type=MESH)
            n_peer += 1
    for e in range(1, n_ly):
        pl.semaphore_signal(barrier, inc=1, device_id=dev(ly_=(ly + e) % n_ly), device_id_type=MESH)
        n_peer += 1
    for e in range(1, n_lx):
        pl.semaphore_signal(barrier, inc=1, device_id=dev(lx_=(lx + e) % n_lx), device_id_type=MESH)
        n_peer += 1
    for d in range(1, n_kh * n_kl):
        pl.semaphore_signal(barrier, inc=1, device_id=dev(k_=(k + d) % (n_kh * n_kl)), device_id_type=MESH)
        n_peer += 1
    pl.semaphore_signal(barrier, inc=1, device_id=dev(c_=1 - c), device_id_type=MESH)
    n_peer += 1
    for d in range(1, n_kl):
        for e in range(1, n_ly):
            diagonal = dev(k_=kh * n_kl + (kl + d) % n_kl, ly_=(ly + e) % n_ly)
            pl.semaphore_signal(barrier, inc=1, device_id=diagonal, device_id_type=MESH)
            n_peer += 1

    def unit(load, dst, first, n, keep=None):
        for o in range(0, n, UNIT):
            x = load(o)
            n2 = jnp.sum(x * x, axis=1, keepdims=True) + EPS
            inv = 1.0 / jnp.sqrt(n2)
            if keep is not None:
                keep(o, inv)
            dst[span(first + o, UNIT, UNIT), :] = (x * inv).astype(BF16)

    def student_unit(src, dst, first, o0, n, inv_ref):
        def load(o):
            return src[pl.ds(o0 + o, UNIT), :].astype(F32)

        def keep(o, inv):
            inv_ref[pl.ds(o0 + o, UNIT), :] = jnp.broadcast_to(inv, (UNIT, 128))
        unit(load, dst, first, n, keep)

    def own_text(h):
        student_unit(st, own_s, toff[h], toff[h], tsz[h], inv_t)

    def own_image(h):
        student_unit(si, img_s, n_img * ioff[h] + islot(kl, ly) * isz[h], ioff[h], isz[h], inv_i)

    def teacher_keep():
        for h in range(HI):
            for y_ in range(n_ly):
                dst = pl.ds(n_ly * ioff[h] + y_ * isz[h], isz[h])
                src = span((y_ * n_lx + lx) * D + ioff[h], isz[h], UNIT)
                pltpu.make_async_copy(ti.at[src, :], raw_i.at[kl, ly, lx, dst, :], rs.at[rid["keep"]]).start()
        for h in range(HT):
            for x_ in range(n_lx):
                dst = pl.ds(n_lx * toff[h] + x_ * tsz[h], tsz[h])
                src = span((ly * n_lx + x_) * D + toff[h], tsz[h], UNIT)
                pltpu.make_async_copy(tt.at[src, :], own_t.at[ly, dst, :], rs.at[rid["keep"]]).start()

    def teacher_kept():
        both = txt_s.at[pl.ds(0, D * (n_ly + n_lx) // n_loop), :]
        pltpu.make_async_copy(both, both, rs.at[rid["keep"]]).wait()

    teacher_keep()
    own_text(0)
    own_image(0)
    pl.semaphore_wait(barrier, n_peer)

    def teacher_exchange():
        for h in range(HI):
            for y_ in range(n_ly):
                dst = pl.ds(n_ly * ioff[h] + y_ * isz[h], isz[h])
                for e in range(1, n_lx):
                    x_ = (lx + e) % n_lx
                    src = span((y_ * n_lx + x_) * D + ioff[h], isz[h], UNIT)
                    send(ti.at[src, :], raw_i.at[kl, ly, lx, dst, :], "t_img", rid["t_img"], dev(lx_=x_))
        for h in range(HT):
            for x_ in range(n_lx):
                dst = pl.ds(n_lx * toff[h] + x_ * tsz[h], tsz[h])
                for e in range(1, n_ly):
                    y_ = (ly + e) % n_ly
                    src = span((y_ * n_lx + x_) * D + toff[h], tsz[h], UNIT)
                    send(tt.at[src, :], own_t.at[ly, dst, :], "t_txt", rid["t_txt"], dev(ly_=y_))

    moved_i = raw_i.at[0, 0, pl.ds(0, n_lx - 1)]
    moved_t = own_t.at[pl.ds(0, n_ly - 1)]

    def image_z(a, h):
        ref = image_ref(a, kl, ly, h)
        for d in range(1, n_kl):
            q = rid[("iz", a)] + d * HI + h
            send(ref, ref, ("img", a), q, dev(k_=kh * n_kl + (kl + d) % n_kl), isz[h])

    def image_y(a, h):
        ref = image_ref(a, kl, ly, h)
        for e in range(1, n_ly):
            send(ref, ref, ("img", a), rid[("iy", a)] + h, dev(ly_=(ly + e) % n_ly), isz[h])

    def image_relay(a, h):
        for d in range(1, n_kl):
            ref = image_ref(a, (kl + n_kl - d) % n_kl, ly, h)
            got(ref, rid[("iz", a)] + d * HI + h)
            for e in range(1, n_ly):
                send(ref, ref, ("img", a), rid[("iy", a)] + h, dev(ly_=(ly + e) % n_ly), isz[h])

    def image_finish(a, h):
        got_rows((n_ly - 1) * n_kl * isz[h], rid[("iy", a)] + h)
        if a == 0:
            return
        for p in range(n_kl):
            for y_ in range(n_ly):
                def load(o):
                    rng = pl.ds(n_ly * ioff[h] + y_ * isz[h] + o, UNIT)
                    xs = [raw_i[p, fy, fx, rng, :] for fy in range(n_ly) for fx in range(n_lx)]
                    return jnp.concatenate(xs, axis=1).astype(F32)
                unit(load, img_t, n_img * ioff[h] + islot(p, y_) * isz[h], isz[h])

    def text_first(a, h):
        src = own_ref(a, h)
        for g in range(n_kh):
            dest = g * n_kl + src_kl
            op = copy(src, text_ref(a, src_j, lx, h), sid[("first", a)],
                      rid[("tz", a)] + src_j * HT + h, dev(k_=dest))

            @pl.when(dest != k)
            def _():
                op.start()

            @pl.when(dest == k)
            def _():
                if a == 0:
                    txt_s[trng(h, tslot(src_j, lx, c)), :] = own_s[pl.ds(toff[h], tsz[h]), :]
                else:
                    rng = pl.ds(n_lx * toff[h], n_lx * tsz[h])
                    raw_t[src_j, lx, :, rng, :] = own_t[:, rng, :]

    def first_left(a):
        @pl.when(src_kl == kl)
        def _():
            left(txt_s.at[pl.ds(0, (n_kh - 1) * D), :], sid[("first", a)])

        @pl.when(src_kl != kl)
        def _():
            left(txt_s.at[pl.ds(0, n_kh * D), :], sid[("first", a)])

    def core_send(a, ref, h):
        send(ref, ref, ("txt", a), rid[("tc", a)] + h, dev(c_=1 - c), tsz[h])

    def text_relay(a, h):
        for j in range(n_kh):
            ref = text_ref(a, j, lx, h)

            @pl.when(kl * n_kh + j != k)
            def _():
                got(ref, rid[("tz", a)] + j * HT + h)

            for e in range(1, n_lx):
                send(ref, ref, ("txt", a), rid[("tx", a)] + e * HT + h, dev(lx_=(lx + e) % n_lx), tsz[h])
            if a == 0:
                core_send(a, ref, h)

    def text_cross(a, h):
        for e in range(1, n_lx):
            got_rows(n_kh * tsz[h], rid[("tx", a)] + e * HT + h)
            for j in range(n_kh):
                if a == 0:
                    core_send(a, text_ref(a, j, (lx + n_lx - e) % n_lx, h), h)
        if a == 0:
            return
        for j in range(n_kh):
            for x_ in range(n_lx):
                def load(o):
                    rng = pl.ds(n_lx * toff[h] + x_ * tsz[h] + o, UNIT)
                    xs = [raw_t[j, fx, fy, rng, :] for fy in range(n_ly) for fx in range(n_lx)]
                    return jnp.concatenate(xs, axis=1).astype(F32)
                unit(load, txt_t, n_txt * toff[h] + tslot(j, x_, c) * tsz[h], tsz[h])
                core_send(a, txt_t.at[trng(h, tslot(j, x_, c)), :], h)

    def text_finish(a, h):
        got_rows(n_lx * n_kh * tsz[h], rid[("tc", a)] + h)

    def tile_of(n, most):
        return max(t for t in range(UNIT, min(n, most) + 1, UNIT) if n % t == 0)

    def logits(txt, img, scale, out, row0, n):
        tile = tile_of(n, TILE)
        m = jnp.full((8, rows), -jnp.inf, F32)
        for o in range(row0, row0 + n, tile):
            v = scale * lax.dot_general(
                txt[pl.ds(o, tile), :], img[...], (((1,), (1,)), ((), ())),
                preferred_element_type=F32,
            )
            out[pl.ds(o, tile), :] = v
            m = jnp.maximum(m, jnp.max(v.reshape(tile // 8, 8, rows), axis=0))
        return jnp.max(m, axis=0, keepdims=True)

    def zipped(image_step, text_step):
        for h in range(max(HI, HT)):
            if h < HT:
                text_step(h)
            if h < HI:
                image_step(h)

    teacher_exchange()

    def student_text(h):
        if h:
            own_text(h)
        text_first(0, h)

    def student_image(h):
        if h:
            own_image(h)
        image_z(0, h)
        image_y(0, h)
    zipped(student_image, student_text)
    text_relay(0, 0)
    image_relay(0, 0)
    teacher_kept()
    got(moved_i, rid["t_img"])
    got(moved_t, rid["t_txt"])
    ahead = min(3, HT)
    for h in range(ahead):
        text_first(1, h)
    for h in range(max(HI, HT - ahead)):
        if h < HI:
            image_z(1, h)
        if ahead + h < HT:
            text_first(1, ahead + h)
    relay_s = [functools.partial(text_relay, 0, h) for h in range(1, HT)]
    relay_t = [functools.partial(text_relay, 1, h) for h in range(HT)]
    image_s = [functools.partial(image_relay, 0, h) for h in range(1, HI)]
    image_t = [functools.partial(image_relay, 1, h) for h in range(HI)]
    cross_s = [functools.partial(text_cross, 0, h) for h in range(HT)]
    cross_t = [functools.partial(text_cross, 1, h) for h in range(HT)]
    finish_t = [functools.partial(image_finish, 1, h) for h in range(HI)]

    def step(*queues):
        for queue in queues:
            if queue:
                queue.pop(0)()

    step(relay_s)
    while relay_s:
        step(image_s, relay_s, cross_s)
    while image_s:
        step(image_s)
    for h in range(HI):
        image_y(1, h)
    while len(cross_s) > 2:
        step(cross_s)
    step(relay_t)
    step(cross_s, cross_s)
    step(relay_t)
    while cross_s:
        step(cross_s)
    for h in range(HI):
        image_finish(0, h)
    for h in range(HT):
        text_finish(0, h)
    step(image_t)
    step(relay_t)
    smax = logits(txt_s, img_s, sscale, slog, 0, cols)
    step(cross_t)
    step(relay_t)
    step(image_t)
    step(cross_t)
    while len(image_t) > 0:
        step(image_t)
    while relay_t:
        step(relay_t)
    while len(cross_t) > 2:
        step(cross_t)
    step(finish_t)
    step(cross_t)
    while finish_t:
        step(finish_t)
    def exps(row0, n, top_t):
        def fold(v):
            return jnp.sum(v.reshape(STEP // 8, 8, rows), axis=0)

        def body(i, carry):
            a, b, x = carry
            o = pl.multiple_of(row0 + i * STEP, STEP)
            s = slog[pl.ds(o, STEP), :]
            t = tlog[pl.ds(o, STEP), :]
            es = jnp.exp(s - smax)
            et = jnp.exp(t - top_t)
            slog[pl.ds(o, STEP), :] = es
            tlog[pl.ds(o, STEP), :] = et
            return (a + fold(es), b + fold(et), x + fold(et * (t - s)))
        zero = jnp.zeros((8, rows), F32)
        return lax.fori_loop(0, n // STEP, body, (zero, zero, zero))

    row0 = [n_txt * o for o in toff]
    height = [n_txt * n for n in tsz]
    tops = []
    sums = []

    def teacher(h0, h1):
        for h in range(h0, h1):
            text_finish(1, h)
        n = sum(height[h0:h1])
        top = logits(txt_t, img_t, tscale, tlog, row0[h0], n)
        if h0 == 0:
            while cross_t:
                step(cross_t)
        tops.append(top)
        tops_at.extend([top] * (h1 - h0))
        sums.append([jnp.sum(v, axis=0, keepdims=True) for v in exps(row0[h0], n, top)])

    tops_at = []
    cuts = sorted({0, max(HT - 2, 0), HT - 1, HT})
    for h0, h1 in zip(cuts, cuts[1:]):
        teacher(h0, h1)

    tmax = functools.reduce(jnp.maximum, tops)
    shift = [jnp.exp(m - tmax) for m in tops]
    asum = sum(v[0] for v in sums)
    bsum = sum(v[1] * e for v, e in zip(sums, shift))
    xsum = sum(v[2] * e for v, e in zip(sums, shift))
    pack = [smax, tmax, asum, bsum, xsum]
    stat[islot(kl, ly)] = jnp.concatenate(pack + [jnp.zeros((3, rows), F32)], axis=0)
    for d in range(n_kl):
        for e in range(n_ly):
            if d or e:
                send(stat.at[islot(kl, ly)], stat.at[islot(kl, ly)], "stat", rid["stat"],
                     dev(k_=kh * n_kl + (kl + d) % n_kl, ly_=(ly + e) % n_ly))
    for a in range(2):
        first_left(a)
        left_rows(("img", a), ("txt", a))
    got(stat.at[pl.ds(0, n_img - 1)], rid["stat"])

    all_stat = [stat[s] for s in range(n_img)]
    gs = functools.reduce(jnp.maximum, [v[0:1] for v in all_stat])
    gt = functools.reduce(jnp.maximum, [v[1:2] for v in all_stat])
    es = [jnp.exp(v[0:1] - gs) for v in all_stat]
    et = [jnp.exp(v[1:2] - gt) for v in all_stat]
    ssum = sum(v[2:3] * e for v, e in zip(all_stat, es))
    tsum = sum(v[3:4] * e for v, e in zip(all_stat, et))
    cross = sum(v[4:5] * e for v, e in zip(all_stat, et))
    diverge = cross / tsum - (gt + jnp.log(tsum)) + (gs + jnp.log(ssum))
    mine = tslot(kh, lx, c)
    part[mine] = jnp.broadcast_to(jnp.sum(diverge, axis=1, keepdims=True), (8, 128))
    for peer in loss_peers:
        send(part.at[mine], part.at[mine], "loss", rid["loss"], loss_peer(*peer))

    s_mul = sscale * jnp.exp(smax - gs) / ssum
    t_scale = sscale / tsum

    t_mul = [t_scale * jnp.exp(m - gt) for m in tops_at]

    dtxt = txt_t

    def grad_of(rng, h):
        v = (slog[rng, :] * s_mul - tlog[rng, :] * t_mul[h]).astype(BF16)
        grad[rng, :] = v
        return v

    def text_piece(j, lx_, c_, fresh=False):
        slot = tslot(j, lx_, c_)
        if fresh:
            g = [grad_of(trng(h, slot), h) for h in range(HT)]
        else:
            g = [grad[trng(h, slot), :] for h in range(HT)]
        v = jnp.dot(jnp.concatenate(g, axis=0), img_s[...], preferred_element_type=F32)
        dtxt[at(slot), :] = v.astype(BF16)

    order = [(n_kh - 1 - kh + i) % n_kh for i in range(n_kh)]

    def to_core(e, i, fresh=False):
        x_ = (lx + e) % n_lx
        j = order[i]
        text_piece(j, x_, 1 - c, fresh)
        for h in range(HB):
            send(dtxt.at[brng(tslot(j, x_, 1 - c), h), :], r1.at[x_ * n_kh + j, part_of[h], :], "dc",
                 rid["dc"] + (e * n_kh + i) * HB + h, dev(c_=1 - c), bsz[h])

    def from_core(e, i, h):
        s = ((lx + e) % n_lx) * n_kh + order[i]
        got(r1.at[s, part_of[h], :], rid["dc"] + (e * n_kh + i) * HB + h)
        return r1[s, part_of[h], :].astype(F32)

    def to_x(e, i):
        x_ = (lx + e) % n_lx
        j = order[i]
        for h in range(HB):
            rng = brng(tslot(j, x_, c), h)
            dtxt[rng, :] = (dtxt[rng, :].astype(F32) + from_core(e, i, h)).astype(BF16)
            q = rid["dx"] + (e * n_kh + i) * HB + h
            send(dtxt.at[rng, :], r2.at[(e - 1) * n_kh + j, part_of[h], :], "dx", q, dev(lx_=x_), bsz[h])

    dimg = img_t
    full = [h for h in range(HI) if (n_kl * isz[h]) % 128 == 0]
    rest = [h for h in range(HI) if h not in full]

    def image_piece(y_, with_rest):
        windows = [span(n_img * ioff[h] + y_ * n_kl * isz[h], n_kl * isz[h], 128) for h in full]
        if with_rest:
            windows += [pl.ds(n_img * ioff[h], n_img * isz[h]) for h in rest]
        tile = tile_of(cols, DOT)
        wide = code if tile == cols else code // 2
        for n0 in range(0, code, wide):
            out = pl.ds(n0, wide)
            v = 0.0
            for o in range(0, cols, tile):
                g = jnp.concatenate([grad[pl.ds(o, tile), w] for w in windows], axis=1)
                v = v + lax.dot_general(
                    g, txt_s[pl.ds(o, tile), out], (((0,), (0,)), ((), ())), preferred_element_type=F32,
                )
            v = v.astype(BF16)
            slots = [(islot(p, y_), h) for h in full for p in range(n_kl)]
            if with_rest:
                slots += [(s, h) for h in rest for s in range(n_img)]
            o = 0
            for s, h in slots:
                dimg[span(s * D + ioff[h], isz[h], UNIT), out] = v[o:o + isz[h]]
                o += isz[h]

    def to_y(e):
        y_ = (ly + e) % n_ly
        image_piece(y_, e == 1)
        for d in [*range(1, n_kl), 0]:
            for h in range(HB):
                q = rid["gy"] + d * HB + h
                send(dimg.at[brng(islot((kl + d) % n_kl, y_), h), :], ry.at[(e - 1) * n_kl + d, part_of[h], :],
                     "gy", q, dev(ly_=y_), bsz[h])

    x1 = (lx + 1) % n_lx
    to_core(1, 0, True)
    text_piece(order[0], x1, c, True)
    for h in range(HT):
        def to_grad(i, _):
            grad_of(span(row0[h] + i * STEP, STEP, STEP), h)
            return 0
        lax.fori_loop(0, height[h] // STEP, to_grad, 0, unroll=2)
    to_x(1, 0)
    to_core(0, 0)
    text_piece(order[0], lx, c)
    for e in range(1, n_ly):
        to_y(e)

    def owner_copy(i, h):
        j = order[i]
        dest = kl * n_kh + j
        op = copy(dtxt.at[brng(tslot(j, lx, c), h), :], r3.at[kh, part_of[h], :], sid["dz"], rid["dz"], dev(k_=dest))
        return dest, op

    def text_sum(i, h):
        j = order[i]
        rng = brng(tslot(j, lx, c), h)
        v = dtxt[rng, :].astype(F32) + from_core(0, i, h)
        for e in range(1, n_lx):
            got(r2.at[(e - 1) * n_kh + j, part_of[h], :], rid["dx"] + (e * n_kh + i) * HB + h)
            v = v + r2[(e - 1) * n_kh + j, part_of[h], :].astype(F32)
        dtxt[rng, :] = v.astype(BF16)
        dest, op = owner_copy(i, h)

        @pl.when(dest != k)
        def _():
            op.start()

        @pl.when(dest == k)
        def _():
            r3[kh, part_of[h], :] = dtxt[rng, :]

    def got_y(d, h):
        got_rows((n_ly - 1) * bsz[h], rid["gy"] + d * HB + h)

    def image_sum(d, h):
        got_y(d, h)
        rng = brng(islot((kl + d) % n_kl, ly), h)
        v = dimg[rng, :].astype(F32)
        for e in range(1, n_ly):
            v = v + ry[(e - 1) * n_kl + d, part_of[h], :].astype(F32)
        dimg[rng, :] = v.astype(BF16)
        send(dimg.at[rng, :], rz.at[d - 1, part_of[h], :], "gz", rid["gz"], dev(k_=kh * n_kl + (kl + d) % n_kl), bsz[h])

    text_sum(0, 0)
    for e in range(1, n_lx):
        for i in range(1 if e == 1 else 0, n_kh):
            to_core(e, i)
            text_piece(order[i], (lx + e) % n_lx, c)
            if e > 1 or i > 1:
                to_x(e, i)
    image_piece(ly, n_ly == 1)
    if n_kh > 1:
        to_x(1, 1)
    texts = [(i, h) for i in range(n_kh) for h in range(HB)][1:]
    images = [(d, h) for d in range(1, n_kl) for h in range(HB)]
    while texts or images:
        if texts:
            i, h = texts.pop(0)
            if h == HB - 1 and i + 1 < n_kh:
                to_core(0, i + 1)
                text_piece(order[i + 1], lx, c)
            text_sum(i, h)
        if images:
            image_sum(*images.pop(0))
    got(part.at[pl.ds(0, len(loss_peers))], rid["loss"])
    loss_out[...] = sum(part[i] for i in range(n_txt)) / float(D * n_row * n_loop)

    def finish(terms, src, inv_ref, out):
        for o in range(0, D, UNIT):
            rng = pl.ds(o, UNIT)
            g = terms(o)
            x = src[rng, :].astype(F32)
            inv = inv_ref[rng, 0:1]
            along = jnp.sum(g * x, axis=1, keepdims=True) * inv * inv
            out[rng, :] = ((g - x * along) * inv).astype(BF16)

    for h in range(HB):
        got_y(0, h)
    got_rows((n_kl - 1) * D, rid["gz"])

    def image_terms(o):
        v = dimg[span(islot(kl, ly) * D + o, UNIT, UNIT), :].astype(F32)
        for e in range(1, n_ly):
            v = v + ry[(e - 1) * n_kl, pl.ds(o, UNIT), :].astype(F32)
        for d in range(1, n_kl):
            v = v + rz[d - 1, pl.ds(o, UNIT), :].astype(F32)
        return v
    finish(image_terms, si, inv_i, gi_out)

    def on_owner(wait):
        @pl.when(src_kl == kl)
        def _():
            wait(n_kh - 1)

        @pl.when(src_kl != kl)
        def _():
            wait(n_kh)
    on_owner(lambda n: got(txt_s.at[pl.ds(0, n * D), :], rid["dz"]))
    finish(lambda o: sum(r3[g, pl.ds(o, UNIT), :].astype(F32) for g in range(n_kh)), st, inv_t, gt_out)

    left(moved_i, sid["t_img"])
    left(moved_t, sid["t_txt"])
    left(stat.at[pl.ds(0, n_img - 1)], sid["stat"])
    left_rows("dc", "dx", "gy", "gz")
    left(part.at[pl.ds(0, len(loss_peers))], sid["loss"])

    on_owner(lambda n: left(txt_s.at[pl.ds(0, n * D), :], sid["dz"]))


def emit(total, gi, gt, loss_out, gi_out, gt_out):
    loss_out[0] = total[0, 0]
    gi_out[...] = gi[...]
    gt_out[...] = gt[...]


def on_device(n_row, n_loop, si, st, ti, tt, ssc, tsc):
    D, code = si.shape
    n_kl, n_lx = 2, 2
    n_kh, n_ly = n_row // (2 * n_kl), n_loop // n_lx
    n_img, n_txt = n_kl * n_ly, n_kh * n_lx * 2
    rows, cols = n_img * D, n_txt * D
    feat = code // n_loop
    rid, sid = make_ids(D, n_kh, n_kl, n_lx, n_ly)
    dims = (n_row, n_loop, n_kh, n_kl, n_lx, n_ly, D, code)
    vm = pl.BlockSpec(memory_space=pltpu.VMEM)
    sm = pl.BlockSpec(memory_space=pltpu.SMEM)
    anywhere = pl.BlockSpec(memory_space=pl.ANY)
    V = pltpu.VMEM
    loss, gi, gt = pl.pallas_call(
        functools.partial(kernel, dims, rid, sid),
        out_shape=(
            jax.ShapeDtypeStruct((8, 128), F32),
            jax.ShapeDtypeStruct((D, code), BF16),
            jax.ShapeDtypeStruct((D, code), BF16),
        ),
        in_specs=[vm, vm, anywhere, anywhere, sm, sm],
        out_specs=(vm, vm, vm),
        scratch_shapes=[
            V((rows, code), BF16), V((rows, code), BF16),
            V((D, code), BF16), V((n_ly, n_lx * D, feat), BF16),
            V((cols, code), BF16), V((cols, code), BF16),
            V((n_kl, n_ly, n_lx, n_ly * D, feat), BF16),
            V((n_kh, n_lx, n_ly, n_lx * D, feat), BF16),
            V((cols, rows), F32), V((cols, rows), F32), V((cols, rows), BF16),
            V((n_img, 8, rows), F32),
            V((n_lx * n_kh, D, code), BF16),
            V(((n_lx - 1) * n_kh, D, code), BF16),
            V((n_kh, D, code), BF16),
            V(((n_ly - 1) * n_kl, D, code), BF16),
            V((n_kl - 1, D, code), BF16),
            V((n_txt, 8, 128), F32),
            V((D, 128), F32), V((D, 128), F32),
            pltpu.SemaphoreType.DMA((sid.count,)),
            pltpu.SemaphoreType.DMA((rid.count,)),
        ],
        compiler_params=pltpu.CompilerParams(
            collective_id=0, has_side_effects=True, vmem_limit_bytes=67043328,
        ),
    )(si, st, ti, tt, ssc, tsc)
    return pl.pallas_call(
        emit,
        out_shape=(
            jax.ShapeDtypeStruct((1,), F32),
            jax.ShapeDtypeStruct((D, code), BF16),
            jax.ShapeDtypeStruct((D, code), BF16),
        ),
        in_specs=[vm] * 3,
        out_specs=(sm, vm, vm),
    )(loss, gi, gt)


def solution(mesh):
    return jax.shard_map(
        functools.partial(on_device, mesh.shape["row"], mesh.shape["loop"]),
        mesh=mesh,
        in_specs=(
            P(("row", "loop"), None),
            P(("row", "loop"), None),
            P("row", "loop"),
            P("row", "loop"),
            P(),
            P(),
        ),
        out_specs=(P(), P(("row", "loop"), None), P(("row", "loop"), None)),
        check_vma=False,
    )
```

```python
import functools
import jax
import jax.numpy as jnp
from jax import lax
from jax.experimental import pallas as pl
from jax.experimental.pallas import tpu as pltpu
from jax.sharding import PartitionSpec as P

EPS = 1e-06
F32 = jnp.float32
BF16 = jnp.bfloat16
MESH = pl.DeviceIdType.MESH
UNIT = 32
IMAGE_PART = 64
STEP = 32
DOT = 1280
TILE = 256


class Ids:
    def __init__(self):
        self.table = {}
        self.count = 0

    def take(self, name, size=1):
        self.table[name] = self.count
        self.count += size

    def __getitem__(self, name):
        return self.table[name]


def split(D, part):
    return [min(part, D - o) for o in range(0, D, part)]


def offsets(sizes):
    return [sum(sizes[:h]) for h in range(len(sizes))]


def back_sizes(D):
    units = D // UNIT
    if units < 4:
        return [UNIT] * units
    return [UNIT, D - 3 * UNIT, UNIT, UNIT]


def make_ids(D, n_kh, n_kl, n_lx, n_ly):
    HI, HT, HB = len(split(D, IMAGE_PART)), D // UNIT, len(back_sizes(D))
    recv, sent = Ids(), Ids()
    recv.take("t_img")
    recv.take("t_txt")
    for a in range(2):
        recv.take(("iz", a), (n_kl - 1) * HI)
        recv.take(("iy", a), HI)
        recv.take(("tz", a), n_kh * HT)
        recv.take(("tx", a), (n_lx - 1) * HT)
        recv.take(("tc", a), HT)
    recv.take("stat")
    recv.take("dc", n_lx * n_kh - 1 + HB)
    recv.take("dx", (n_lx - 1) * n_kh * HB)
    recv.take("dz")
    recv.take("gy", n_kl * HB)
    recv.take("gz")
    recv.take("loss")
    recv.take("keep")
    recv.take("load", 2)
    for name in ("t_img", "t_txt", "stat", "dc", "dx", "dz", "gy", "gz", "loss"):
        sent.take(name)
    for a in range(2):
        for kind in ("img", "first", "txt"):
            sent.take((kind, a))
    return recv, sent


def kernel(
    dims, rid, sid,
    si_in, st_in, ti, tt, ssc, tsc,
    loss_out, gi_out, gt_out,
    img_s, img_t, own_s, own_t, txt_s, txt_t, raw_i, raw_t,
    slog, tlog, grad, stat, r1, r2, r3, ry, rz, part, inv_i, inv_t, si, st,
    ss, rs,
):
    n_row, n_loop, n_kh, n_kl, n_lx, n_ly, D, code = dims
    isz, tsz, bsz = split(D, IMAGE_PART), split(D, UNIT), back_sizes(D)
    ioff, toff, boff = offsets(isz), offsets(tsz), offsets(bsz)
    HI, HT, HB = len(isz), len(tsz), len(bsz)
    n_img = n_kl * n_ly
    n_txt = n_kh * n_lx * 2
    rows = n_img * D
    cols = n_txt * D
    r = lax.axis_index("row")
    l = lax.axis_index("loop")
    k, c = r // 2, r % 2
    kh, kl = k // n_kl, k % n_kl
    src_kl, src_j = k // n_kh, k % n_kh
    ly, lx = l // n_lx, l % n_lx
    sscale = ssc[0]
    tscale = tsc[0]

    def dev(k_=None, c_=None, ly_=None, lx_=None):
        kk = k if k_ is None else k_
        cc = c if c_ is None else c_
        yy = ly if ly_ is None else ly_
        xx = lx if lx_ is None else lx_
        return (kk * 2 + cc, yy * n_lx + xx)

    def islot(kl_, ly_):
        return ly_ * n_kl + kl_

    def tslot(j, lx_, c_):
        return (j * n_lx + lx_) * 2 + c_

    def span(start, size, step):
        return pl.ds(pl.multiple_of(start, step), size)

    def irng(h, slot):
        return span(n_img * ioff[h] + slot * isz[h], isz[h], UNIT)

    def trng(h, slot):
        return span(n_txt * toff[h] + slot * tsz[h], tsz[h], UNIT)

    def brng(slot, h):
        return span(slot * D + boff[h], bsz[h], UNIT)

    def at(slot):
        return span(slot * D, D, UNIT)

    part_of = [pl.ds(boff[h], bsz[h]) for h in range(HB)]

    def image_ref(a, kl_, ly_, h):
        if a == 0:
            return img_s.at[irng(h, islot(kl_, ly_)), :]
        return raw_i.at[kl_, ly_, :, pl.ds(n_ly * ioff[h], n_ly * isz[h]), :]

    def text_ref(a, j, lx_, h):
        if a == 0:
            return txt_s.at[trng(h, tslot(j, lx_, c)), :]
        return raw_t.at[j, lx_, :, pl.ds(n_lx * toff[h], n_lx * tsz[h]), :]

    def own_ref(a, h):
        if a == 0:
            return own_s.at[pl.ds(toff[h], tsz[h]), :]
        return own_t.at[:, pl.ds(n_lx * toff[h], n_lx * tsz[h]), :]

    def copy(src, dst, q_send, q_recv, device):
        return pltpu.make_async_remote_copy(
            src_ref=src, dst_ref=dst, send_sem=ss.at[q_send], recv_sem=rs.at[q_recv],
            device_id=device, device_id_type=MESH,
        )

    sent_rows = {}

    def send(src, dst, name, q, device, n=0):
        copy(src, dst, sid[name], q, device).start()
        sent_rows[name] = sent_rows.get(name, 0) + n

    def got(dst, q):
        copy(dst, dst, 0, q, dev(c_=1 - c)).wait_recv()

    def got_rows(n, q):
        got(txt_s.at[pl.ds(0, n), :], q)

    def left(ref, q):
        copy(ref, ref, q, 0, dev(c_=1 - c)).wait_send()

    def left_rows(*names):
        for name in names:
            left(txt_s.at[pl.ds(0, sent_rows.pop(name)), :], sid[name])

    loss_peers = [
        (kd, xd, cd) for kd in range(n_kh) for xd in range(n_lx) for cd in range(2) if kd or xd or cd
    ]

    def loss_peer(kd, xd, cd):
        return dev(k_=((kh + kd) % n_kh) * n_kl + kl, c_=(c + cd) % 2, lx_=(lx + xd) % n_lx)

    barrier = pltpu.get_barrier_semaphore()
    n_peer = 0
    for kd, xd, cd in loss_peers:
        if (kd != 0) + (xd != 0) + (cd != 0) > 1:
            pl.semaphore_signal(barrier, inc=1, device_id=loss_peer(kd, xd, cd), device_id_type=MESH)
            n_peer += 1
    for e in range(1, n_ly):
        pl.semaphore_signal(barrier, inc=1, device_id=dev(ly_=(ly + e) % n_ly), device_id_type=MESH)
        n_peer += 1
    for e in range(1, n_lx):
        pl.semaphore_signal(barrier, inc=1, device_id=dev(lx_=(lx + e) % n_lx), device_id_type=MESH)
        n_peer += 1
    for d in range(1, n_kh * n_kl):
        pl.semaphore_signal(barrier, inc=1, device_id=dev(k_=(k + d) % (n_kh * n_kl)), device_id_type=MESH)
        n_peer += 1
    pl.semaphore_signal(barrier, inc=1, device_id=dev(c_=1 - c), device_id_type=MESH)
    n_peer += 1
    for d in range(1, n_kl):
        for e in range(1, n_ly):
            diagonal = dev(k_=kh * n_kl + (kl + d) % n_kl, ly_=(ly + e) % n_ly)
            pl.semaphore_signal(barrier, inc=1, device_id=diagonal, device_id_type=MESH)
            n_peer += 1

    def unit(load, dst, first, n, keep=None):
        for o in range(0, n, UNIT):
            x = load(o)
            n2 = jnp.sum(x * x, axis=1, keepdims=True) + EPS
            inv = 1.0 / jnp.sqrt(n2)
            if keep is not None:
                keep(o, inv)
            dst[span(first + o, UNIT, UNIT), :] = (x * inv).astype(BF16)

    def student_unit(src, dst, first, o0, n, inv_ref):
        def load(o):
            return src[pl.ds(o0 + o, UNIT), :].astype(F32)

        def keep(o, inv):
            inv_ref[pl.ds(o0 + o, UNIT), :] = jnp.broadcast_to(inv, (UNIT, 128))
        unit(load, dst, first, n, keep)

    def own_text(h):
        student_unit(st, own_s, toff[h], toff[h], tsz[h], inv_t)

    def own_image(h):
        student_unit(si, img_s, n_img * ioff[h] + islot(kl, ly) * isz[h], ioff[h], isz[h], inv_i)

    def teacher_keep():
        for h in range(HI):
            for y_ in range(n_ly):
                dst = pl.ds(n_ly * ioff[h] + y_ * isz[h], isz[h])
                src = span((y_ * n_lx + lx) * D + ioff[h], isz[h], UNIT)
                pltpu.make_async_copy(ti.at[src, :], raw_i.at[kl, ly, lx, dst, :], rs.at[rid["keep"]]).start()
        for h in range(HT):
            for x_ in range(n_lx):
                dst = pl.ds(n_lx * toff[h] + x_ * tsz[h], tsz[h])
                src = span((ly * n_lx + x_) * D + toff[h], tsz[h], UNIT)
                pltpu.make_async_copy(tt.at[src, :], own_t.at[ly, dst, :], rs.at[rid["keep"]]).start()

    def teacher_kept():
        both = txt_s.at[pl.ds(0, D * (n_ly + n_lx) // n_loop), :]
        pltpu.make_async_copy(both, both, rs.at[rid["keep"]]).wait()

    load_t = pltpu.make_async_copy(st_in, st, rs.at[rid["load"]])
    load_i = pltpu.make_async_copy(si_in, si, rs.at[rid["load"] + 1])
    load_t.start()
    load_i.start()
    teacher_keep()
    load_t.wait()
    own_text(0)
    load_i.wait()
    own_image(0)
    pl.semaphore_wait(barrier, n_peer)

    def teacher_exchange():
        for h in range(HI):
            for y_ in range(n_ly):
                dst = pl.ds(n_ly * ioff[h] + y_ * isz[h], isz[h])
                for e in range(1, n_lx):
                    x_ = (lx + e) % n_lx
                    src = span((y_ * n_lx + x_) * D + ioff[h], isz[h], UNIT)
                    send(ti.at[src, :], raw_i.at[kl, ly, lx, dst, :], "t_img", rid["t_img"], dev(lx_=x_))
        for h in range(HT):
            for x_ in range(n_lx):
                dst = pl.ds(n_lx * toff[h] + x_ * tsz[h], tsz[h])
                for e in range(1, n_ly):
                    y_ = (ly + e) % n_ly
                    src = span((y_ * n_lx + x_) * D + toff[h], tsz[h], UNIT)
                    send(tt.at[src, :], own_t.at[ly, dst, :], "t_txt", rid["t_txt"], dev(ly_=y_))

    moved_i = raw_i.at[0, 0, pl.ds(0, n_lx - 1)]
    moved_t = own_t.at[pl.ds(0, n_ly - 1)]

    def image_z(a, h):
        ref = image_ref(a, kl, ly, h)
        for d in range(1, n_kl):
            q = rid[("iz", a)] + (d - 1) * HI + h
            send(ref, ref, ("img", a), q, dev(k_=kh * n_kl + (kl + d) % n_kl), isz[h])

    def image_y(a, h):
        ref = image_ref(a, kl, ly, h)
        for e in range(1, n_ly):
            send(ref, ref, ("img", a), rid[("iy", a)] + h, dev(ly_=(ly + e) % n_ly), isz[h])

    def image_relay(a, h):
        for d in range(1, n_kl):
            ref = image_ref(a, (kl + n_kl - d) % n_kl, ly, h)
            got(ref, rid[("iz", a)] + (d - 1) * HI + h)
            for e in range(1, n_ly):
                send(ref, ref, ("img", a), rid[("iy", a)] + h, dev(ly_=(ly + e) % n_ly), isz[h])

    def image_finish(a, h):
        got_rows((n_ly - 1) * n_kl * isz[h], rid[("iy", a)] + h)
        if a == 0:
            return
        for p in range(n_kl):
            for y_ in range(n_ly):
                def load(o):
                    rng = pl.ds(n_ly * ioff[h] + y_ * isz[h] + o, UNIT)
                    xs = [raw_i[p, fy, fx, rng, :] for fy in range(n_ly) for fx in range(n_lx)]
                    return jnp.concatenate(xs, axis=1).astype(F32)
                unit(load, img_t, n_img * ioff[h] + islot(p, y_) * isz[h], isz[h])

    def text_first(a, h):
        src = own_ref(a, h)
        for g in range(n_kh):
            dest = g * n_kl + src_kl
            op = copy(src, text_ref(a, src_j, lx, h), sid[("first", a)],
                      rid[("tz", a)] + src_j * HT + h, dev(k_=dest))

            @pl.when(dest != k)
            def _():
                op.start()

            @pl.when(dest == k)
            def _():
                if a == 0:
                    txt_s[trng(h, tslot(src_j, lx, c)), :] = own_s[pl.ds(toff[h], tsz[h]), :]
                else:
                    rng = pl.ds(n_lx * toff[h], n_lx * tsz[h])
                    raw_t[src_j, lx, :, rng, :] = own_t[:, rng, :]

    def first_left(a):
        @pl.when(src_kl == kl)
        def _():
            left(txt_s.at[pl.ds(0, (n_kh - 1) * D), :], sid[("first", a)])

        @pl.when(src_kl != kl)
        def _():
            left(txt_s.at[pl.ds(0, n_kh * D), :], sid[("first", a)])

    def core_send(a, ref, h):
        send(ref, ref, ("txt", a), rid[("tc", a)] + h, dev(c_=1 - c), tsz[h])

    def text_relay(a, h):
        for j in range(n_kh):
            ref = text_ref(a, j, lx, h)

            @pl.when(kl * n_kh + j != k)
            def _():
                got(ref, rid[("tz", a)] + j * HT + h)

            for e in range(1, n_lx):
                send(ref, ref, ("txt", a), rid[("tx", a)] + (e - 1) * HT + h, dev(lx_=(lx + e) % n_lx), tsz[h])
            if a == 0:
                core_send(a, ref, h)

    def text_cross(a, h):
        for e in range(1, n_lx):
            got_rows(n_kh * tsz[h], rid[("tx", a)] + (e - 1) * HT + h)
            for j in range(n_kh):
                if a == 0:
                    core_send(a, text_ref(a, j, (lx + n_lx - e) % n_lx, h), h)
        if a == 0:
            return
        for j in range(n_kh):
            for x_ in range(n_lx):
                def load(o):
                    rng = pl.ds(n_lx * toff[h] + x_ * tsz[h] + o, UNIT)
                    xs = [raw_t[j, fx, fy, rng, :] for fy in range(n_ly) for fx in range(n_lx)]
                    return jnp.concatenate(xs, axis=1).astype(F32)
                unit(load, txt_t, n_txt * toff[h] + tslot(j, x_, c) * tsz[h], tsz[h])
                core_send(a, txt_t.at[trng(h, tslot(j, x_, c)), :], h)

    def text_finish(a, h):
        got_rows(n_lx * n_kh * tsz[h], rid[("tc", a)] + h)

    def tile_of(n, most):
        return max(t for t in range(UNIT, min(n, most) + 1, UNIT) if n % t == 0)

    def logits(txt, img, scale, out, row0, n):
        tile = tile_of(n, TILE)
        m = jnp.full((8, rows), -jnp.inf, F32)
        for o in range(row0, row0 + n, tile):
            v = scale * lax.dot_general(
                txt[pl.ds(o, tile), :], img[...], (((1,), (1,)), ((), ())),
                preferred_element_type=F32,
            )
            out[pl.ds(o, tile), :] = v
            m = jnp.maximum(m, jnp.max(v.reshape(tile // 8, 8, rows), axis=0))
        return jnp.max(m, axis=0, keepdims=True)

    def zipped(image_step, text_step):
        for h in range(max(HI, HT)):
            if h < HT:
                text_step(h)
            if h < HI:
                image_step(h)

    teacher_exchange()

    def student_text(h):
        if h:
            own_text(h)
        text_first(0, h)

    def student_image(h):
        if h:
            own_image(h)
        image_z(0, h)
        image_y(0, h)
    zipped(student_image, student_text)
    text_relay(0, 0)
    image_relay(0, 0)
    teacher_kept()
    got(moved_i, rid["t_img"])
    got(moved_t, rid["t_txt"])
    ahead = min(3, HT)
    for h in range(ahead):
        text_first(1, h)
    for h in range(max(HI, HT - ahead)):
        if h < HI:
            image_z(1, h)
        if ahead + h < HT:
            text_first(1, ahead + h)
    relay_s = [functools.partial(text_relay, 0, h) for h in range(1, HT)]
    relay_t = [functools.partial(text_relay, 1, h) for h in range(HT)]
    image_s = [functools.partial(image_relay, 0, h) for h in range(1, HI)]
    image_t = [functools.partial(image_relay, 1, h) for h in range(HI)]
    cross_s = [functools.partial(text_cross, 0, h) for h in range(HT)]
    cross_t = [functools.partial(text_cross, 1, h) for h in range(HT)]
    finish_t = [functools.partial(image_finish, 1, h) for h in range(HI)]

    def step(*queues):
        for queue in queues:
            if queue:
                queue.pop(0)()

    step(relay_s)
    while relay_s:
        step(image_s, relay_s, cross_s)
    while image_s:
        step(image_s)
    for h in range(HI):
        image_y(1, h)
    while len(cross_s) > 2:
        step(cross_s)
    step(relay_t)
    step(cross_s, cross_s)
    step(relay_t)
    while cross_s:
        step(cross_s)
    for h in range(HI):
        image_finish(0, h)
    for h in range(HT):
        text_finish(0, h)
    step(image_t)
    step(relay_t)
    smax = logits(txt_s, img_s, sscale, slog, 0, cols)
    step(cross_t)
    step(relay_t)
    step(image_t)
    step(cross_t)
    while len(image_t) > 0:
        step(image_t)
    while relay_t:
        step(relay_t)
    while len(cross_t) > 2:
        step(cross_t)
    step(finish_t)
    step(cross_t)
    while finish_t:
        step(finish_t)
    def exps(row0, n, top_t):
        def fold(v):
            return jnp.sum(v.reshape(STEP // 8, 8, rows), axis=0)

        def body(i, carry):
            a, b, x = carry
            o = pl.multiple_of(row0 + i * STEP, STEP)
            s = slog[pl.ds(o, STEP), :]
            t = tlog[pl.ds(o, STEP), :]
            es = jnp.exp(s - smax)
            et = jnp.exp(t - top_t)
            slog[pl.ds(o, STEP), :] = es
            tlog[pl.ds(o, STEP), :] = et
            return (a + fold(es), b + fold(et), x + fold(et * (t - s)))
        zero = jnp.zeros((8, rows), F32)
        return lax.fori_loop(0, n // STEP, body, (zero, zero, zero))

    row0 = [n_txt * o for o in toff]
    height = [n_txt * n for n in tsz]
    tops = []
    sums = []

    def teacher(h0, h1):
        for h in range(h0, h1):
            text_finish(1, h)
        n = sum(height[h0:h1])
        top = logits(txt_t, img_t, tscale, tlog, row0[h0], n)
        if h0 == 0:
            while cross_t:
                step(cross_t)
        tops.append(top)
        tops_at.extend([top] * (h1 - h0))
        sums.append([jnp.sum(v, axis=0, keepdims=True) for v in exps(row0[h0], n, top)])

    tops_at = []
    cuts = sorted({0, max(HT - 2, 0), HT - 1, HT})
    for h0, h1 in zip(cuts, cuts[1:]):
        teacher(h0, h1)

    tmax = functools.reduce(jnp.maximum, tops)
    shift = [jnp.exp(m - tmax) for m in tops]
    asum = sum(v[0] for v in sums)
    bsum = sum(v[1] * e for v, e in zip(sums, shift))
    xsum = sum(v[2] * e for v, e in zip(sums, shift))
    pack = [smax, tmax, asum, bsum, xsum]
    stat[islot(kl, ly)] = jnp.concatenate(pack + [jnp.zeros((3, rows), F32)], axis=0)
    for d in range(n_kl):
        for e in range(n_ly):
            if d or e:
                send(stat.at[islot(kl, ly)], stat.at[islot(kl, ly)], "stat", rid["stat"],
                     dev(k_=kh * n_kl + (kl + d) % n_kl, ly_=(ly + e) % n_ly))
    for a in range(2):
        first_left(a)
        left_rows(("img", a), ("txt", a))
    got(stat.at[pl.ds(0, n_img - 1)], rid["stat"])

    all_stat = [stat[s] for s in range(n_img)]
    gs = functools.reduce(jnp.maximum, [v[0:1] for v in all_stat])
    gt = functools.reduce(jnp.maximum, [v[1:2] for v in all_stat])
    es = [jnp.exp(v[0:1] - gs) for v in all_stat]
    et = [jnp.exp(v[1:2] - gt) for v in all_stat]
    ssum = sum(v[2:3] * e for v, e in zip(all_stat, es))
    tsum = sum(v[3:4] * e for v, e in zip(all_stat, et))
    cross = sum(v[4:5] * e for v, e in zip(all_stat, et))
    diverge = cross / tsum - (gt + jnp.log(tsum)) + (gs + jnp.log(ssum))
    mine = tslot(kh, lx, c)
    part[mine] = jnp.broadcast_to(jnp.sum(diverge, axis=1, keepdims=True), (8, 128))
    for peer in loss_peers:
        send(part.at[mine], part.at[mine], "loss", rid["loss"], loss_peer(*peer))

    s_mul = sscale * jnp.exp(smax - gs) / ssum
    t_scale = sscale / tsum

    t_mul = [t_scale * jnp.exp(m - gt) for m in tops_at]

    dtxt = txt_t

    def grad_of(rng, h):
        v = (slog[rng, :] * s_mul - tlog[rng, :] * t_mul[h]).astype(BF16)
        grad[rng, :] = v
        return v

    def text_piece(j, lx_, c_, fresh=False):
        slot = tslot(j, lx_, c_)
        if fresh:
            g = [grad_of(trng(h, slot), h) for h in range(HT)]
        else:
            g = [grad[trng(h, slot), :] for h in range(HT)]
        v = jnp.dot(jnp.concatenate(g, axis=0), img_s[...], preferred_element_type=F32)
        dtxt[at(slot), :] = v.astype(BF16)

    order = [(n_kh - 1 - kh + i) % n_kh for i in range(n_kh)]

    def core_id(e, i):
        first = n_kh if n_lx > 1 else 0
        n = e * n_kh + i
        if n == first:
            return rid["dc"] + n_lx * n_kh - 1
        return rid["dc"] + (n if n < first else n - 1)

    def chunked(e, i):
        return e == (1 if n_lx > 1 else 0) and i == 0

    def to_core(e, i, fresh=False):
        x_ = (lx + e) % n_lx
        j = order[i]
        text_piece(j, x_, 1 - c, fresh)
        if chunked(e, i):
            for h in range(HB):
                send(dtxt.at[brng(tslot(j, x_, 1 - c), h), :], r1.at[x_ * n_kh + j, part_of[h], :], "dc",
                     core_id(e, i) + h, dev(c_=1 - c), bsz[h])
        else:
            send(dtxt.at[at(tslot(j, x_, 1 - c)), :], r1.at[x_ * n_kh + j], "dc", core_id(e, i), dev(c_=1 - c), D)

    def from_core(e, i, h):
        s = ((lx + e) % n_lx) * n_kh + order[i]
        if chunked(e, i):
            got(r1.at[s, part_of[h], :], core_id(e, i) + h)
        elif h == 0:
            got(r1.at[s], core_id(e, i))
        return r1[s, part_of[h], :].astype(F32)

    def to_x(e, i):
        x_ = (lx + e) % n_lx
        j = order[i]
        for h in range(HB):
            rng = brng(tslot(j, x_, c), h)
            dtxt[rng, :] = (dtxt[rng, :].astype(F32) + from_core(e, i, h)).astype(BF16)
            q = rid["dx"] + ((e - 1) * n_kh + i) * HB + h
            send(dtxt.at[rng, :], r2.at[(e - 1) * n_kh + j, part_of[h], :], "dx", q, dev(lx_=x_), bsz[h])

    dimg = img_t
    full = [h for h in range(HI) if (n_kl * isz[h]) % 128 == 0]
    rest = [h for h in range(HI) if h not in full]

    def image_piece(y_, with_rest):
        windows = [span(n_img * ioff[h] + y_ * n_kl * isz[h], n_kl * isz[h], 128) for h in full]
        if with_rest:
            windows += [pl.ds(n_img * ioff[h], n_img * isz[h]) for h in rest]
        tile = tile_of(cols, DOT)
        wide = code if tile == cols else code // 2
        for n0 in range(0, code, wide):
            out = pl.ds(n0, wide)
            v = 0.0
            for o in range(0, cols, tile):
                g = jnp.concatenate([grad[pl.ds(o, tile), w] for w in windows], axis=1)
                v = v + lax.dot_general(
                    g, txt_s[pl.ds(o, tile), out], (((0,), (0,)), ((), ())), preferred_element_type=F32,
                )
            v = v.astype(BF16)
            slots = [(islot(p, y_), h) for h in full for p in range(n_kl)]
            if with_rest:
                slots += [(s, h) for h in rest for s in range(n_img)]
            o = 0
            for s, h in slots:
                dimg[span(s * D + ioff[h], isz[h], UNIT), out] = v[o:o + isz[h]]
                o += isz[h]

    def to_y(e):
        y_ = (ly + e) % n_ly
        image_piece(y_, e == 1)
        for d in [*range(1, n_kl), 0]:
            for h in range(HB):
                q = rid["gy"] + d * HB + h
                send(dimg.at[brng(islot((kl + d) % n_kl, y_), h), :], ry.at[(e - 1) * n_kl + d, part_of[h], :],
                     "gy", q, dev(ly_=y_), bsz[h])

    x1 = (lx + 1) % n_lx
    to_core(1, 0, True)
    text_piece(order[0], x1, c, True)
    for h in range(HT):
        def to_grad(i, _):
            grad_of(span(row0[h] + i * STEP, STEP, STEP), h)
            return 0
        lax.fori_loop(0, height[h] // STEP, to_grad, 0, unroll=2)
    to_x(1, 0)
    to_core(0, 0)
    text_piece(order[0], lx, c)
    for e in range(1, n_ly):
        to_y(e)

    def owner_copy(i, h):
        j = order[i]
        dest = kl * n_kh + j
        op = copy(dtxt.at[brng(tslot(j, lx, c), h), :], r3.at[kh, part_of[h], :], sid["dz"], rid["dz"], dev(k_=dest))
        return dest, op

    def text_sum(i, h):
        j = order[i]
        rng = brng(tslot(j, lx, c), h)
        v = dtxt[rng, :].astype(F32) + from_core(0, i, h)
        for e in range(1, n_lx):
            got(r2.at[(e - 1) * n_kh + j, part_of[h], :], rid["dx"] + ((e - 1) * n_kh + i) * HB + h)
            v = v + r2[(e - 1) * n_kh + j, part_of[h], :].astype(F32)
        dtxt[rng, :] = v.astype(BF16)
        dest, op = owner_copy(i, h)

        @pl.when(dest != k)
        def _():
            op.start()

        @pl.when(dest == k)
        def _():
            r3[kh, part_of[h], :] = dtxt[rng, :]

    def got_y(d, h):
        got_rows((n_ly - 1) * bsz[h], rid["gy"] + d * HB + h)

    def image_sum(d, h):
        got_y(d, h)
        rng = brng(islot((kl + d) % n_kl, ly), h)
        v = dimg[rng, :].astype(F32)
        for e in range(1, n_ly):
            v = v + ry[(e - 1) * n_kl + d, part_of[h], :].astype(F32)
        dimg[rng, :] = v.astype(BF16)
        send(dimg.at[rng, :], rz.at[d - 1, part_of[h], :], "gz", rid["gz"], dev(k_=kh * n_kl + (kl + d) % n_kl), bsz[h])

    text_sum(0, 0)
    for e in range(1, n_lx):
        for i in range(1 if e == 1 else 0, n_kh):
            to_core(e, i)
            text_piece(order[i], (lx + e) % n_lx, c)
            if e > 1 or i > 1:
                to_x(e, i)
    image_piece(ly, n_ly == 1)
    if n_kh > 1:
        to_x(1, 1)
    texts = [(i, h) for i in range(n_kh) for h in range(HB)][1:]
    images = [(d, h) for d in range(1, n_kl) for h in range(HB)]
    while texts or images:
        if texts:
            i, h = texts.pop(0)
            if h == HB - 1 and i + 1 < n_kh:
                to_core(0, i + 1)
                text_piece(order[i + 1], lx, c)
            text_sum(i, h)
        if images:
            image_sum(*images.pop(0))
    got(part.at[pl.ds(0, len(loss_peers))], rid["loss"])
    loss_out[...] = sum(part[i] for i in range(n_txt)) / float(D * n_row * n_loop)

    def finish(terms, src, inv_ref, out):
        for o in range(0, D, UNIT):
            rng = pl.ds(o, UNIT)
            g = terms(o)
            x = src[rng, :].astype(F32)
            inv = inv_ref[rng, 0:1]
            along = jnp.sum(g * x, axis=1, keepdims=True) * inv * inv
            out[rng, :] = ((g - x * along) * inv).astype(BF16)

    for h in range(HB):
        got_y(0, h)
    got_rows((n_kl - 1) * D, rid["gz"])

    def image_terms(o):
        v = dimg[span(islot(kl, ly) * D + o, UNIT, UNIT), :].astype(F32)
        for e in range(1, n_ly):
            v = v + ry[(e - 1) * n_kl, pl.ds(o, UNIT), :].astype(F32)
        for d in range(1, n_kl):
            v = v + rz[d - 1, pl.ds(o, UNIT), :].astype(F32)
        return v
    finish(image_terms, si, inv_i, gi_out)

    def on_owner(wait):
        @pl.when(src_kl == kl)
        def _():
            wait(n_kh - 1)

        @pl.when(src_kl != kl)
        def _():
            wait(n_kh)
    on_owner(lambda n: got(txt_s.at[pl.ds(0, n * D), :], rid["dz"]))
    finish(lambda o: sum(r3[g, pl.ds(o, UNIT), :].astype(F32) for g in range(n_kh)), st, inv_t, gt_out)

    left(moved_i, sid["t_img"])
    left(moved_t, sid["t_txt"])
    left(stat.at[pl.ds(0, n_img - 1)], sid["stat"])
    left_rows("dc", "dx", "gy", "gz")
    left(part.at[pl.ds(0, len(loss_peers))], sid["loss"])

    on_owner(lambda n: left(txt_s.at[pl.ds(0, n * D), :], sid["dz"]))


def emit(total, gi, gt, loss_out, gi_out, gt_out):
    loss_out[0] = total[0, 0]
    gi_out[...] = gi[...]
    gt_out[...] = gt[...]


def on_device(n_row, n_loop, si, st, ti, tt, ssc, tsc):
    D, code = si.shape
    n_kl, n_lx = 2, 2
    n_kh, n_ly = n_row // (2 * n_kl), n_loop // n_lx
    n_img, n_txt = n_kl * n_ly, n_kh * n_lx * 2
    rows, cols = n_img * D, n_txt * D
    feat = code // n_loop
    rid, sid = make_ids(D, n_kh, n_kl, n_lx, n_ly)
    dims = (n_row, n_loop, n_kh, n_kl, n_lx, n_ly, D, code)
    vm = pl.BlockSpec(memory_space=pltpu.VMEM)
    sm = pl.BlockSpec(memory_space=pltpu.SMEM)
    anywhere = pl.BlockSpec(memory_space=pl.ANY)
    V = pltpu.VMEM
    loss, gi, gt = pl.pallas_call(
        functools.partial(kernel, dims, rid, sid),
        out_shape=(
            jax.ShapeDtypeStruct((8, 128), F32),
            jax.ShapeDtypeStruct((D, code), BF16),
            jax.ShapeDtypeStruct((D, code), BF16),
        ),
        in_specs=[anywhere] * 4 + [sm] * 2,
        out_specs=(vm, vm, vm),
        scratch_shapes=[
            V((rows, code), BF16), V((rows, code), BF16),
            V((D, code), BF16), V((n_ly, n_lx * D, feat), BF16),
            V((cols, code), BF16), V((cols, code), BF16),
            V((n_kl, n_ly, n_lx, n_ly * D, feat), BF16),
            V((n_kh, n_lx, n_ly, n_lx * D, feat), BF16),
            V((cols, rows), F32), V((cols, rows), F32), V((cols, rows), BF16),
            V((n_img, 8, rows), F32),
            V((n_lx * n_kh, D, code), BF16),
            V(((n_lx - 1) * n_kh, D, code), BF16),
            V((n_kh, D, code), BF16),
            V(((n_ly - 1) * n_kl, D, code), BF16),
            V((n_kl - 1, D, code), BF16),
            V((n_txt, 8, 128), F32),
            V((D, 128), F32), V((D, 128), F32),
            V((D, code), BF16), V((D, code), BF16),
            pltpu.SemaphoreType.DMA((sid.count,)),
            pltpu.SemaphoreType.DMA((rid.count,)),
        ],
        compiler_params=pltpu.CompilerParams(
            collective_id=0, has_side_effects=True, vmem_limit_bytes=67043328,
        ),
    )(si, st, ti, tt, ssc, tsc)
    return pl.pallas_call(
        emit,
        out_shape=(
            jax.ShapeDtypeStruct((1,), F32),
            jax.ShapeDtypeStruct((D, code), BF16),
            jax.ShapeDtypeStruct((D, code), BF16),
        ),
        in_specs=[vm] * 3,
        out_specs=(sm, vm, vm),
    )(loss, gi, gt)


def solution(mesh):
    return jax.shard_map(
        functools.partial(on_device, mesh.shape["row"], mesh.shape["loop"]),
        mesh=mesh,
        in_specs=(
            P(("row", "loop"), None),
            P(("row", "loop"), None),
            P("row", "loop"),
            P("row", "loop"),
            P(),
            P(),
        ),
        out_specs=(P(), P(("row", "loop"), None), P(("row", "loop"), None)),
        check_vma=False,
    )
```

```python
import functools
import jax
import jax.numpy as jnp
from jax import lax
from jax.experimental import pallas as pl
from jax.experimental.pallas import tpu as pltpu
from jax.sharding import PartitionSpec as P

EPS = 1e-06
F32 = jnp.float32
BF16 = jnp.bfloat16
MESH = pl.DeviceIdType.MESH
UNIT = 32
IMAGE_PART = 64
STEP = 32
DOT = 1280
TILE = 256


class Ids:
    def __init__(self):
        self.table = {}
        self.count = 0

    def take(self, name, size=1):
        self.table[name] = self.count
        self.count += size

    def __getitem__(self, name):
        return self.table[name]


def split(D, part):
    return [min(part, D - o) for o in range(0, D, part)]


def offsets(sizes):
    return [sum(sizes[:h]) for h in range(len(sizes))]


def back_sizes(D):
    units = D // UNIT
    if units < 4:
        return [UNIT] * units
    return [UNIT, D - 3 * UNIT, UNIT, UNIT]


def make_ids(D, n_kh, n_kl, n_lx, n_ly):
    HI, HT, HB = len(split(D, IMAGE_PART)), D // UNIT, len(back_sizes(D))
    recv, sent = Ids(), Ids()
    recv.take("t_img")
    recv.take("t_txt")
    for a in range(2):
        recv.take(("iz", a), (n_kl - 1) * HI)
        recv.take(("iy", a), HI)
        recv.take(("tz", a), n_kh * HT)
        recv.take(("tx", a), (n_lx - 1) * HT)
        recv.take(("tc", a), HT)
    recv.take("stat")
    recv.take("dc", n_lx * n_kh - 1 + HB)
    recv.take("dx", (n_lx - 1) * n_kh * HB)
    recv.take("dz")
    recv.take("gy", n_kl * HB)
    recv.take("gz")
    recv.take("loss")
    recv.take("keep")
    recv.take("load", 2)
    for name in ("t_img", "t_txt", "stat", "dc", "dx", "dz", "gy", "gz", "loss"):
        sent.take(name)
    for a in range(2):
        for kind in ("img", "first", "txt"):
            sent.take((kind, a))
    return recv, sent


def kernel(
    dims, rid, sid,
    si_in, st_in, ti, tt, ssc, tsc,
    loss_out, gi_out, gt_out,
    img_s, img_t, own_s, own_t, txt_s, txt_t, raw_i, raw_t,
    slog, tlog, grad, stat, r1, r2, r3, ry, rz, part, inv_i, inv_t, si, st,
    ss, rs,
):
    n_row, n_loop, n_kh, n_kl, n_lx, n_ly, D, code = dims
    isz, tsz, bsz = split(D, IMAGE_PART), split(D, UNIT), back_sizes(D)
    ioff, toff, boff = offsets(isz), offsets(tsz), offsets(bsz)
    HI, HT, HB = len(isz), len(tsz), len(bsz)
    n_img = n_kl * n_ly
    n_txt = n_kh * n_lx * 2
    rows = n_img * D
    cols = n_txt * D
    r = lax.axis_index("row")
    l = lax.axis_index("loop")
    k, c = r // 2, r % 2
    kh, kl = k // n_kl, k % n_kl
    src_kl, src_j = k // n_kh, k % n_kh
    ly, lx = l // n_lx, l % n_lx
    sscale = ssc[0]
    tscale = tsc[0]

    def dev(k_=None, c_=None, ly_=None, lx_=None):
        kk = k if k_ is None else k_
        cc = c if c_ is None else c_
        yy = ly if ly_ is None else ly_
        xx = lx if lx_ is None else lx_
        return (kk * 2 + cc, yy * n_lx + xx)

    def islot(kl_, ly_):
        return ly_ * n_kl + kl_

    def tslot(j, lx_, c_):
        return (j * n_lx + lx_) * 2 + c_

    def span(start, size, step):
        return pl.ds(pl.multiple_of(start, step), size)

    def irng(h, slot):
        return span(n_img * ioff[h] + slot * isz[h], isz[h], UNIT)

    def trng(h, slot):
        return span(n_txt * toff[h] + slot * tsz[h], tsz[h], UNIT)

    def brng(slot, h):
        return span(slot * D + boff[h], bsz[h], UNIT)

    def at(slot):
        return span(slot * D, D, UNIT)

    part_of = [pl.ds(boff[h], bsz[h]) for h in range(HB)]

    def image_ref(a, kl_, ly_, h):
        if a == 0:
            return img_s.at[irng(h, islot(kl_, ly_)), :]
        return raw_i.at[kl_, ly_, :, pl.ds(n_ly * ioff[h], n_ly * isz[h]), :]

    def text_ref(a, j, lx_, h):
        if a == 0:
            return txt_s.at[trng(h, tslot(j, lx_, c)), :]
        return raw_t.at[j, lx_, :, pl.ds(n_lx * toff[h], n_lx * tsz[h]), :]

    def own_ref(a, h):
        if a == 0:
            return own_s.at[pl.ds(toff[h], tsz[h]), :]
        return own_t.at[:, pl.ds(n_lx * toff[h], n_lx * tsz[h]), :]

    def copy(src, dst, q_send, q_recv, device):
        return pltpu.make_async_remote_copy(
            src_ref=src, dst_ref=dst, send_sem=ss.at[q_send], recv_sem=rs.at[q_recv],
            device_id=device, device_id_type=MESH,
        )

    sent_rows = {}

    def send(src, dst, name, q, device, n=0):
        copy(src, dst, sid[name], q, device).start()
        sent_rows[name] = sent_rows.get(name, 0) + n

    def got(dst, q):
        copy(dst, dst, 0, q, dev(c_=1 - c)).wait_recv()

    def got_rows(n, q):
        got(txt_s.at[pl.ds(0, n), :], q)

    def left(ref, q):
        copy(ref, ref, q, 0, dev(c_=1 - c)).wait_send()

    def left_rows(*names):
        for name in names:
            left(txt_s.at[pl.ds(0, sent_rows.pop(name)), :], sid[name])

    loss_peers = [
        (kd, xd, cd) for kd in range(n_kh) for xd in range(n_lx) for cd in range(2) if kd or xd or cd
    ]

    def loss_peer(kd, xd, cd):
        return dev(k_=((kh + kd) % n_kh) * n_kl + kl, c_=(c + cd) % 2, lx_=(lx + xd) % n_lx)

    barrier = pltpu.get_barrier_semaphore()
    n_peer = 0
    for kd, xd, cd in loss_peers:
        if (kd != 0) + (xd != 0) + (cd != 0) > 1:
            pl.semaphore_signal(barrier, inc=1, device_id=loss_peer(kd, xd, cd), device_id_type=MESH)
            n_peer += 1
    for e in range(1, n_ly):
        pl.semaphore_signal(barrier, inc=1, device_id=dev(ly_=(ly + e) % n_ly), device_id_type=MESH)
        n_peer += 1
    for e in range(1, n_lx):
        pl.semaphore_signal(barrier, inc=1, device_id=dev(lx_=(lx + e) % n_lx), device_id_type=MESH)
        n_peer += 1
    for d in range(1, n_kh * n_kl):
        pl.semaphore_signal(barrier, inc=1, device_id=dev(k_=(k + d) % (n_kh * n_kl)), device_id_type=MESH)
        n_peer += 1
    pl.semaphore_signal(barrier, inc=1, device_id=dev(c_=1 - c), device_id_type=MESH)
    n_peer += 1
    for d in range(1, n_kl):
        for e in range(1, n_ly):
            diagonal = dev(k_=kh * n_kl + (kl + d) % n_kl, ly_=(ly + e) % n_ly)
            pl.semaphore_signal(barrier, inc=1, device_id=diagonal, device_id_type=MESH)
            n_peer += 1

    def unit(load, dst, first, n, keep=None):
        for o in range(0, n, UNIT):
            x = load(o)
            n2 = jnp.sum(x * x, axis=1, keepdims=True) + EPS
            inv = 1.0 / jnp.sqrt(n2)
            if keep is not None:
                keep(o, inv)
            dst[span(first + o, UNIT, UNIT), :] = (x * inv).astype(BF16)

    def student_unit(src, dst, first, o0, n, inv_ref):
        def load(o):
            return src[pl.ds(o0 + o, UNIT), :].astype(F32)

        def keep(o, inv):
            inv_ref[pl.ds(o0 + o, UNIT), :] = jnp.broadcast_to(inv, (UNIT, 128))
        unit(load, dst, first, n, keep)

    def own_text(h):
        student_unit(st, own_s, toff[h], toff[h], tsz[h], inv_t)

    def own_image(h):
        student_unit(si, img_s, n_img * ioff[h] + islot(kl, ly) * isz[h], ioff[h], isz[h], inv_i)

    def teacher_keep():
        for h in range(HI):
            for y_ in range(n_ly):
                dst = pl.ds(n_ly * ioff[h] + y_ * isz[h], isz[h])
                src = span((y_ * n_lx + lx) * D + ioff[h], isz[h], UNIT)
                pltpu.make_async_copy(ti.at[src, :], raw_i.at[kl, ly, lx, dst, :], rs.at[rid["keep"]]).start()
        for h in range(HT):
            for x_ in range(n_lx):
                dst = pl.ds(n_lx * toff[h] + x_ * tsz[h], tsz[h])
                src = span((ly * n_lx + x_) * D + toff[h], tsz[h], UNIT)
                pltpu.make_async_copy(tt.at[src, :], own_t.at[ly, dst, :], rs.at[rid["keep"]]).start()

    def teacher_kept():
        both = txt_s.at[pl.ds(0, D * (n_ly + n_lx) // n_loop), :]
        pltpu.make_async_copy(both, both, rs.at[rid["keep"]]).wait()

    load_t = pltpu.make_async_copy(st_in, st, rs.at[rid["load"]])
    load_i = pltpu.make_async_copy(si_in, si, rs.at[rid["load"] + 1])
    load_t.start()
    load_i.start()
    teacher_keep()
    load_t.wait()
    own_text(0)
    load_i.wait()
    own_image(0)
    pl.semaphore_wait(barrier, n_peer)

    def teacher_exchange():
        for h in range(HI):
            for y_ in range(n_ly):
                dst = pl.ds(n_ly * ioff[h] + y_ * isz[h], isz[h])
                for e in range(1, n_lx):
                    x_ = (lx + e) % n_lx
                    src = span((y_ * n_lx + x_) * D + ioff[h], isz[h], UNIT)
                    send(ti.at[src, :], raw_i.at[kl, ly, lx, dst, :], "t_img", rid["t_img"], dev(lx_=x_))
        for h in range(HT):
            for x_ in range(n_lx):
                dst = pl.ds(n_lx * toff[h] + x_ * tsz[h], tsz[h])
                for e in range(1, n_ly):
                    y_ = (ly + e) % n_ly
                    src = span((y_ * n_lx + x_) * D + toff[h], tsz[h], UNIT)
                    send(tt.at[src, :], own_t.at[ly, dst, :], "t_txt", rid["t_txt"], dev(ly_=y_))

    moved_i = raw_i.at[0, 0, pl.ds(0, n_lx - 1)]
    moved_t = own_t.at[pl.ds(0, n_ly - 1)]

    def image_z(a, h):
        ref = image_ref(a, kl, ly, h)
        for d in range(1, n_kl):
            q = rid[("iz", a)] + (d - 1) * HI + h
            send(ref, ref, ("img", a), q, dev(k_=kh * n_kl + (kl + d) % n_kl), isz[h])

    def image_y(a, h):
        ref = image_ref(a, kl, ly, h)
        for e in range(1, n_ly):
            send(ref, ref, ("img", a), rid[("iy", a)] + h, dev(ly_=(ly + e) % n_ly), isz[h])

    def image_relay(a, h):
        for d in range(1, n_kl):
            ref = image_ref(a, (kl + n_kl - d) % n_kl, ly, h)
            got(ref, rid[("iz", a)] + (d - 1) * HI + h)
            for e in range(1, n_ly):
                send(ref, ref, ("img", a), rid[("iy", a)] + h, dev(ly_=(ly + e) % n_ly), isz[h])

    def image_finish(a, h):
        got_rows((n_ly - 1) * n_kl * isz[h], rid[("iy", a)] + h)
        if a == 0:
            return
        for p in range(n_kl):
            for y_ in range(n_ly):
                def load(o):
                    rng = pl.ds(n_ly * ioff[h] + y_ * isz[h] + o, UNIT)
                    xs = [raw_i[p, fy, fx, rng, :] for fy in range(n_ly) for fx in range(n_lx)]
                    return jnp.concatenate(xs, axis=1).astype(F32)
                unit(load, img_t, n_img * ioff[h] + islot(p, y_) * isz[h], isz[h])

    def text_first(a, h):
        src = own_ref(a, h)
        for g in range(n_kh):
            dest = g * n_kl + src_kl
            op = copy(src, text_ref(a, src_j, lx, h), sid[("first", a)],
                      rid[("tz", a)] + src_j * HT + h, dev(k_=dest))

            @pl.when(dest != k)
            def _():
                op.start()

            @pl.when(dest == k)
            def _():
                if a == 0:
                    txt_s[trng(h, tslot(src_j, lx, c)), :] = own_s[pl.ds(toff[h], tsz[h]), :]
                else:
                    rng = pl.ds(n_lx * toff[h], n_lx * tsz[h])
                    raw_t[src_j, lx, :, rng, :] = own_t[:, rng, :]

    def first_left(a):
        @pl.when(src_kl == kl)
        def _():
            left(txt_s.at[pl.ds(0, (n_kh - 1) * D), :], sid[("first", a)])

        @pl.when(src_kl != kl)
        def _():
            left(txt_s.at[pl.ds(0, n_kh * D), :], sid[("first", a)])

    def core_send(a, ref, h):
        send(ref, ref, ("txt", a), rid[("tc", a)] + h, dev(c_=1 - c), tsz[h])

    def text_relay(a, h):
        for j in range(n_kh):
            ref = text_ref(a, j, lx, h)

            @pl.when(kl * n_kh + j != k)
            def _():
                got(ref, rid[("tz", a)] + j * HT + h)

            for e in range(1, n_lx):
                send(ref, ref, ("txt", a), rid[("tx", a)] + (e - 1) * HT + h, dev(lx_=(lx + e) % n_lx), tsz[h])
            if a == 0:
                core_send(a, ref, h)

    def text_cross(a, h):
        for e in range(1, n_lx):
            got_rows(n_kh * tsz[h], rid[("tx", a)] + (e - 1) * HT + h)
            for j in range(n_kh):
                if a == 0:
                    core_send(a, text_ref(a, j, (lx + n_lx - e) % n_lx, h), h)
        if a == 0:
            return
        for j in range(n_kh):
            for x_ in range(n_lx):
                def load(o):
                    rng = pl.ds(n_lx * toff[h] + x_ * tsz[h] + o, UNIT)
                    xs = [raw_t[j, fx, fy, rng, :] for fy in range(n_ly) for fx in range(n_lx)]
                    return jnp.concatenate(xs, axis=1).astype(F32)
                unit(load, txt_t, n_txt * toff[h] + tslot(j, x_, c) * tsz[h], tsz[h])
                core_send(a, txt_t.at[trng(h, tslot(j, x_, c)), :], h)

    def text_finish(a, h):
        got_rows(n_lx * n_kh * tsz[h], rid[("tc", a)] + h)

    def tile_of(n, most):
        return max(t for t in range(UNIT, min(n, most) + 1, UNIT) if n % t == 0)

    def logits(txt, img, scale, out, row0, n, lane0=0, width=rows):
        tile = tile_of(n, TILE)
        lanes = pl.ds(lane0, width)
        m = jnp.full((8, width), -jnp.inf, F32)
        for o in range(row0, row0 + n, tile):
            v = scale * lax.dot_general(
                txt[pl.ds(o, tile), :], img[lanes, :], (((1,), (1,)), ((), ())),
                preferred_element_type=F32,
            )
            out[pl.ds(o, tile), lanes] = v
            m = jnp.maximum(m, jnp.max(v.reshape(tile // 8, 8, width), axis=0))
        return jnp.max(m, axis=0, keepdims=True)

    def zipped(image_step, text_step):
        for h in range(max(HI, HT)):
            if h < HT:
                text_step(h)
            if h < HI:
                image_step(h)

    teacher_exchange()

    def student_text(h):
        if h:
            own_text(h)
        text_first(0, h)

    def student_image(h):
        if h:
            own_image(h)
        image_z(0, h)
        image_y(0, h)
    zipped(student_image, student_text)
    text_relay(0, 0)
    image_relay(0, 0)
    teacher_kept()
    got(moved_i, rid["t_img"])
    got(moved_t, rid["t_txt"])
    ahead = min(2, HT)
    for h in range(ahead):
        text_first(1, h)
    for h in range(max(HI, HT - ahead)):
        if h < HI:
            image_z(1, h)
        if ahead + h < HT:
            text_first(1, ahead + h)
    relay_s = [functools.partial(text_relay, 0, h) for h in range(1, HT)]
    relay_t = [functools.partial(text_relay, 1, h) for h in range(HT)]
    image_s = [functools.partial(image_relay, 0, h) for h in range(1, HI)]
    image_t = [functools.partial(image_relay, 1, h) for h in range(HI)]
    cross_s = [functools.partial(text_cross, 0, h) for h in range(HT)]
    cross_t = [functools.partial(text_cross, 1, h) for h in range(HT)]
    finish_t = [functools.partial(image_finish, 1, h) for h in range(HI)]

    def step(*queues):
        for queue in queues:
            if queue:
                queue.pop(0)()

    step(relay_s)
    while relay_s:
        step(image_s, relay_s, cross_s)
    while image_s:
        step(image_s)
    for h in range(HI):
        image_y(1, h)
    while len(cross_s) > 2:
        step(cross_s)
    step(relay_t)
    step(cross_s, cross_s)
    step(relay_t)
    while cross_s:
        step(cross_s)
    for h in range(HI):
        image_finish(0, h)
    for h in range(HT):
        text_finish(0, h)
    step(image_t)
    step(relay_t)
    smax = logits(txt_s, img_s, sscale, slog, 0, cols)
    step(image_t)
    step(cross_t)
    step(relay_t)
    step(image_t)
    step(cross_t)
    while image_t:
        step(image_t)
    while relay_t:
        step(relay_t)
    while len(cross_t) > 2:
        step(cross_t)

    def exps(row0, n, top_t, lane0=0, width=rows):
        lanes = pl.ds(lane0, width)
        top_s = smax[:, lane0:lane0 + width]

        def fold(v):
            return jnp.sum(v.reshape(STEP // 8, 8, width), axis=0)

        def body(i, carry):
            a, b, x = carry
            o = pl.multiple_of(row0 + i * STEP, STEP)
            s = slog[pl.ds(o, STEP), lanes]
            t = tlog[pl.ds(o, STEP), lanes]
            es = jnp.exp(s - top_s)
            et = jnp.exp(t - top_t)
            slog[pl.ds(o, STEP), lanes] = es
            tlog[pl.ds(o, STEP), lanes] = et
            return (a + fold(es), b + fold(et), x + fold(et * (t - s)))
        zero = jnp.zeros((8, width), F32)
        sums = lax.fori_loop(0, n // STEP, body, (zero, zero, zero))
        return [jnp.sum(v, axis=0, keepdims=True) for v in sums]

    row0 = [n_txt * o for o in toff]
    height = [n_txt * n for n in tsz]
    tops = []
    sums = []

    tops_at = []

    def keep_stats(top, sums_, n):
        tops.append(top)
        tops_at.extend([top] * n)
        sums.append(sums_)

    def teacher(h):
        text_finish(1, h)
        top = logits(txt_t, img_t, tscale, tlog, row0[h], height[h])
        keep_stats(top, exps(row0[h], height[h], top), 1)

    first = max(HT - 3, 1)
    n0 = sum(height[:first])
    for h in range(first):
        text_finish(1, h)
    parts = []
    for i in range(HI):
        step(finish_t)
        window = (n_img * ioff[i], n_img * isz[i])
        top = logits(txt_t, img_t, tscale, tlog, 0, n0, *window)
        parts.append([top] + exps(0, n0, top, *window))
        if i + 2 == HI and len(cross_t) > 1:
            step(cross_t)
    parts = [jnp.concatenate(v, axis=1) for v in zip(*parts)]
    keep_stats(parts[0], parts[1:], first)
    for h in range(first, HT):
        teacher(h)
        while h == first and cross_t:
            step(cross_t)

    tmax = functools.reduce(jnp.maximum, tops)
    shift = [jnp.exp(m - tmax) for m in tops]
    asum = sum(v[0] for v in sums)
    bsum = sum(v[1] * e for v, e in zip(sums, shift))
    xsum = sum(v[2] * e for v, e in zip(sums, shift))
    pack = [smax, tmax, asum, bsum, xsum]
    stat[islot(kl, ly)] = jnp.concatenate(pack + [jnp.zeros((3, rows), F32)], axis=0)
    for d in range(n_kl):
        for e in range(n_ly):
            if d or e:
                send(stat.at[islot(kl, ly)], stat.at[islot(kl, ly)], "stat", rid["stat"],
                     dev(k_=kh * n_kl + (kl + d) % n_kl, ly_=(ly + e) % n_ly))
    for a in range(2):
        first_left(a)
        left_rows(("img", a), ("txt", a))
    got(stat.at[pl.ds(0, n_img - 1)], rid["stat"])

    all_stat = [stat[s] for s in range(n_img)]
    gs = functools.reduce(jnp.maximum, [v[0:1] for v in all_stat])
    gt = functools.reduce(jnp.maximum, [v[1:2] for v in all_stat])
    es = [jnp.exp(v[0:1] - gs) for v in all_stat]
    et = [jnp.exp(v[1:2] - gt) for v in all_stat]
    ssum = sum(v[2:3] * e for v, e in zip(all_stat, es))
    tsum = sum(v[3:4] * e for v, e in zip(all_stat, et))
    cross = sum(v[4:5] * e for v, e in zip(all_stat, et))
    diverge = cross / tsum - (gt + jnp.log(tsum)) + (gs + jnp.log(ssum))
    mine = tslot(kh, lx, c)
    part[mine] = jnp.broadcast_to(jnp.sum(diverge, axis=1, keepdims=True), (8, 128))
    for peer in loss_peers:
        send(part.at[mine], part.at[mine], "loss", rid["loss"], loss_peer(*peer))

    s_mul = sscale * jnp.exp(smax - gs) / ssum
    t_scale = sscale / tsum

    t_mul = [t_scale * jnp.exp(m - gt) for m in tops_at]

    dtxt = txt_t

    def grad_of(rng, h):
        v = (slog[rng, :] * s_mul - tlog[rng, :] * t_mul[h]).astype(BF16)
        grad[rng, :] = v
        return v

    def text_piece(j, lx_, c_, fresh=False):
        slot = tslot(j, lx_, c_)
        if fresh:
            g = [grad_of(trng(h, slot), h) for h in range(HT)]
        else:
            g = [grad[trng(h, slot), :] for h in range(HT)]
        v = jnp.dot(jnp.concatenate(g, axis=0), img_s[...], preferred_element_type=F32)
        dtxt[at(slot), :] = v.astype(BF16)

    order = [(n_kh - 1 - kh + i) % n_kh for i in range(n_kh)]

    def core_id(e, i):
        first = n_kh if n_lx > 1 else 0
        n = e * n_kh + i
        if n == first:
            return rid["dc"] + n_lx * n_kh - 1
        return rid["dc"] + (n if n < first else n - 1)

    def chunked(e, i):
        return e == (1 if n_lx > 1 else 0) and i == 0

    def to_core(e, i, fresh=False):
        x_ = (lx + e) % n_lx
        j = order[i]
        text_piece(j, x_, 1 - c, fresh)
        if chunked(e, i):
            for h in range(HB):
                send(dtxt.at[brng(tslot(j, x_, 1 - c), h), :], r1.at[x_ * n_kh + j, part_of[h], :], "dc",
                     core_id(e, i) + h, dev(c_=1 - c), bsz[h])
        else:
            send(dtxt.at[at(tslot(j, x_, 1 - c)), :], r1.at[x_ * n_kh + j], "dc", core_id(e, i), dev(c_=1 - c), D)

    def from_core(e, i, h):
        s = ((lx + e) % n_lx) * n_kh + order[i]
        if chunked(e, i):
            got(r1.at[s, part_of[h], :], core_id(e, i) + h)
        elif h == 0:
            got(r1.at[s], core_id(e, i))
        return r1[s, part_of[h], :].astype(F32)

    def to_x(e, i):
        x_ = (lx + e) % n_lx
        j = order[i]
        for h in range(HB):
            rng = brng(tslot(j, x_, c), h)
            dtxt[rng, :] = (dtxt[rng, :].astype(F32) + from_core(e, i, h)).astype(BF16)
            q = rid["dx"] + ((e - 1) * n_kh + i) * HB + h
            send(dtxt.at[rng, :], r2.at[(e - 1) * n_kh + j, part_of[h], :], "dx", q, dev(lx_=x_), bsz[h])

    dimg = img_t
    full = [h for h in range(HI) if (n_kl * isz[h]) % 128 == 0]
    rest = [h for h in range(HI) if h not in full]

    def image_piece(y_, with_rest):
        windows = [span(n_img * ioff[h] + y_ * n_kl * isz[h], n_kl * isz[h], 128) for h in full]
        if with_rest:
            windows += [pl.ds(n_img * ioff[h], n_img * isz[h]) for h in rest]
        tile = tile_of(cols, DOT)
        wide = code if tile == cols else code // 2
        for n0 in range(0, code, wide):
            out = pl.ds(n0, wide)
            v = 0.0
            for o in range(0, cols, tile):
                g = jnp.concatenate([grad[pl.ds(o, tile), w] for w in windows], axis=1)
                v = v + lax.dot_general(
                    g, txt_s[pl.ds(o, tile), out], (((0,), (0,)), ((), ())), preferred_element_type=F32,
                )
            v = v.astype(BF16)
            slots = [(islot(p, y_), h) for h in full for p in range(n_kl)]
            if with_rest:
                slots += [(s, h) for h in rest for s in range(n_img)]
            o = 0
            for s, h in slots:
                dimg[span(s * D + ioff[h], isz[h], UNIT), out] = v[o:o + isz[h]]
                o += isz[h]

    def to_y(e):
        y_ = (ly + e) % n_ly
        image_piece(y_, e == 1)
        for d in [*range(1, n_kl), 0]:
            for h in range(HB):
                q = rid["gy"] + d * HB + h
                send(dimg.at[brng(islot((kl + d) % n_kl, y_), h), :], ry.at[(e - 1) * n_kl + d, part_of[h], :],
                     "gy", q, dev(ly_=y_), bsz[h])

    x1 = (lx + 1) % n_lx
    to_core(1, 0, True)
    text_piece(order[0], x1, c, True)
    for h in range(HT):
        def to_grad(i, _):
            grad_of(span(row0[h] + i * STEP, STEP, STEP), h)
            return 0
        lax.fori_loop(0, height[h] // STEP, to_grad, 0, unroll=2)
    to_x(1, 0)
    to_core(0, 0)
    text_piece(order[0], lx, c)
    for e in range(1, n_ly):
        to_y(e)

    def owner_copy(i, h):
        j = order[i]
        dest = kl * n_kh + j
        op = copy(dtxt.at[brng(tslot(j, lx, c), h), :], r3.at[kh, part_of[h], :], sid["dz"], rid["dz"], dev(k_=dest))
        return dest, op

    def text_sum(i, h):
        j = order[i]
        rng = brng(tslot(j, lx, c), h)
        v = dtxt[rng, :].astype(F32) + from_core(0, i, h)
        for e in range(1, n_lx):
            got(r2.at[(e - 1) * n_kh + j, part_of[h], :], rid["dx"] + ((e - 1) * n_kh + i) * HB + h)
            v = v + r2[(e - 1) * n_kh + j, part_of[h], :].astype(F32)
        dtxt[rng, :] = v.astype(BF16)
        dest, op = owner_copy(i, h)

        @pl.when(dest != k)
        def _():
            op.start()

        @pl.when(dest == k)
        def _():
            r3[kh, part_of[h], :] = dtxt[rng, :]

    def got_y(d, h):
        got_rows((n_ly - 1) * bsz[h], rid["gy"] + d * HB + h)

    def image_sum(d, h):
        got_y(d, h)
        rng = brng(islot((kl + d) % n_kl, ly), h)
        v = dimg[rng, :].astype(F32)
        for e in range(1, n_ly):
            v = v + ry[(e - 1) * n_kl + d, part_of[h], :].astype(F32)
        dimg[rng, :] = v.astype(BF16)
        send(dimg.at[rng, :], rz.at[d - 1, part_of[h], :], "gz", rid["gz"], dev(k_=kh * n_kl + (kl + d) % n_kl), bsz[h])

    text_sum(0, 0)
    for e in range(1, n_lx):
        for i in range(1 if e == 1 else 0, n_kh):
            to_core(e, i)
            text_piece(order[i], (lx + e) % n_lx, c)
            if e > 1 or i > 1:
                to_x(e, i)
    image_piece(ly, n_ly == 1)
    if n_kh > 1:
        to_x(1, 1)
    texts = [(i, h) for i in range(n_kh) for h in range(HB)][1:]
    images = [(d, h) for d in range(1, n_kl) for h in range(HB)]
    while texts or images:
        if texts:
            i, h = texts.pop(0)
            if h == HB - 1 and i + 1 < n_kh:
                to_core(0, i + 1)
                text_piece(order[i + 1], lx, c)
            text_sum(i, h)
        if images:
            image_sum(*images.pop(0))
    got(part.at[pl.ds(0, len(loss_peers))], rid["loss"])
    loss_out[...] = sum(part[i] for i in range(n_txt)) / float(D * n_row * n_loop)

    def finish(terms, src, inv_ref, out):
        for o in range(0, D, UNIT):
            rng = pl.ds(o, UNIT)
            g = terms(o)
            x = src[rng, :].astype(F32)
            inv = inv_ref[rng, 0:1]
            along = jnp.sum(g * x, axis=1, keepdims=True) * inv * inv
            out[rng, :] = ((g - x * along) * inv).astype(BF16)

    for h in range(HB):
        got_y(0, h)
    got_rows((n_kl - 1) * D, rid["gz"])

    def image_terms(o):
        v = dimg[span(islot(kl, ly) * D + o, UNIT, UNIT), :].astype(F32)
        for e in range(1, n_ly):
            v = v + ry[(e - 1) * n_kl, pl.ds(o, UNIT), :].astype(F32)
        for d in range(1, n_kl):
            v = v + rz[d - 1, pl.ds(o, UNIT), :].astype(F32)
        return v
    finish(image_terms, si, inv_i, gi_out)

    def on_owner(wait):
        @pl.when(src_kl == kl)
        def _():
            wait(n_kh - 1)

        @pl.when(src_kl != kl)
        def _():
            wait(n_kh)
    on_owner(lambda n: got(txt_s.at[pl.ds(0, n * D), :], rid["dz"]))
    finish(lambda o: sum(r3[g, pl.ds(o, UNIT), :].astype(F32) for g in range(n_kh)), st, inv_t, gt_out)

    left(moved_i, sid["t_img"])
    left(moved_t, sid["t_txt"])
    left(stat.at[pl.ds(0, n_img - 1)], sid["stat"])
    left_rows("dc", "dx", "gy", "gz")
    left(part.at[pl.ds(0, len(loss_peers))], sid["loss"])

    on_owner(lambda n: left(txt_s.at[pl.ds(0, n * D), :], sid["dz"]))


def emit(total, gi, gt, loss_out, gi_out, gt_out):
    loss_out[0] = total[0, 0]
    gi_out[...] = gi[...]
    gt_out[...] = gt[...]


def on_device(n_row, n_loop, si, st, ti, tt, ssc, tsc):
    D, code = si.shape
    n_kl, n_lx = 2, 2
    n_kh, n_ly = n_row // (2 * n_kl), n_loop // n_lx
    n_img, n_txt = n_kl * n_ly, n_kh * n_lx * 2
    rows, cols = n_img * D, n_txt * D
    feat = code // n_loop
    rid, sid = make_ids(D, n_kh, n_kl, n_lx, n_ly)
    dims = (n_row, n_loop, n_kh, n_kl, n_lx, n_ly, D, code)
    vm = pl.BlockSpec(memory_space=pltpu.VMEM)
    sm = pl.BlockSpec(memory_space=pltpu.SMEM)
    anywhere = pl.BlockSpec(memory_space=pl.ANY)
    V = pltpu.VMEM
    loss, gi, gt = pl.pallas_call(
        functools.partial(kernel, dims, rid, sid),
        out_shape=(
            jax.ShapeDtypeStruct((8, 128), F32),
            jax.ShapeDtypeStruct((D, code), BF16),
            jax.ShapeDtypeStruct((D, code), BF16),
        ),
        in_specs=[anywhere] * 4 + [sm] * 2,
        out_specs=(vm, vm, vm),
        scratch_shapes=[
            V((rows, code), BF16), V((rows, code), BF16),
            V((D, code), BF16), V((n_ly, n_lx * D, feat), BF16),
            V((cols, code), BF16), V((cols, code), BF16),
            V((n_kl, n_ly, n_lx, n_ly * D, feat), BF16),
            V((n_kh, n_lx, n_ly, n_lx * D, feat), BF16),
            V((cols, rows), F32), V((cols, rows), F32), V((cols, rows), BF16),
            V((n_img, 8, rows), F32),
            V((n_lx * n_kh, D, code), BF16),
            V(((n_lx - 1) * n_kh, D, code), BF16),
            V((n_kh, D, code), BF16),
            V(((n_ly - 1) * n_kl, D, code), BF16),
            V((n_kl - 1, D, code), BF16),
            V((n_txt, 8, 128), F32),
            V((D, 128), F32), V((D, 128), F32),
            V((D, code), BF16), V((D, code), BF16),
            pltpu.SemaphoreType.DMA((sid.count,)),
            pltpu.SemaphoreType.DMA((rid.count,)),
        ],
        compiler_params=pltpu.CompilerParams(
            collective_id=0, has_side_effects=True, vmem_limit_bytes=67043328,
        ),
    )(si, st, ti, tt, ssc, tsc)
    return pl.pallas_call(
        emit,
        out_shape=(
            jax.ShapeDtypeStruct((1,), F32),
            jax.ShapeDtypeStruct((D, code), BF16),
            jax.ShapeDtypeStruct((D, code), BF16),
        ),
        in_specs=[vm] * 3,
        out_specs=(sm, vm, vm),
    )(loss, gi, gt)


def solution(mesh):
    return jax.shard_map(
        functools.partial(on_device, mesh.shape["row"], mesh.shape["loop"]),
        mesh=mesh,
        in_specs=(
            P(("row", "loop"), None),
            P(("row", "loop"), None),
            P("row", "loop"),
            P("row", "loop"),
            P(),
            P(),
        ),
        out_specs=(P(), P(("row", "loop"), None), P(("row", "loop"), None)),
        check_vma=False,
    )
```

```python
import functools
import jax
import jax.numpy as jnp
from jax import lax
from jax.experimental import pallas as pl
from jax.experimental.pallas import tpu as pltpu
from jax.sharding import PartitionSpec as P

EPS = 1e-06
F32 = jnp.float32
BF16 = jnp.bfloat16
MESH = pl.DeviceIdType.MESH
UNIT = 32
IMAGE_PART = 64
STEP = 32
DOT = 1280
TILE = 256


class Ids:
    def __init__(self):
        self.table = {}
        self.count = 0

    def take(self, name, size=1):
        self.table[name] = self.count
        self.count += size

    def __getitem__(self, name):
        return self.table[name]


def split(D, part):
    return [min(part, D - o) for o in range(0, D, part)]


def offsets(sizes):
    return [sum(sizes[:h]) for h in range(len(sizes))]


def back_sizes(D):
    units = D // UNIT
    if units < 4:
        return [UNIT] * units
    return [UNIT, D - 3 * UNIT, UNIT, UNIT]


def make_ids(D, n_kh, n_kl, n_lx, n_ly):
    HI, HT, HB = len(split(D, IMAGE_PART)), D // UNIT, len(back_sizes(D))
    recv, sent = Ids(), Ids()
    recv.take("t_img")
    recv.take("t_txt")
    for a in range(2):
        recv.take(("iz", a), (n_kl - 1) * HI)
        recv.take(("iy", a), HI)
        recv.take(("tz", a), n_kh * HT)
        recv.take(("tx", a), (n_lx - 1) * HT)
        recv.take(("tc", a), HT)
    recv.take("stat")
    recv.take("dc", n_lx * n_kh - 1 + HB)
    recv.take("dx", (n_lx - 1) * n_kh * HB)
    recv.take("dz")
    recv.take("gy", n_kl * HB)
    recv.take("gz")
    recv.take("loss")
    recv.take("keep")
    recv.take("load", 2)
    for name in ("t_img", "t_txt", "stat", "dc", "dx", "dz", "gy", "gz", "loss"):
        sent.take(name)
    for a in range(2):
        for kind in ("img", "first", "txt"):
            sent.take((kind, a))
    return recv, sent


def kernel(
    dims, rid, sid,
    si_in, st_in, ti, tt, ssc, tsc,
    loss_out, gi_out, gt_out,
    img_s, img_t, own_s, own_t, txt_s, txt_t, raw_i, raw_t,
    slog, tlog, grad, stat, r1, r2, r3, ry, rz, part, inv_i, inv_t, si, st,
    ss, rs,
):
    n_row, n_loop, n_kh, n_kl, n_lx, n_ly, D, code = dims
    isz, tsz, bsz = split(D, IMAGE_PART), split(D, UNIT), back_sizes(D)
    ioff, toff, boff = offsets(isz), offsets(tsz), offsets(bsz)
    HI, HT, HB = len(isz), len(tsz), len(bsz)
    n_img = n_kl * n_ly
    n_txt = n_kh * n_lx * 2
    rows = n_img * D
    cols = n_txt * D
    r = lax.axis_index("row")
    l = lax.axis_index("loop")
    k, c = r // 2, r % 2
    kh, kl = k // n_kl, k % n_kl
    src_kl, src_j = k // n_kh, k % n_kh
    ly, lx = l // n_lx, l % n_lx
    sscale = ssc[0]
    tscale = tsc[0]

    def dev(k_=None, c_=None, ly_=None, lx_=None):
        kk = k if k_ is None else k_
        cc = c if c_ is None else c_
        yy = ly if ly_ is None else ly_
        xx = lx if lx_ is None else lx_
        return (kk * 2 + cc, yy * n_lx + xx)

    def islot(kl_, ly_):
        return ly_ * n_kl + kl_

    def tslot(j, lx_, c_):
        return (j * n_lx + lx_) * 2 + c_

    def span(start, size, step):
        return pl.ds(pl.multiple_of(start, step), size)

    def irng(h, slot):
        return span(n_img * ioff[h] + slot * isz[h], isz[h], UNIT)

    def trng(h, slot):
        return span(n_txt * toff[h] + slot * tsz[h], tsz[h], UNIT)

    def brng(slot, h):
        return span(slot * D + boff[h], bsz[h], UNIT)

    def at(slot):
        return span(slot * D, D, UNIT)

    part_of = [pl.ds(boff[h], bsz[h]) for h in range(HB)]

    def image_ref(a, kl_, ly_, h):
        if a == 0:
            return img_s.at[irng(h, islot(kl_, ly_)), :]
        return raw_i.at[kl_, ly_, :, pl.ds(n_ly * ioff[h], n_ly * isz[h]), :]

    def text_ref(a, j, lx_, h):
        if a == 0:
            return txt_s.at[trng(h, tslot(j, lx_, c)), :]
        return raw_t.at[j, lx_, :, pl.ds(n_lx * toff[h], n_lx * tsz[h]), :]

    def own_ref(a, h):
        if a == 0:
            return own_s.at[pl.ds(toff[h], tsz[h]), :]
        return own_t.at[:, pl.ds(n_lx * toff[h], n_lx * tsz[h]), :]

    def copy(src, dst, q_send, q_recv, device):
        return pltpu.make_async_remote_copy(
            src_ref=src, dst_ref=dst, send_sem=ss.at[q_send], recv_sem=rs.at[q_recv],
            device_id=device, device_id_type=MESH,
        )

    sent_rows = {}

    def send(src, dst, name, q, device, n=0):
        copy(src, dst, sid[name], q, device).start()
        sent_rows[name] = sent_rows.get(name, 0) + n

    def got(dst, q):
        copy(dst, dst, 0, q, dev(c_=1 - c)).wait_recv()

    def got_rows(n, q):
        got(txt_s.at[pl.ds(0, n), :], q)

    def left(ref, q):
        copy(ref, ref, q, 0, dev(c_=1 - c)).wait_send()

    def left_rows(*names):
        for name in names:
            left(txt_s.at[pl.ds(0, sent_rows.pop(name)), :], sid[name])

    loss_peers = [
        (kd, xd, cd) for kd in range(n_kh) for xd in range(n_lx) for cd in range(2) if kd or xd or cd
    ]

    def loss_peer(kd, xd, cd):
        return dev(k_=((kh + kd) % n_kh) * n_kl + kl, c_=(c + cd) % 2, lx_=(lx + xd) % n_lx)

    barrier = pltpu.get_barrier_semaphore()
    n_peer = 0
    for kd, xd, cd in loss_peers:
        if (kd != 0) + (xd != 0) + (cd != 0) > 1:
            pl.semaphore_signal(barrier, inc=1, device_id=loss_peer(kd, xd, cd), device_id_type=MESH)
            n_peer += 1
    for e in range(1, n_ly):
        pl.semaphore_signal(barrier, inc=1, device_id=dev(ly_=(ly + e) % n_ly), device_id_type=MESH)
        n_peer += 1
    for e in range(1, n_lx):
        pl.semaphore_signal(barrier, inc=1, device_id=dev(lx_=(lx + e) % n_lx), device_id_type=MESH)
        n_peer += 1
    for d in range(1, n_kh * n_kl):
        pl.semaphore_signal(barrier, inc=1, device_id=dev(k_=(k + d) % (n_kh * n_kl)), device_id_type=MESH)
        n_peer += 1
    pl.semaphore_signal(barrier, inc=1, device_id=dev(c_=1 - c), device_id_type=MESH)
    n_peer += 1
    for d in range(1, n_kl):
        for e in range(1, n_ly):
            diagonal = dev(k_=kh * n_kl + (kl + d) % n_kl, ly_=(ly + e) % n_ly)
            pl.semaphore_signal(barrier, inc=1, device_id=diagonal, device_id_type=MESH)
            n_peer += 1

    def unit(load, dst, first, n, keep=None):
        for o in range(0, n, UNIT):
            x = load(o)
            n2 = jnp.sum(x * x, axis=1, keepdims=True) + EPS
            inv = 1.0 / jnp.sqrt(n2)
            if keep is not None:
                keep(o, inv)
            dst[span(first + o, UNIT, UNIT), :] = (x * inv).astype(BF16)

    def student_unit(src, dst, first, o0, n, inv_ref):
        def load(o):
            return src[pl.ds(o0 + o, UNIT), :].astype(F32)

        def keep(o, inv):
            inv_ref[pl.ds(o0 + o, UNIT), :] = jnp.broadcast_to(inv, (UNIT, 128))
        unit(load, dst, first, n, keep)

    def own_text(h):
        student_unit(st, own_s, toff[h], toff[h], tsz[h], inv_t)

    def own_image(h):
        student_unit(si, img_s, n_img * ioff[h] + islot(kl, ly) * isz[h], ioff[h], isz[h], inv_i)

    def teacher_keep():
        for h in range(HI):
            for y_ in range(n_ly):
                dst = pl.ds(n_ly * ioff[h] + y_ * isz[h], isz[h])
                src = span((y_ * n_lx + lx) * D + ioff[h], isz[h], UNIT)
                pltpu.make_async_copy(ti.at[src, :], raw_i.at[kl, ly, lx, dst, :], rs.at[rid["keep"]]).start()
        for h in range(HT):
            for x_ in range(n_lx):
                dst = pl.ds(n_lx * toff[h] + x_ * tsz[h], tsz[h])
                src = span((ly * n_lx + x_) * D + toff[h], tsz[h], UNIT)
                pltpu.make_async_copy(tt.at[src, :], own_t.at[ly, dst, :], rs.at[rid["keep"]]).start()

    def teacher_kept():
        both = txt_s.at[pl.ds(0, D * (n_ly + n_lx) // n_loop), :]
        pltpu.make_async_copy(both, both, rs.at[rid["keep"]]).wait()

    load_t = pltpu.make_async_copy(st_in, st, rs.at[rid["load"]])
    load_i = pltpu.make_async_copy(si_in, si, rs.at[rid["load"] + 1])
    load_t.start()
    load_i.start()
    teacher_keep()
    load_t.wait()
    own_text(0)
    load_i.wait()
    own_image(0)
    pl.semaphore_wait(barrier, n_peer)

    def teacher_exchange():
        for h in range(HI):
            for y_ in range(n_ly):
                dst = pl.ds(n_ly * ioff[h] + y_ * isz[h], isz[h])
                for e in range(1, n_lx):
                    x_ = (lx + e) % n_lx
                    src = span((y_ * n_lx + x_) * D + ioff[h], isz[h], UNIT)
                    send(ti.at[src, :], raw_i.at[kl, ly, lx, dst, :], "t_img", rid["t_img"], dev(lx_=x_))
        for h in range(HT):
            for x_ in range(n_lx):
                dst = pl.ds(n_lx * toff[h] + x_ * tsz[h], tsz[h])
                for e in range(1, n_ly):
                    y_ = (ly + e) % n_ly
                    src = span((y_ * n_lx + x_) * D + toff[h], tsz[h], UNIT)
                    send(tt.at[src, :], own_t.at[ly, dst, :], "t_txt", rid["t_txt"], dev(ly_=y_))

    moved_i = raw_i.at[0, 0, pl.ds(0, n_lx - 1)]
    moved_t = own_t.at[pl.ds(0, n_ly - 1)]

    def image_z(a, h):
        ref = image_ref(a, kl, ly, h)
        for d in range(1, n_kl):
            q = rid[("iz", a)] + (d - 1) * HI + h
            send(ref, ref, ("img", a), q, dev(k_=kh * n_kl + (kl + d) % n_kl), isz[h])

    def image_y(a, h):
        ref = image_ref(a, kl, ly, h)
        for e in range(1, n_ly):
            send(ref, ref, ("img", a), rid[("iy", a)] + h, dev(ly_=(ly + e) % n_ly), isz[h])

    def image_relay(a, h):
        for d in range(1, n_kl):
            ref = image_ref(a, (kl + n_kl - d) % n_kl, ly, h)
            got(ref, rid[("iz", a)] + (d - 1) * HI + h)
            for e in range(1, n_ly):
                send(ref, ref, ("img", a), rid[("iy", a)] + h, dev(ly_=(ly + e) % n_ly), isz[h])

    def image_finish(a, h):
        got_rows((n_ly - 1) * n_kl * isz[h], rid[("iy", a)] + h)
        if a == 0:
            return
        for p in range(n_kl):
            for y_ in range(n_ly):
                def load(o):
                    rng = pl.ds(n_ly * ioff[h] + y_ * isz[h] + o, UNIT)
                    xs = [raw_i[p, fy, fx, rng, :] for fy in range(n_ly) for fx in range(n_lx)]
                    return jnp.concatenate(xs, axis=1).astype(F32)
                unit(load, img_t, n_img * ioff[h] + islot(p, y_) * isz[h], isz[h])

    def text_first(a, h):
        src = own_ref(a, h)
        for g in range(n_kh):
            dest = g * n_kl + src_kl
            op = copy(src, text_ref(a, src_j, lx, h), sid[("first", a)],
                      rid[("tz", a)] + src_j * HT + h, dev(k_=dest))

            @pl.when(dest != k)
            def _():
                op.start()

            @pl.when(dest == k)
            def _():
                if a == 0:
                    txt_s[trng(h, tslot(src_j, lx, c)), :] = own_s[pl.ds(toff[h], tsz[h]), :]
                else:
                    rng = pl.ds(n_lx * toff[h], n_lx * tsz[h])
                    raw_t[src_j, lx, :, rng, :] = own_t[:, rng, :]

    def first_left(a):
        @pl.when(src_kl == kl)
        def _():
            left(txt_s.at[pl.ds(0, (n_kh - 1) * D), :], sid[("first", a)])

        @pl.when(src_kl != kl)
        def _():
            left(txt_s.at[pl.ds(0, n_kh * D), :], sid[("first", a)])

    def core_send(a, ref, h):
        send(ref, ref, ("txt", a), rid[("tc", a)] + h, dev(c_=1 - c), tsz[h])

    def text_relay(a, h):
        for j in range(n_kh):
            ref = text_ref(a, j, lx, h)

            @pl.when(kl * n_kh + j != k)
            def _():
                got(ref, rid[("tz", a)] + j * HT + h)

            for e in range(1, n_lx):
                send(ref, ref, ("txt", a), rid[("tx", a)] + (e - 1) * HT + h, dev(lx_=(lx + e) % n_lx), tsz[h])
            if a == 0:
                core_send(a, ref, h)

    def text_cross(a, h):
        for e in range(1, n_lx):
            got_rows(n_kh * tsz[h], rid[("tx", a)] + (e - 1) * HT + h)
            for j in range(n_kh):
                if a == 0:
                    core_send(a, text_ref(a, j, (lx + n_lx - e) % n_lx, h), h)
        if a == 0:
            return
        for j in range(n_kh):
            for x_ in range(n_lx):
                def load(o):
                    rng = pl.ds(n_lx * toff[h] + x_ * tsz[h] + o, UNIT)
                    xs = [raw_t[j, fx, fy, rng, :] for fy in range(n_ly) for fx in range(n_lx)]
                    return jnp.concatenate(xs, axis=1).astype(F32)
                unit(load, txt_t, n_txt * toff[h] + tslot(j, x_, c) * tsz[h], tsz[h])
                core_send(a, txt_t.at[trng(h, tslot(j, x_, c)), :], h)

    def text_finish(a, h):
        got_rows(n_lx * n_kh * tsz[h], rid[("tc", a)] + h)

    def tile_of(n, most):
        return max(t for t in range(UNIT, min(n, most) + 1, UNIT) if n % t == 0)

    def logits(txt, img, scale, out, row0, n, lane0=0, width=rows):
        tile = tile_of(n, TILE)
        lanes = pl.ds(lane0, width)
        m = jnp.full((8, width), -jnp.inf, F32)
        for o in range(row0, row0 + n, tile):
            v = scale * lax.dot_general(
                txt[pl.ds(o, tile), :], img[lanes, :], (((1,), (1,)), ((), ())),
                preferred_element_type=F32,
            )
            out[pl.ds(o, tile), lanes] = v
            m = jnp.maximum(m, jnp.max(v.reshape(tile // 8, 8, width), axis=0))
        return jnp.max(m, axis=0, keepdims=True)

    def zipped(image_step, text_step):
        for h in range(max(HI, HT)):
            if h < HT:
                text_step(h)
            if h < HI:
                image_step(h)

    teacher_exchange()

    def student_text(h):
        if h:
            own_text(h)
        text_first(0, h)

    def student_image(h):
        if h:
            own_image(h)
        image_z(0, h)
        image_y(0, h)
    zipped(student_image, student_text)
    text_relay(0, 0)
    image_relay(0, 0)
    teacher_kept()
    got(moved_i, rid["t_img"])
    got(moved_t, rid["t_txt"])
    ahead = min(2, HT)
    for h in range(ahead):
        text_first(1, h)
    for h in range(max(HI, HT - ahead)):
        if h < HI:
            image_z(1, h)
        if ahead + h < HT:
            text_first(1, ahead + h)
    relay_s = [functools.partial(text_relay, 0, h) for h in range(1, HT)]
    relay_t = [functools.partial(text_relay, 1, h) for h in range(HT)]
    image_s = [functools.partial(image_relay, 0, h) for h in range(1, HI)]
    image_t = [functools.partial(image_relay, 1, h) for h in range(HI)]
    cross_s = [functools.partial(text_cross, 0, h) for h in range(HT)]
    cross_t = [functools.partial(text_cross, 1, h) for h in range(HT)]
    finish_t = [functools.partial(image_finish, 1, h) for h in range(HI)]

    def step(*queues):
        for queue in queues:
            if queue:
                queue.pop(0)()

    step(relay_s)
    while relay_s:
        step(image_s, relay_s, cross_s)
    while image_s:
        step(image_s)
    for h in range(HI):
        image_y(1, h)
    while len(cross_s) > 2:
        step(cross_s)
    step(relay_t)
    step(cross_s, cross_s)
    step(relay_t)
    while cross_s:
        step(cross_s)
    for h in range(HI):
        image_finish(0, h)
    for h in range(HT):
        text_finish(0, h)
    step(image_t)
    step(relay_t)
    smax = logits(txt_s, img_s, sscale, slog, 0, cols)
    step(image_t)
    step(cross_t)
    step(relay_t)
    step(image_t)
    step(cross_t)
    while image_t:
        step(image_t)
    while relay_t:
        step(relay_t)
    while len(cross_t) > 2:
        step(cross_t)

    def exps(row0, n, top_t, lane0=0, width=rows):
        lanes = pl.ds(lane0, width)
        top_s = smax[:, lane0:lane0 + width]

        def fold(v):
            return jnp.sum(v.reshape(STEP // 8, 8, width), axis=0)

        def body(i, carry):
            a, b, x = carry
            o = pl.multiple_of(row0 + i * STEP, STEP)
            s = slog[pl.ds(o, STEP), lanes]
            t = tlog[pl.ds(o, STEP), lanes]
            es = jnp.exp(s - top_s)
            et = jnp.exp(t - top_t)
            slog[pl.ds(o, STEP), lanes] = es
            tlog[pl.ds(o, STEP), lanes] = et
            return (a + fold(es), b + fold(et), x + fold(et * (t - s)))
        zero = jnp.zeros((8, width), F32)
        sums = lax.fori_loop(0, n // STEP, body, (zero, zero, zero))
        return [jnp.sum(v, axis=0, keepdims=True) for v in sums]

    row0 = [n_txt * o for o in toff]
    height = [n_txt * n for n in tsz]
    tops = []
    sums = []

    tops_at = []

    def keep_stats(top, sums_, n):
        tops.append(top)
        tops_at.extend([top] * n)
        sums.append(sums_)

    def teacher(h):
        text_finish(1, h)
        top = logits(txt_t, img_t, tscale, tlog, row0[h], height[h])
        while cross_t:
            step(cross_t)
        keep_stats(top, exps(row0[h], height[h], top), 1)

    first = max(HT - 3, 1)
    n0 = sum(height[:first])
    for h in range(first):
        text_finish(1, h)
    parts = []
    for i in range(HI):
        step(finish_t)
        window = (n_img * ioff[i], n_img * isz[i])
        top = logits(txt_t, img_t, tscale, tlog, 0, n0, *window)
        parts.append([top] + exps(0, n0, top, *window))
        if i + 2 == HI and len(cross_t) > 1:
            step(cross_t)
    parts = [jnp.concatenate(v, axis=1) for v in zip(*parts)]
    keep_stats(parts[0], parts[1:], first)
    for h in range(first, HT):
        teacher(h)

    tmax = functools.reduce(jnp.maximum, tops)
    shift = [jnp.exp(m - tmax) for m in tops]
    asum = sum(v[0] for v in sums)
    bsum = sum(v[1] * e for v, e in zip(sums, shift))
    xsum = sum(v[2] * e for v, e in zip(sums, shift))
    pack = [smax, tmax, asum, bsum, xsum]
    stat[islot(kl, ly)] = jnp.concatenate(pack + [jnp.zeros((3, rows), F32)], axis=0)
    for d in range(n_kl):
        for e in range(n_ly):
            if d or e:
                send(stat.at[islot(kl, ly)], stat.at[islot(kl, ly)], "stat", rid["stat"],
                     dev(k_=kh * n_kl + (kl + d) % n_kl, ly_=(ly + e) % n_ly))
    for a in range(2):
        first_left(a)
        left_rows(("img", a), ("txt", a))
    got(stat.at[pl.ds(0, n_img - 1)], rid["stat"])

    all_stat = [stat[s] for s in range(n_img)]
    gs = functools.reduce(jnp.maximum, [v[0:1] for v in all_stat])
    gt = functools.reduce(jnp.maximum, [v[1:2] for v in all_stat])
    es = [jnp.exp(v[0:1] - gs) for v in all_stat]
    et = [jnp.exp(v[1:2] - gt) for v in all_stat]
    ssum = sum(v[2:3] * e for v, e in zip(all_stat, es))
    tsum = sum(v[3:4] * e for v, e in zip(all_stat, et))
    cross = sum(v[4:5] * e for v, e in zip(all_stat, et))
    diverge = cross / tsum - (gt + jnp.log(tsum)) + (gs + jnp.log(ssum))
    mine = tslot(kh, lx, c)
    part[mine] = jnp.broadcast_to(jnp.sum(diverge, axis=1, keepdims=True), (8, 128))
    for peer in loss_peers:
        send(part.at[mine], part.at[mine], "loss", rid["loss"], loss_peer(*peer))

    s_mul = sscale * jnp.exp(smax - gs) / ssum
    t_scale = sscale / tsum

    t_mul = [t_scale * jnp.exp(m - gt) for m in tops_at]

    dtxt = txt_t

    def grad_of(rng, h):
        v = (slog[rng, :] * s_mul - tlog[rng, :] * t_mul[h]).astype(BF16)
        grad[rng, :] = v
        return v

    def text_piece(j, lx_, c_, fresh=False):
        slot = tslot(j, lx_, c_)
        if fresh:
            g = [grad_of(trng(h, slot), h) for h in range(HT)]
        else:
            g = [grad[trng(h, slot), :] for h in range(HT)]
        v = jnp.dot(jnp.concatenate(g, axis=0), img_s[...], preferred_element_type=F32)
        dtxt[at(slot), :] = v.astype(BF16)

    order = [(n_kh - 1 - kh + i) % n_kh for i in range(n_kh)]

    def core_id(e, i):
        first = n_kh if n_lx > 1 else 0
        n = e * n_kh + i
        if n == first:
            return rid["dc"] + n_lx * n_kh - 1
        return rid["dc"] + (n if n < first else n - 1)

    def chunked(e, i):
        return e == (1 if n_lx > 1 else 0) and i == 0

    def to_core(e, i, fresh=False):
        x_ = (lx + e) % n_lx
        j = order[i]
        text_piece(j, x_, 1 - c, fresh)
        if chunked(e, i):
            for h in range(HB):
                send(dtxt.at[brng(tslot(j, x_, 1 - c), h), :], r1.at[x_ * n_kh + j, part_of[h], :], "dc",
                     core_id(e, i) + h, dev(c_=1 - c), bsz[h])
        else:
            send(dtxt.at[at(tslot(j, x_, 1 - c)), :], r1.at[x_ * n_kh + j], "dc", core_id(e, i), dev(c_=1 - c), D)

    def from_core(e, i, h):
        s = ((lx + e) % n_lx) * n_kh + order[i]
        if chunked(e, i):
            got(r1.at[s, part_of[h], :], core_id(e, i) + h)
        elif h == 0:
            got(r1.at[s], core_id(e, i))
        return r1[s, part_of[h], :].astype(F32)

    def to_x(e, i):
        x_ = (lx + e) % n_lx
        j = order[i]
        for h in range(HB):
            rng = brng(tslot(j, x_, c), h)
            dtxt[rng, :] = (dtxt[rng, :].astype(F32) + from_core(e, i, h)).astype(BF16)
            q = rid["dx"] + ((e - 1) * n_kh + i) * HB + h
            send(dtxt.at[rng, :], r2.at[(e - 1) * n_kh + j, part_of[h], :], "dx", q, dev(lx_=x_), bsz[h])

    dimg = img_t
    full = [h for h in range(HI) if (n_kl * isz[h]) % 128 == 0]
    rest = [h for h in range(HI) if h not in full]

    def image_piece(y_, with_rest):
        windows = [span(n_img * ioff[h] + y_ * n_kl * isz[h], n_kl * isz[h], 128) for h in full]
        if with_rest:
            windows += [pl.ds(n_img * ioff[h], n_img * isz[h]) for h in rest]
        tile = tile_of(cols, DOT)
        wide = code if tile == cols else code // 2
        for n0 in range(0, code, wide):
            out = pl.ds(n0, wide)
            v = 0.0
            for o in range(0, cols, tile):
                g = jnp.concatenate([grad[pl.ds(o, tile), w] for w in windows], axis=1)
                v = v + lax.dot_general(
                    g, txt_s[pl.ds(o, tile), out], (((0,), (0,)), ((), ())), preferred_element_type=F32,
                )
            v = v.astype(BF16)
            slots = [(islot(p, y_), h) for h in full for p in range(n_kl)]
            if with_rest:
                slots += [(s, h) for h in rest for s in range(n_img)]
            o = 0
            for s, h in slots:
                dimg[span(s * D + ioff[h], isz[h], UNIT), out] = v[o:o + isz[h]]
                o += isz[h]

    def to_y(e):
        y_ = (ly + e) % n_ly
        image_piece(y_, e == 1)
        for d in [*range(1, n_kl), 0]:
            for h in range(HB):
                q = rid["gy"] + d * HB + h
                send(dimg.at[brng(islot((kl + d) % n_kl, y_), h), :], ry.at[(e - 1) * n_kl + d, part_of[h], :],
                     "gy", q, dev(ly_=y_), bsz[h])

    x1 = (lx + 1) % n_lx
    to_core(1, 0, True)
    text_piece(order[0], x1, c, True)
    for h in range(HT):
        def to_grad(i, _):
            grad_of(span(row0[h] + i * STEP, STEP, STEP), h)
            return 0
        lax.fori_loop(0, height[h] // STEP, to_grad, 0, unroll=2)
    to_x(1, 0)
    to_core(0, 0)
    text_piece(order[0], lx, c)
    for e in range(1, n_ly):
        to_y(e)

    def owner_copy(i, h):
        j = order[i]
        dest = kl * n_kh + j
        op = copy(dtxt.at[brng(tslot(j, lx, c), h), :], r3.at[kh, part_of[h], :], sid["dz"], rid["dz"], dev(k_=dest))
        return dest, op

    def text_sum(i, h):
        j = order[i]
        rng = brng(tslot(j, lx, c), h)
        v = dtxt[rng, :].astype(F32) + from_core(0, i, h)
        for e in range(1, n_lx):
            got(r2.at[(e - 1) * n_kh + j, part_of[h], :], rid["dx"] + ((e - 1) * n_kh + i) * HB + h)
            v = v + r2[(e - 1) * n_kh + j, part_of[h], :].astype(F32)
        dtxt[rng, :] = v.astype(BF16)
        dest, op = owner_copy(i, h)

        @pl.when(dest != k)
        def _():
            op.start()

        @pl.when(dest == k)
        def _():
            r3[kh, part_of[h], :] = dtxt[rng, :]

    def got_y(d, h):
        got_rows((n_ly - 1) * bsz[h], rid["gy"] + d * HB + h)

    def image_sum(d, h):
        got_y(d, h)
        rng = brng(islot((kl + d) % n_kl, ly), h)
        v = dimg[rng, :].astype(F32)
        for e in range(1, n_ly):
            v = v + ry[(e - 1) * n_kl + d, part_of[h], :].astype(F32)
        dimg[rng, :] = v.astype(BF16)
        send(dimg.at[rng, :], rz.at[d - 1, part_of[h], :], "gz", rid["gz"], dev(k_=kh * n_kl + (kl + d) % n_kl), bsz[h])

    text_sum(0, 0)
    for e in range(1, n_lx):
        for i in range(1 if e == 1 else 0, n_kh):
            to_core(e, i)
            text_piece(order[i], (lx + e) % n_lx, c)
            if e > 1 or i > 1:
                to_x(e, i)
    image_piece(ly, n_ly == 1)
    if n_kh > 1:
        to_x(1, 1)
    texts = [(i, h) for i in range(n_kh) for h in range(HB)][1:]
    images = [(d, h) for d in range(1, n_kl) for h in range(HB)]
    while texts or images:
        if texts:
            i, h = texts.pop(0)
            if h == HB - 1 and i + 1 < n_kh:
                to_core(0, i + 1)
                text_piece(order[i + 1], lx, c)
            text_sum(i, h)
        if images:
            image_sum(*images.pop(0))
    got(part.at[pl.ds(0, len(loss_peers))], rid["loss"])
    loss_out[...] = sum(part[i] for i in range(n_txt)) / float(D * n_row * n_loop)

    def finish(terms, src, inv_ref, out):
        for o in range(0, D, UNIT):
            rng = pl.ds(o, UNIT)
            g = terms(o)
            x = src[rng, :].astype(F32)
            inv = inv_ref[rng, 0:1]
            along = jnp.sum(g * x, axis=1, keepdims=True) * inv * inv
            out[rng, :] = ((g - x * along) * inv).astype(BF16)

    for h in range(HB):
        got_y(0, h)
    got_rows((n_kl - 1) * D, rid["gz"])

    def image_terms(o):
        v = dimg[span(islot(kl, ly) * D + o, UNIT, UNIT), :].astype(F32)
        for e in range(1, n_ly):
            v = v + ry[(e - 1) * n_kl, pl.ds(o, UNIT), :].astype(F32)
        for d in range(1, n_kl):
            v = v + rz[d - 1, pl.ds(o, UNIT), :].astype(F32)
        return v
    finish(image_terms, si, inv_i, gi_out)

    def on_owner(wait):
        @pl.when(src_kl == kl)
        def _():
            wait(n_kh - 1)

        @pl.when(src_kl != kl)
        def _():
            wait(n_kh)
    on_owner(lambda n: got(txt_s.at[pl.ds(0, n * D), :], rid["dz"]))
    finish(lambda o: sum(r3[g, pl.ds(o, UNIT), :].astype(F32) for g in range(n_kh)), st, inv_t, gt_out)

    left(moved_i, sid["t_img"])
    left(moved_t, sid["t_txt"])
    left(stat.at[pl.ds(0, n_img - 1)], sid["stat"])
    left_rows("dc", "dx", "gy", "gz")
    left(part.at[pl.ds(0, len(loss_peers))], sid["loss"])

    on_owner(lambda n: left(txt_s.at[pl.ds(0, n * D), :], sid["dz"]))


def emit(total, gi, gt, loss_out, gi_out, gt_out):
    loss_out[0] = total[0, 0]
    gi_out[...] = gi[...]
    gt_out[...] = gt[...]


def on_device(n_row, n_loop, si, st, ti, tt, ssc, tsc):
    D, code = si.shape
    n_kl, n_lx = 2, 2
    n_kh, n_ly = n_row // (2 * n_kl), n_loop // n_lx
    n_img, n_txt = n_kl * n_ly, n_kh * n_lx * 2
    rows, cols = n_img * D, n_txt * D
    feat = code // n_loop
    rid, sid = make_ids(D, n_kh, n_kl, n_lx, n_ly)
    dims = (n_row, n_loop, n_kh, n_kl, n_lx, n_ly, D, code)
    vm = pl.BlockSpec(memory_space=pltpu.VMEM)
    sm = pl.BlockSpec(memory_space=pltpu.SMEM)
    anywhere = pl.BlockSpec(memory_space=pl.ANY)
    V = pltpu.VMEM
    loss, gi, gt = pl.pallas_call(
        functools.partial(kernel, dims, rid, sid),
        out_shape=(
            jax.ShapeDtypeStruct((8, 128), F32),
            jax.ShapeDtypeStruct((D, code), BF16),
            jax.ShapeDtypeStruct((D, code), BF16),
        ),
        in_specs=[anywhere] * 4 + [sm] * 2,
        out_specs=(vm, vm, vm),
        scratch_shapes=[
            V((rows, code), BF16), V((rows, code), BF16),
            V((D, code), BF16), V((n_ly, n_lx * D, feat), BF16),
            V((cols, code), BF16), V((cols, code), BF16),
            V((n_kl, n_ly, n_lx, n_ly * D, feat), BF16),
            V((n_kh, n_lx, n_ly, n_lx * D, feat), BF16),
            V((cols, rows), F32), V((cols, rows), F32), V((cols, rows), BF16),
            V((n_img, 8, rows), F32),
            V((n_lx * n_kh, D, code), BF16),
            V(((n_lx - 1) * n_kh, D, code), BF16),
            V((n_kh, D, code), BF16),
            V(((n_ly - 1) * n_kl, D, code), BF16),
            V((n_kl - 1, D, code), BF16),
            V((n_txt, 8, 128), F32),
            V((D, 128), F32), V((D, 128), F32),
            V((D, code), BF16), V((D, code), BF16),
            pltpu.SemaphoreType.DMA((sid.count,)),
            pltpu.SemaphoreType.DMA((rid.count,)),
        ],
        compiler_params=pltpu.CompilerParams(
            collective_id=0, has_side_effects=True, vmem_limit_bytes=67043328,
        ),
    )(si, st, ti, tt, ssc, tsc)
    return pl.pallas_call(
        emit,
        out_shape=(
            jax.ShapeDtypeStruct((1,), F32),
            jax.ShapeDtypeStruct((D, code), BF16),
            jax.ShapeDtypeStruct((D, code), BF16),
        ),
        in_specs=[vm] * 3,
        out_specs=(sm, vm, vm),
    )(loss, gi, gt)


def solution(mesh):
    return jax.shard_map(
        functools.partial(on_device, mesh.shape["row"], mesh.shape["loop"]),
        mesh=mesh,
        in_specs=(
            P(("row", "loop"), None),
            P(("row", "loop"), None),
            P("row", "loop"),
            P("row", "loop"),
            P(),
            P(),
        ),
        out_specs=(P(), P(("row", "loop"), None), P(("row", "loop"), None)),
        check_vma=False,
    )
```
